256 devices in a mesh: seq: 16 (over y_lo, z), tensor: 16 (over y_hi, x, core).
Axes of the slice: x: 4, y: 4 (y_hi: 2, y_lo: 2; y = y_hi * 2 + y_lo), z: 8, core: 2. Of those that a mesh axis runs over, the one named last changes fastest.
Arguments:
- fixed_point: bfloat16 [2048, 4096], P(('seq', 'tensor')), may hold values from -6 to 6
- incoming: bfloat16 [2048, 4096], P(('seq', 'tensor')), may hold values from -6 to 6
- norm_gain: float32 [4096], replicated, may hold values from 0.1 to 1.9
- query_weight: bfloat16 [4096, 4096], P(None, 'tensor'), may hold values from -0.21875 to 0.21875, as said below
- key_weight: bfloat16 [4096, 4096], P(None, 'tensor'), may hold values from -0.265625 to 0.265625, as said below
- value_weight: bfloat16 [4096, 4096], P(None, 'tensor'), may hold values from -0.09375 to 0.09375
- out_weight: bfloat16 [4096, 4096], P('tensor'), may hold values from -0.09375 to 0.09375
- layout: int32 [32, 32], replicated, may hold values 0 or 1
Outputs:
- adjoint: float32 [2048, 4096], P(('seq', 'tensor'))
- gain_grad: float32 [4096], replicated
The draws below stay inside these ranges and needn't reach their ends.
Inputs may be any that keep to these rules, and one draw needn't show every extreme that they name: `query_weight`: entries of the columns of each head are independent; their spread may differ between heads. `key_weight`: entries are independent within a draw; columns of some heads may follow the same head's columns of query_weight. `layout`: A key block strictly before a query block is attended where the entry at row query block, column key block is 1; a block always attends itself causally; entries on or above the diagonal are not read.
All inputs are finite; a program needn't handle non-finite values.
Results may differ from the reference program's by a relative error of at most 0.03.
Values may be sent and summed in bfloat16 or wider, within the bound.
A program may use at most 64 MiB of HBM per device.

```python
import jax
import jax.numpy as jnp
from jax import lax

D = 4096
HEADS = 32
HEAD_DIM = 128
BLK = 64
ITERS = 2
HEADS_DEV = 2
LENGTH = 2048
NBLK = 32


def projection_pair(key):
    first = jax.random.truncated_normal(jax.random.fold_in(key, 11), -4.0, 4.0, (D, D), jnp.float32)
    second = jax.random.truncated_normal(jax.random.fold_in(key, 23), -4.0, 4.0, (D, D), jnp.float32)
    plain = (2.0 / D) ** 0.5
    query = first * plain
    keyed = second * plain
    return (query, keyed)


def draw_query_weight(key, part):
    return projection_pair(key)[0].astype(jnp.bfloat16)


def draw_key_weight(key, part):
    return projection_pair(key)[1].astype(jnp.bfloat16)


def set_ends(values, stream_key, least, top_value):
    shape = values.shape
    place = [jax.random.randint(jax.random.fold_in(stream_key, axis), (), 0, shape[axis]) for axis in range(len(shape))]
    values = values.at[tuple(place)].set(least)
    longest = shape.index(max(shape))
    place[longest] = (place[longest] + 1) % shape[longest]
    return values.at[tuple(place)].set(top_value)


def block_levels(own_key, shape, cuts, smallest, top_value):
    def one(dim, parts):
        heights = jax.random.uniform(jax.random.fold_in(jax.random.fold_in(own_key, 6), dim), (parts,), jnp.float32, smallest / len(cuts), top_value / len(cuts))
        return jnp.repeat(jnp.exp(heights), shape[dim] // parts).reshape((-1,) + (1,) * (len(shape) - dim - 1))

    loudness = one(*cuts[0])
    for cut in cuts[1:]:
        loudness = loudness * one(*cut)
    return loudness


def noise(stream_key, dims, scale, bound, cuts=(), kind=jnp.bfloat16):
    values = scale * jax.random.normal(stream_key, dims, jnp.float32)
    if cuts:
        values = values * block_levels(stream_key, dims, cuts, -0.22, 0.18)
    return jnp.clip(values, -bound, bound).astype(kind)


def setup_inputs(seed: int = 0) -> dict:
    splits = jax.random.split(jax.random.key(seed), 9)
    fixed_point = noise(splits[0], (LENGTH, D), 1.0, 6.0, ((0, 256),))
    incoming = noise(splits[1], (LENGTH, D), 1.0, 6.0, ((0, 256),))
    norm_gain = jnp.clip(1.0 + 0.18 * jax.random.normal(splits[2], (D,), jnp.float32), 0.1, 1.9)
    query_weight = draw_query_weight(jax.random.fold_in(splits[8], 71), 0)
    key_weight = draw_key_weight(jax.random.fold_in(splits[8], 71), 0)
    value_weight = noise(splits[5], (D, D), D ** -0.5, 0.09375, ((1, 16),))
    out_weight = noise(splits[6], (D, D), D ** -0.5, 0.09375, ((0, 16),))
    layout = set_ends((jax.random.randint(splits[7], (NBLK, NBLK), 0, 4) < 3).astype(jnp.int32), jax.random.fold_in(splits[7], 1), 0, 1)
    return dict(fixed_point=fixed_point, incoming=incoming, norm_gain=norm_gain, query_weight=query_weight, key_weight=key_weight, value_weight=value_weight, out_weight=out_weight, layout=layout)


EPS = 1e-05
THETA = 10000.0
MASKED = -1e+30

def round_low(values):
    return lax.optimization_barrier(values.astype(jnp.bfloat16)).astype(jnp.float32)

def rope_tables(positions):
    freq = THETA ** (-jnp.arange(0, HEAD_DIM, 2, dtype=jnp.float32) / HEAD_DIM)
    angle = positions.astype(jnp.float32)[:, None] * freq[None, :]
    cosine = jnp.concatenate([jnp.cos(angle), jnp.cos(angle)], axis=1)[:, None, :]
    sine = jnp.concatenate([jnp.sin(angle), jnp.sin(angle)], axis=1)[:, None, :]
    return (cosine, sine)

def rotate(values, cosine, sine):
    half = HEAD_DIM // 2
    turned = jnp.concatenate([-values[..., half:], values[..., :half]], axis=-1)
    return values * cosine + turned * sine

def rotate_back(values, cosine, sine):
    half = HEAD_DIM // 2
    weighted = values * sine
    turned = jnp.concatenate([weighted[..., half:], -weighted[..., :half]], axis=-1)
    return values * cosine + turned

def expand_blocks(chosen):
    return jnp.repeat(jnp.repeat(chosen, BLK, axis=0), BLK, axis=1)

def pair_mask(query_pos, key_pos, chosen):
    query_block = (query_pos // BLK)[:, None]
    key_block = (key_pos // BLK)[None, :]
    earlier = (key_block < query_block) & chosen
    same = (key_block == query_block) & (key_pos[None, :] <= query_pos[:, None])
    return earlier | same

def reference(fixed_point, incoming, norm_gain, query_weight, key_weight, value_weight, out_weight, layout):
    groups = HEADS // HEADS_DEV
    width = HEADS_DEV * HEAD_DIM
    score_scale = HEAD_DIM ** (-0.5)
    point = fixed_point.astype(jnp.float32)
    inv_rms = lax.rsqrt(lax.optimization_barrier(jnp.mean(point * point, axis=1, keepdims=True)) + EPS)
    scaled = point * inv_rms
    normed = (norm_gain * scaled).astype(jnp.bfloat16)
    positions = jnp.arange(LENGTH, dtype=jnp.int32)
    cosine, sine = rope_tables(positions)

    def project(weight):
        return jnp.dot(normed, weight, preferred_element_type=jnp.float32).reshape(LENGTH, HEADS, HEAD_DIM)

    def split_heads(values):
        return values.reshape(LENGTH, groups, HEADS_DEV, HEAD_DIM).transpose(1, 0, 2, 3)
    queries = split_heads(rotate(project(query_weight), cosine, sine).astype(jnp.bfloat16))
    keys = split_heads(rotate(project(key_weight), cosine, sine).astype(jnp.bfloat16))
    values = split_heads(project(value_weight).astype(jnp.bfloat16))
    allowed = pair_mask(positions, positions, expand_blocks(layout > 0))[None]

    def probabilities(query_group, key_group):
        scores = jnp.einsum('qhd,khd->hqk', query_group.astype(jnp.float32), key_group.astype(jnp.float32)) * score_scale
        scores = jnp.where(allowed, scores, MASKED)
        return jnp.exp(scores - jax.nn.logsumexp(scores, axis=2, keepdims=True))

    def forward_group(operands):
        query_group, key_group, value_group = operands
        probs = probabilities(query_group, key_group)
        attended = jnp.einsum('hqk,khd->qhd', round_low(probs), value_group.astype(jnp.float32))
        return attended.astype(jnp.bfloat16)
    attended = lax.map(forward_group, (queries, keys, values))
    query_cols = query_weight.reshape(D, groups, width).transpose(1, 0, 2)
    key_cols = key_weight.reshape(D, groups, width).transpose(1, 0, 2)
    value_cols = value_weight.reshape(D, groups, width).transpose(1, 0, 2)
    out_rows = out_weight.reshape(groups, width, D)

    def backprop(cotangent):
        cotangent_low = cotangent.astype(jnp.bfloat16)

        def group_step(total, operands):
            query_group, key_group, value_group, attended_group, query_col, key_col, value_col, out_row = operands
            grad_out = jnp.dot(cotangent_low, out_row.T, preferred_element_type=jnp.float32).astype(jnp.bfloat16)
            grad_wide = grad_out.astype(jnp.float32).reshape(LENGTH, HEADS_DEV, HEAD_DIM)
            delta = lax.optimization_barrier(jnp.sum(grad_wide * attended_group.astype(jnp.float32), axis=2)).T
            probs = probabilities(query_group, key_group)
            grad_probs = jnp.einsum('qhd,khd->hqk', grad_wide, value_group.astype(jnp.float32))
            grad_scores = round_low(probs * (grad_probs - delta[:, :, None]))
            grad_query = jnp.einsum('hqk,khd->qhd', grad_scores, key_group.astype(jnp.float32)) * score_scale
            grad_key = jnp.einsum('hqk,qhd->khd', grad_scores, query_group.astype(jnp.float32)) * score_scale
            grad_value = jnp.einsum('hqk,qhd->khd', round_low(probs), grad_wide)
            query_low = rotate_back(grad_query, cosine, sine).astype(jnp.bfloat16).reshape(LENGTH, width)
            key_low = rotate_back(grad_key, cosine, sine).astype(jnp.bfloat16).reshape(LENGTH, width)
            value_low = grad_value.astype(jnp.bfloat16).reshape(LENGTH, width)
            partial_sum = jnp.dot(query_low, query_col.T, preferred_element_type=jnp.float32)
            partial_sum = partial_sum + jnp.dot(key_low, key_col.T, preferred_element_type=jnp.float32)
            partial_sum = partial_sum + jnp.dot(value_low, value_col.T, preferred_element_type=jnp.float32)
            return (total + round_low(partial_sum), None)
        operands = (queries, keys, values, attended, query_cols, key_cols, value_cols, out_rows)
        grad_normed, _ = lax.scan(group_step, jnp.zeros((LENGTH, D), jnp.float32), operands)
        return grad_normed
    cotangent = incoming.astype(jnp.float32)
    adjoint = cotangent
    gain_total = jnp.zeros((D,), jnp.float32)
    for term_index in range(ITERS):
        grad_normed = backprop(cotangent)
        gain_total = gain_total + lax.optimization_barrier(jnp.sum(grad_normed * scaled, axis=0))
        weighted = norm_gain * grad_normed
        inner = lax.optimization_barrier(jnp.sum(weighted * scaled, axis=1, keepdims=True))
        cotangent = inv_rms * (weighted - scaled * (inner / D))
        adjoint = adjoint + cotangent
    return (adjoint, gain_total * LENGTH ** (-0.5))
```

```python
import functools

import jax
import jax.numpy as jnp
from jax import lax
from jax.experimental import pallas as pl
from jax.experimental.pallas import tpu as pltpu
from jax.sharding import Mesh
from jax.sharding import PartitionSpec as P

HEAD_DIM = 128
BLK = 64
ITERS = 2
EPS = 1e-05
THETA = 10000.0
MASKED = -1e30
AXES = ("seq_0", "seq_1", "tensor_0", "tensor_1", "tensor_2")
TENSOR = ("tensor_0", "tensor_1", "tensor_2")
SEQ = ("seq_0", "seq_1")
SEQ_TENSOR = AXES
MESH = pl.DeviceIdType.MESH
F32, BF16 = jnp.float32, jnp.bfloat16

NY, NZ, NH, NX, NC = 2, 8, 2, 4, 2
CHIPS = NH * NX
ROWS = 8
CROWS = NC * ROWS
TOK = CHIPS * CROWS
PLANE = NZ * TOK
D = 4096
HALF = D // 2
HEADS_DEV = 2
WIDTH = HEADS_DEV * HEAD_DIM
NBLK = 32

CHIP_STEPS = ((0, 1), (0, 3), (1, 0), (0, 2), (1, 1), (1, 3), (1, 2))
SEQ_STEPS = tuple((a, b) for a in range(NY) for b in range(NZ) if (a, b) != (0, 0))
KV, QDO, OTHER, DO2, OTHER2 = range(5)

NN = (((1,), (0,)), ((), ()))
NT = (((1,), (1,)), ((), ()))


def dot(a, b, dims=NN):
    return lax.dot_general(a, b, dims, preferred_element_type=F32)


def kernel(
    point_ref, inc_ref, gain_ref, cos_ref, sin_ref, lay_ref, wq_hbm, wk_hbm, wv_hbm, wo_hbm,
    adj_ref, gg_ref,
    wq, wk, wv, wo, loc, sc16, in16, ir16, irl, agx, agi, agc,
    kv, qdo, oth, do2, oth2, st, bq, bk, pq, pk, att, dqkv, tot, totf, drv, rsrc, rrv, gn,
    inl, inr, adj16, adjr, gacc, gt, gs, gh,
    w_sem, ags, agr, fws, fwr, d2s, d2r, rgs, rgr, yxs, yxr, sts, str_, rss, rsr, gts, gtr, gss, gsr,
):
    yl, z, yh, x, c = (lax.axis_index(a) for a in AXES)
    chip = yh * NX + x
    s = yl * NZ + z
    scale = HEAD_DIM ** (-0.5)

    def dev(yl_=None, z_=None, yh_=None, x_=None, c_=None):
        pick = lambda a, b: a if b is None else b
        return (pick(yl, yl_), pick(z, z_), pick(yh, yh_), pick(x, x_), pick(c, c_))

    partner = dev(c_=1 - c)
    own_half = pl.ds(pl.multiple_of(c * HALF, HALF), HALF)
    far_half = pl.ds(pl.multiple_of((1 - c) * HALF, HALF), HALF)
    own_rows = pl.ds(pl.multiple_of(c * ROWS, ROWS), ROWS)
    far_rows = pl.ds(pl.multiple_of((1 - c) * ROWS, ROWS), ROWS)

    def remote(src, dst, ssem, rsem, to):
        return pltpu.make_async_remote_copy(
            src_ref=src, dst_ref=dst, send_sem=ssem, recv_sem=rsem, device_id=to, device_id_type=MESH
        )

    def chip_to(k):
        a, b = CHIP_STEPS[k]
        return lax.rem(yh + a, NH), lax.rem(x + b, NX)

    def chip_from(k):
        a, b = CHIP_STEPS[k]
        return lax.rem(yh + NH - a, NH) * NX + lax.rem(x + NX - b, NX)

    def seq_to(k):
        a, b = SEQ_STEPS[k]
        return lax.rem(yl + a, NY), lax.rem(z + b, NZ)

    def seq_from(k):
        a, b = SEQ_STEPS[k]
        return lax.rem(yl + NY - a, NY) * NZ + lax.rem(z + NZ - b, NZ)

    loads = [
        pltpu.make_async_copy(h, v, w_sem.at[i])
        for i, (h, v) in enumerate(((wq_hbm, wq), (wk_hbm, wk), (wv_hbm, wv), (wo_hbm, wo)))
    ]
    for cp in loads:
        cp.start()

    @pl.loop(0, NZ)
    def _(i):
        kv[i] = jnp.zeros((TOK, 2 * WIDTH), BF16)
        qdo[i] = jnp.zeros((TOK, 2 * WIDTH), BF16)
        do2[i] = jnp.zeros((TOK, WIDTH), BF16)

    bar = pltpu.get_barrier_semaphore()
    greet = [partner]
    for k in range(len(CHIP_STEPS)):
        a, b = chip_to(k)
        greet.append(dev(yh_=a, x_=b))
    for k in range(len(SEQ_STEPS)):
        a, b = seq_to(k)
        greet.append(dev(yl_=a, z_=b))
    for g in greet:
        pl.semaphore_signal(bar, inc=1, device_id=g, device_id_type=MESH)

    pt = point_ref[...].astype(F32)
    inv = lax.rsqrt(jnp.mean(pt * pt, axis=1, keepdims=True) + EPS)
    loc[0] = pt * inv
    loc[1] = inc_ref[...].astype(F32)
    irl[...] = jnp.broadcast_to(inv, (ROWS, 128))
    pl.semaphore_wait(bar, len(greet))

    swaps = [
        remote(loc.at[0, :, far_half], sc16.at[own_rows, :], d2s.at[0], d2r.at[0], partner),
        remote(loc.at[1, :, far_half], in16.at[own_rows, :], d2s.at[1], d2r.at[1], partner),
        remote(irl, ir16.at[own_rows, :], d2s.at[2], d2r.at[2], partner),
    ]
    for cp in swaps:
        cp.start()
    sc16[own_rows, :] = loc[0, :, own_half]
    in16[own_rows, :] = loc[1, :, own_half]
    ir16[own_rows, :] = irl[...]
    gain_half = gain_ref[:, own_half]
    for cp, buf in zip(swaps, (sc16, in16, ir16)):
        cp.wait_send()
    remote(loc.at[0, :, far_half], sc16.at[far_rows, :], d2s.at[0], d2r.at[0], partner).wait_recv()
    remote(loc.at[1, :, far_half], in16.at[far_rows, :], d2s.at[1], d2r.at[1], partner).wait_recv()
    remote(irl, ir16.at[far_rows, :], d2s.at[2], d2r.at[2], partner).wait_recv()

    def gather_sends(buf, g):
        mine = buf.at[chip, :, own_half]
        out = [remote(mine, mine, ags.at[g, 7], agr.at[g, 7], partner)]
        for k in range(7):
            a, b = chip_to(k)
            out.append(remote(mine, mine, ags.at[g, k], agr.at[g, k], dev(yh_=a, x_=b)))
        return out

    def gather_start(buf, g):
        for cp in gather_sends(buf, g):
            cp.start()

    def gather_finish(buf, g):
        forwards = []
        for k in range(7):
            slot = buf.at[chip_from(k), :, own_half]
            remote(slot, slot, ags.at[g, k], agr.at[g, k], partner).wait_recv()
            cp = remote(slot, slot, fws.at[g, k], fwr.at[g, k], partner)
            cp.start()
            forwards.append(cp)
        far = buf.at[chip, :, far_half]
        remote(far, far, ags.at[g, 7], agr.at[g, 7], partner).wait_recv()
        for k in range(7):
            far = buf.at[chip_from(k), :, far_half]
            remote(far, far, fws.at[g, k], fwr.at[g, k], partner).wait_recv()
        for cp in forwards + gather_sends(buf, g):
            cp.wait_send()

    agx[chip, :, own_half] = (gain_half * sc16[...]).astype(BF16)
    gather_start(agx, 0)
    agi[chip, :, own_half] = in16[...].astype(BF16)
    gather_start(agi, 1)

    row_tok = s * TOK + lax.broadcasted_iota(jnp.int32, (TOK, 1), 0)
    row_blk = row_tok // BLK
    blk_col = lax.broadcasted_iota(jnp.int32, (TOK, NBLK), 1)
    lay = lay_ref[...].astype(BF16)
    onehot = jnp.where(blk_col == row_blk, 1.0, 0.0).astype(BF16)
    chosen_q = jnp.where(blk_col < row_blk, dot(onehot, lay), 0.0).astype(BF16)
    chosen_k = jnp.where(blk_col > row_blk, dot(onehot, lay, NT), 0.0).astype(BF16)
    for part in range(2):
        plane = yl if part == 0 else 1 - yl
        col_blk = plane * (PLANE // BLK) + lax.broadcasted_iota(jnp.int32, (NBLK, PLANE), 1) // BLK
        spread = jnp.where(lax.broadcasted_iota(jnp.int32, (NBLK, PLANE), 0) == col_blk, 1.0, 0.0)
        spread = spread.astype(BF16)
        col_tok = plane * PLANE + lax.broadcasted_iota(jnp.int32, (1, PLANE), 1)
        same = row_blk == col_tok // BLK
        ok = (dot(chosen_q, spread) > 0.5) | (same & (col_tok <= row_tok))
        bq[part] = jnp.where(ok, 0.0, MASKED)
        ok = (dot(chosen_k, spread) > 0.5) | (same & (col_tok >= row_tok))
        bk[part] = jnp.where(ok, 0.0, MASKED)

    def turn(v, h, back=False):
        v = v[:, h * HEAD_DIM : (h + 1) * HEAD_DIM]
        turned = pltpu.roll(v, HEAD_DIM // 2, 1) * sin_ref[...]
        return v * cos_ref[...] - turned if back else v * cos_ref[...] + turned

    for cp in loads:
        cp.wait()
    gather_finish(agx, 0)

    feats = agx[...].reshape(TOK, D)
    key_f = dot(feats, wk[...])
    val_f = dot(feats, wv[...])
    for h in range(HEADS_DEV):
        kv[z, :, h * HEAD_DIM : (h + 1) * HEAD_DIM] = turn(key_f, h).astype(BF16)
    kv[z, :, WIDTH:] = val_f.astype(BF16)

    def depth(sgn):
        return NZ // 2 - c if sgn > 0 else NZ // 2 - 1 + c

    def wanted(stream, sgn, d, at):
        full = depth(sgn)
        near = d <= full
        if stream in (OTHER, OTHER2):
            return near if stream == OTHER else near & (yl == 0)
        origin = lax.rem(at - sgn * d + NZ, NZ)
        later = stream == KV
        if later == (sgn > 0):
            return near & ((at >= d) if sgn > 0 else (at + d <= NZ - 1))
        return near & ((origin + full >= NZ) if sgn > 0 else (origin < full))

    bufs = (kv, qdo, oth, do2, oth2)

    def hop(stream, sgn, d):
        block = bufs[stream].at[lax.rem(z - sgn * (d - 1) + NZ, NZ)]
        to = dev(z_=lax.rem(z + sgn + NZ, NZ))
        i = 0 if sgn > 0 else 1
        return remote(block, block, rgs.at[stream, i, d - 1], rgr.at[stream, i, d - 1], to)

    def send_hop(stream, sgn, d):
        @pl.when(wanted(stream, sgn, d, lax.rem(z + sgn + NZ, NZ)))
        def _():
            hop(stream, sgn, d).start()

    def sent_hop(stream, sgn, d):
        @pl.when(wanted(stream, sgn, d, lax.rem(z + sgn + NZ, NZ)))
        def _():
            hop(stream, sgn, d).wait_send()

    def take_hop(stream, sgn, d):
        @pl.when(wanted(stream, sgn, d, z))
        def _():
            block = bufs[stream].at[lax.rem(z - sgn * d + NZ, NZ)]
            i = 0 if sgn > 0 else 1
            to = dev(z_=lax.rem(z + sgn + NZ, NZ))
            remote(
                block, block, rgs.at[stream, i, d - 1], rgr.at[stream, i, d - 1], to
            ).wait_recv()

    def ring_start(stream):
        for sgn in (1, -1):
            send_hop(stream, sgn, 1)

    def ring_step(streams, d):
        for stream in streams:
            for sgn in (1, -1):
                take_hop(stream, sgn, d)
                if d < NZ // 2:
                    send_hop(stream, sgn, d + 1)

    def ring_sent(streams):
        for d in range(1, NZ // 2 + 1):
            for stream in streams:
                for sgn in (1, -1):
                    sent_hop(stream, sgn, d)

    across = dev(yl_=1 - yl)

    def cross(stream, i):
        dst = bufs[stream].at[z]
        return remote(dst, dst, yxs.at[i], yxr.at[i], across)

    def cross_from(src, stream, i):
        return remote(src.at[z], bufs[stream].at[z], yxs.at[i], yxr.at[i], across)

    @pl.when(yl == 0)
    def _():
        cross_from(kv, OTHER, 0).start()

    ring_start(KV)
    que_f = dot(feats, wq[...])
    for h in range(HEADS_DEV):
        qdo[z, :, h * HEAD_DIM : (h + 1) * HEAD_DIM] = turn(que_f, h).astype(BF16)
    gather_finish(agi, 1)
    qdo[z, :, WIDTH:] = dot(agi[...].reshape(TOK, D), wo[...], NT).astype(BF16)

    @pl.when(yl == 1)
    def _():
        cross_from(qdo, OTHER, 0).start()

    ring_start(QDO)
    cross(OTHER, 0).wait_recv()
    ring_start(OTHER)
    for d in range(1, NZ // 2 + 1):
        ring_step((KV, QDO, OTHER), d)

    def lanes(h, base=0):
        return pl.ds(base + h * HEAD_DIM, HEAD_DIM)

    def rows_of(buf, h, base=0):
        return buf[:, :, lanes(h, base)].reshape(PLANE, HEAD_DIM)

    def as_row(col):
        return jnp.transpose(jnp.broadcast_to(col, (TOK, TOK)))[0:1, :]

    def forward(parts):
        for h in range(HEADS_DEV):
            query = qdo[z, :, lanes(h)]
            top = None
            for i, buf in enumerate(parts):
                sc = dot(query, rows_of(buf, h), NT) * scale + bq[i]
                pq[h, i] = sc
                m = jnp.max(sc, axis=1, keepdims=True)
                top = m if top is None else jnp.maximum(top, m)
            total = None
            for i, buf in enumerate(parts):
                e = jnp.exp(pq[h, i] - top)
                pq[h, i] = e
                l = jnp.sum(e, axis=1, keepdims=True)
                total = l if total is None else total + l
            inv_total = 1.0 / total
            out = None
            for i, buf in enumerate(parts):
                p = pq[h, i] * inv_total
                pq[h, i] = p
                o = dot(p.astype(BF16), rows_of(buf, h, WIDTH))
                out = o if out is None else out + o
            out = out.astype(BF16)
            att[:, lanes(h)] = out
            grad = qdo[z, :, lanes(h, WIDTH)]
            st[0, s, pl.ds(h, 1), :] = as_row(top + jnp.log(total))
            st[0, s, pl.ds(2 + h, 1), :] = as_row(
                jnp.sum(grad.astype(F32) * out.astype(F32), axis=1, keepdims=True)
            )

    @pl.when(yl == 0)
    def _():
        forward((kv,))

    @pl.when(yl == 1)
    def _():
        forward((kv, oth))

    def stats_sends(it):
        out = []
        for k in range(len(SEQ_STEPS)):
            a, b = seq_to(k)
            mine = st.at[it, s]
            out.append(remote(mine, mine, sts.at[it, k], str_.at[it, k], dev(yl_=a, z_=b)))
        return out

    def stats_wait(it):
        for k in range(len(SEQ_STEPS)):
            slot = st.at[it, seq_from(k)]
            remote(slot, slot, sts.at[it, k], str_.at[it, k], partner).wait_recv()
        for cp in stats_sends(it):
            cp.wait_send()

    def own_grad(it, h):
        return qdo[z, :, lanes(h, WIDTH)] if it == 0 else do2[z, :, lanes(h)]

    def query_side(it, parts):
        for h in range(HEADS_DEV):
            grad = own_grad(it, h)
            delta = jnp.sum(
                grad.astype(F32) * att[:, lanes(h)].astype(F32), axis=1, keepdims=True
            )
            out = None
            for i, buf in enumerate(parts):
                gp = dot(grad, rows_of(buf, h, WIDTH), NT)
                gsc = (pq[h, i] * (gp - delta)).astype(BF16)
                o = dot(gsc, rows_of(buf, h))
                out = o if out is None else out + o
            out = jnp.concatenate([out] * HEADS_DEV, axis=1) * scale
            dqkv[0, :, lanes(h)] = turn(out, h, True).astype(BF16)

    def key_side(it, parts, planes):
        grads = ((qdo, WIDTH), (oth, WIDTH)) if it == 0 else ((do2, 0), (oth2, 0))
        for h in range(HEADS_DEV):
            key = kv[z, :, lanes(h)]
            value = kv[z, :, lanes(h, WIDTH)]
            gk, gv = None, None
            for i, buf in enumerate(parts):
                row = lambda n, r: jnp.concatenate(
                    [st[n, planes[i] * NZ + j, pl.ds(r, 1), :] for j in range(NZ)], axis=1
                )
                query = rows_of(buf, h)
                if it == 0:
                    p = jnp.exp(dot(key, query, NT) * scale + bk[i] - row(0, h))
                    pk[h, i] = p
                else:
                    p = pk[h, i]
                grad = rows_of(grads[i][0], h, grads[i][1])
                v = dot(p.astype(BF16), grad)
                gv = v if gv is None else gv + v
                gp = dot(value, grad, NT)
                gsc = (p * (gp - row(it, 2 + h))).astype(BF16)
                k = dot(gsc, query)
                gk = k if gk is None else gk + k
            gk = jnp.concatenate([gk] * HEADS_DEV, axis=1) * scale
            dqkv[1, :, lanes(h)] = turn(gk, h, True).astype(BF16)
            dqkv[2, :, lanes(h)] = gv.astype(BF16)

    def backward(it):
        @pl.when(yl == 0)
        def _():
            query_side(it, (kv,))

        @pl.when(yl == 1)
        def _():
            query_side(it, (kv, oth))

        stats_wait(it)

        @pl.when(yl == 0)
        def _():
            key_side(it, (qdo, oth), (yl, 1 - yl))

        @pl.when(yl == 1)
        def _():
            key_side(it, (qdo,), (yl,))

        dq, dk, dv = dqkv[0], dqkv[1], dqkv[2]
        step = 512

        def part_of(base, j):
            rows = pl.ds(pl.multiple_of(base + j * step, step), step)
            return (
                dot(dq, wq[rows, :], NT) + dot(dk, wk[rows, :], NT) + dot(dv, wv[rows, :], NT)
            )

        @pl.loop(0, HALF // step)
        def _(j):
            cols = pl.ds(pl.multiple_of(j * step, step), step)
            tot[it, :, :, cols] = (
                part_of((1 - c) * HALF, j).astype(BF16).reshape(CHIPS, CROWS, step)
            )

        give = remote(tot.at[it], drv.at[it], d2s.at[3 + it], d2r.at[3 + it], partner)
        give.start()

        @pl.loop(0, HALF // step)
        def _(j):
            cols = pl.ds(pl.multiple_of(j * step, step), step)
            totf[:, :, cols] = part_of(c * HALF, j).reshape(CHIPS, CROWS, step)

        give.wait_recv()
        sends = []
        for k in range(7):
            a, b = chip_to(k)
            other = a * NX + b
            rsrc[it, k] = (totf[other] + drv[it, other].astype(F32)).astype(BF16)
            cp = remote(
                rsrc.at[it, k], rrv.at[it, k], rss.at[it, k], rsr.at[it, k], dev(yh_=a, x_=b)
            )
            cp.start()
            sends.append(cp)
        gn[...] = totf[chip] + drv[it, chip].astype(F32)
        for k in range(7):
            sends[k].wait_recv()
            gn[...] += rrv[it, k].astype(F32)

        grad_normed = gn[...]
        scaled = sc16[...]
        term = jnp.sum(grad_normed * scaled, axis=0, keepdims=True)
        gacc[...] = term if it == 0 else gacc[...] + term
        weighted = gain_half * grad_normed
        inl[it] = jnp.broadcast_to(
            jnp.sum(weighted * scaled, axis=1, keepdims=True), (CROWS, 128)
        )
        share = remote(inl.at[it], inr.at[it], d2s.at[5 + it], d2r.at[5 + it], partner)
        share.start()
        share.wait_recv()
        inner = (inl[it] + inr[it])[:, 0:1]
        cot = ir16[:, 0:1] * (weighted - scaled * (inner / D))
        adj16[...] = (in16[...] if it == 0 else adj16[...]) + cot
        give.wait_send()
        share.wait_send()
        for cp in sends:
            cp.wait_send()
        return cot

    for cp in stats_sends(0):
        cp.start()
    cot = backward(0)

    agc[chip, :, own_half] = cot.astype(BF16)
    gather_start(agc, 2)
    ring_sent((KV, QDO, OTHER))
    cross(OTHER, 0).wait_send()
    gather_finish(agc, 2)
    do2[z] = dot(agc[...].reshape(TOK, D), wo[...], NT).astype(BF16)

    @pl.when(yl == 1)
    def _():
        cross_from(do2, OTHER2, 1).start()

    ring_start(DO2)
    for h in range(HEADS_DEV):
        st[1, s, pl.ds(2 + h, 1), :] = as_row(
            jnp.sum(
                do2[z, :, lanes(h)].astype(F32) * att[:, lanes(h)].astype(F32),
                axis=1,
                keepdims=True,
            )
        )
    for cp in stats_sends(1):
        cp.start()

    @pl.when(yl == 0)
    def _():
        cross(OTHER2, 1).wait_recv()

    ring_start(OTHER2)
    for d in range(1, NZ // 2 + 1):
        ring_step((DO2, OTHER2), d)
    backward(1)

    back = remote(adj16.at[far_rows, :], adjr, d2s.at[7], d2r.at[7], partner)
    back.start()
    gt[chip] = gacc[...]
    sends = []
    for k in range(7):
        a, b = chip_to(k)
        cp = remote(gt.at[chip], gt.at[chip], gts.at[k], gtr.at[k], dev(yh_=a, x_=b))
        cp.start()
        sends.append(cp)
    for k in range(7):
        slot = gt.at[chip_from(k)]
        remote(slot, slot, gts.at[k], gtr.at[k], partner).wait_recv()
    acc = gt[0]
    for i in range(1, CHIPS):
        acc = acc + gt[i]
    gs[s] = acc
    for k in range(len(SEQ_STEPS)):
        a, b = seq_to(k)
        cp = remote(gs.at[s], gs.at[s], gss.at[k], gsr.at[k], dev(yl_=a, z_=b))
        cp.start()
        sends.append(cp)
    adj_ref[:, own_half] = adj16[own_rows, :]
    back.wait_recv()
    adj_ref[:, far_half] = adjr[...]
    for k in range(len(SEQ_STEPS)):
        slot = gs.at[seq_from(k)]
        remote(slot, slot, gss.at[k], gsr.at[k], partner).wait_recv()
    acc = gs[0]
    for i in range(1, NY * NZ):
        acc = acc + gs[i]
    gh[0] = acc * (NY * NZ * TOK) ** (-0.5)
    last = remote(gh.at[0], gh.at[1], d2s.at[8], d2r.at[8], partner)
    last.start()
    gg_ref[:, own_half] = gh[0]
    last.wait_recv()
    gg_ref[:, far_half] = gh[1]

    ring_sent((DO2, OTHER2))

    @pl.when(yl == 1)
    def _():
        cross_from(do2, OTHER2, 1).wait_send()

    for cp in sends + [back, last]:
        cp.wait_send()


def scratch():
    v = pltpu.VMEM
    dma = pltpu.SemaphoreType.DMA
    return [
        v((D, WIDTH), BF16), v((D, WIDTH), BF16), v((D, WIDTH), BF16), v((WIDTH, D), BF16),
        v((2, ROWS, D), F32), v((CROWS, HALF), F32), v((CROWS, HALF), F32), v((CROWS, 128), F32),
        v((ROWS, 128), F32),
        v((CHIPS, CROWS, D), BF16), v((CHIPS, CROWS, D), BF16), v((CHIPS, CROWS, D), BF16),
        v((NZ, TOK, 2 * WIDTH), BF16), v((NZ, TOK, 2 * WIDTH), BF16), v((NZ, TOK, 2 * WIDTH), BF16),
        v((NZ, TOK, WIDTH), BF16), v((NZ, TOK, WIDTH), BF16),
        v((ITERS, NY * NZ, 8, TOK), F32),
        v((2, TOK, PLANE), F32), v((2, TOK, PLANE), F32),
        v((HEADS_DEV, 2, TOK, PLANE), F32), v((HEADS_DEV, 2, TOK, PLANE), F32),
        v((TOK, WIDTH), BF16), v((3, TOK, WIDTH), BF16),
        v((ITERS, CHIPS, CROWS, HALF), BF16), v((CHIPS, CROWS, HALF), F32),
        v((ITERS, CHIPS, CROWS, HALF), BF16), v((ITERS, 7, CROWS, HALF), BF16),
        v((ITERS, 7, CROWS, HALF), BF16), v((CROWS, HALF), F32),
        v((ITERS, CROWS, 128), F32), v((ITERS, CROWS, 128), F32),
        v((CROWS, HALF), F32), v((ROWS, HALF), F32), v((1, HALF), F32),
        v((CHIPS, 1, HALF), F32), v((NY * NZ, 1, HALF), F32), v((2, 1, HALF), F32),
        dma((4,)), dma((3, 8)), dma((3, 8)), dma((3, 7)), dma((3, 7)), dma((9,)), dma((9,)),
        dma((5, 2, 4)), dma((5, 2, 4)), dma((2,)), dma((2,)),
        dma((ITERS, 15)), dma((ITERS, 15)), dma((ITERS, 7)), dma((ITERS, 7)),
        dma((7,)), dma((7,)), dma((15,)), dma((15,)),
    ]


def body(
    fixed_point, incoming, norm_gain, query_weight, key_weight, value_weight, out_weight, layout
):
    seq_index = lax.axis_index(SEQ)
    positions = (seq_index * TOK + jnp.arange(TOK, dtype=jnp.int32)).astype(F32)
    freq = THETA ** (-jnp.arange(0, HEAD_DIM, 2, dtype=F32) / HEAD_DIM)
    angle = positions[:, None] * freq[None, :]
    cosine = jnp.concatenate([jnp.cos(angle), jnp.cos(angle)], axis=1)
    sine = jnp.concatenate([-jnp.sin(angle), jnp.sin(angle)], axis=1)
    vmem = pl.BlockSpec(memory_space=pltpu.VMEM)
    hbm = pl.BlockSpec(memory_space=pl.ANY)
    adjoint, gain = pl.pallas_call(
        kernel,
        out_shape=(
            jax.ShapeDtypeStruct((ROWS, D), F32),
            jax.ShapeDtypeStruct((1, D), F32),
        ),
        in_specs=[vmem] * 6 + [hbm] * 4,
        out_specs=(vmem, vmem),
        scratch_shapes=scratch(),
        compiler_params=pltpu.CompilerParams(
            collective_id=0, has_side_effects=True, vmem_limit_bytes=60 * 1024 * 1024
        ),
        name="deq_backward",
    )(
        fixed_point, incoming, norm_gain[None, :], cosine, sine, (layout > 0).astype(F32),
        query_weight, key_weight, value_weight, out_weight,
    )
    return adjoint, gain[0]


def solution(mesh):
    split = Mesh(mesh.devices.reshape(NY, NZ, NH, NX, NC), AXES)
    in_specs = (
        P(SEQ_TENSOR, None),
        P(SEQ_TENSOR, None),
        P(),
        P(None, TENSOR),
        P(None, TENSOR),
        P(None, TENSOR),
        P(TENSOR, None),
        P(),
    )
    out_specs = (P(SEQ_TENSOR, None), P())
    return jax.shard_map(body, mesh=split, in_specs=in_specs, out_specs=out_specs, check_vma=False)
```

```python
import functools

import jax
import jax.numpy as jnp
from jax import lax
from jax.experimental import pallas as pl
from jax.experimental.pallas import tpu as pltpu
from jax.sharding import Mesh
from jax.sharding import PartitionSpec as P

HEAD_DIM = 128
BLK = 64
ITERS = 2
EPS = 1e-05
THETA = 10000.0
MASKED = -1e30
AXES = ("seq_0", "seq_1", "tensor_0", "tensor_1", "tensor_2")
TENSOR = ("tensor_0", "tensor_1", "tensor_2")
SEQ = ("seq_0", "seq_1")
SEQ_TENSOR = AXES
MESH = pl.DeviceIdType.MESH
F32, BF16 = jnp.float32, jnp.bfloat16

NY, NZ, NH, NX, NC = 2, 8, 2, 4, 2
CHIPS = NH * NX
ROWS = 8
CROWS = NC * ROWS
TOK = CHIPS * CROWS
PLANE = NZ * TOK
D = 4096
HALF = D // 2
HEADS_DEV = 2
WIDTH = HEADS_DEV * HEAD_DIM
NBLK = 32

CHIP_STEPS = ((1, 2), (1, 1), (1, 3), (0, 2), (1, 0), (0, 1), (0, 3))
SEQ_STEPS = tuple(
    (a, b % NZ) for b in (4, 3, -3, 2, -2, 1, -1, 0) for a in (1, 0) if (a, b) != (0, 0)
)
K, V, Q, G, OA, GA, GB, OA2 = range(8)
CHUNKS = 2

NN = (((1,), (0,)), ((), ()))
NT = (((1,), (1,)), ((), ()))


def dot(a, b, dims=NN):
    return lax.dot_general(a, b, dims, preferred_element_type=F32)


def kernel(
    point_ref, inc_ref, gain_ref, freq_ref, lay_ref, wq_hbm, wk_hbm, wv_hbm, wo_hbm,
    adj_ref, gg_ref,
    wqkv, wo, wqkv_t, wo_t, cosb, sinb, loc, sc16, in16, ir16, irl, agx, agi, agc,
    kb, vb, qb, gb, oa, ob, ga2, gb2, oa2, ob2, st, bq, bk, pq, pk, att, dqkv,
    tot, drv, rsrc, rrv, pair, gn, inl, inr, adj16, adjr, gacc, gt, gs, gh,
    w_sem, ags, agr, fws, fwr, d2s, d2r, rgs, rgr, yxs, yxr, yfs, yfr, sts, str_,
    gvs, gvr, rss, rsr, gts, gtr, gss, gsr,
):
    yl, z, yh, x, c = (lax.axis_index(a) for a in AXES)
    chip = yh * NX + x
    s = yl * NZ + z
    scale = HEAD_DIM ** (-0.5)

    def dev(yl_=None, z_=None, yh_=None, x_=None, c_=None):
        pick = lambda a, b: a if b is None else b
        return (pick(yl, yl_), pick(z, z_), pick(yh, yh_), pick(x, x_), pick(c, c_))

    partner = dev(c_=1 - c)
    own_half = pl.ds(pl.multiple_of(c * HALF, HALF), HALF)
    far_half = pl.ds(pl.multiple_of((1 - c) * HALF, HALF), HALF)
    own_rows = pl.ds(pl.multiple_of(c * ROWS, ROWS), ROWS)
    far_rows = pl.ds(pl.multiple_of((1 - c) * ROWS, ROWS), ROWS)

    def remote(src, dst, ssem, rsem, to):
        return pltpu.make_async_remote_copy(
            src_ref=src, dst_ref=dst, send_sem=ssem, recv_sem=rsem, device_id=to, device_id_type=MESH
        )

    def chip_to(k):
        a, b = CHIP_STEPS[k]
        return lax.rem(yh + a, NH), lax.rem(x + b, NX)

    def chip_from(k):
        a, b = CHIP_STEPS[k]
        return lax.rem(yh + NH - a, NH) * NX + lax.rem(x + NX - b, NX)

    def seq_to(k):
        a, b = SEQ_STEPS[k]
        return lax.rem(yl + a, NY), lax.rem(z + b, NZ)

    def seq_from(k):
        a, b = SEQ_STEPS[k]
        return lax.rem(yl + NY - a, NY) * NZ + lax.rem(z + NZ - b, NZ)

    loads = [
        pltpu.make_async_copy(h, wqkv.at[:, pl.ds(i * WIDTH, WIDTH)], w_sem.at[i])
        for i, h in enumerate((wq_hbm, wk_hbm, wv_hbm))
    ]
    loads.append(pltpu.make_async_copy(wo_hbm, wo, w_sem.at[3]))
    for cp in loads:
        cp.start()

    @pl.loop(0, NZ)
    def _(i):
        for buf in (kb, vb, qb, gb):
            buf[i] = jnp.zeros((TOK, WIDTH), BF16)
        for buf in (ga2, gb2):
            buf[i] = jnp.zeros((TOK, HEAD_DIM), BF16)

    bar = pltpu.get_barrier_semaphore()
    greet = [partner]
    for k in range(len(CHIP_STEPS)):
        a, b = chip_to(k)
        greet.append(dev(yh_=a, x_=b))
    for k in range(len(SEQ_STEPS)):
        a, b = seq_to(k)
        greet.append(dev(yl_=a, z_=b))
    for g in greet:
        pl.semaphore_signal(bar, inc=1, device_id=g, device_id_type=MESH)

    pt = point_ref[...].astype(F32)
    inv = lax.rsqrt(jnp.mean(pt * pt, axis=1, keepdims=True) + EPS)
    loc[0] = pt * inv
    loc[1] = inc_ref[...].astype(F32)
    irl[...] = jnp.broadcast_to(inv, (ROWS, 128))
    pl.semaphore_wait(bar, len(greet))

    swaps = [
        remote(loc.at[0, :, far_half], sc16.at[own_rows, :], d2s.at[0], d2r.at[0], partner),
        remote(loc.at[1, :, far_half], in16.at[own_rows, :], d2s.at[1], d2r.at[1], partner),
        remote(irl, ir16.at[own_rows, :], d2s.at[2], d2r.at[2], partner),
    ]
    for cp in swaps:
        cp.start()
    sc16[own_rows, :] = loc[0, :, own_half]
    in16[own_rows, :] = loc[1, :, own_half]
    ir16[own_rows, :] = irl[...]
    gain_half = gain_ref[:, own_half]
    for cp, buf in zip(swaps, (sc16, in16, ir16)):
        cp.wait_send()
    remote(loc.at[0, :, far_half], sc16.at[far_rows, :], d2s.at[0], d2r.at[0], partner).wait_recv()
    remote(loc.at[1, :, far_half], in16.at[far_rows, :], d2s.at[1], d2r.at[1], partner).wait_recv()
    remote(irl, ir16.at[far_rows, :], d2s.at[2], d2r.at[2], partner).wait_recv()

    def gather_sends(buf, g):
        mine = buf.at[chip, :, own_half]
        out = [remote(mine, mine, ags.at[g, 7], agr.at[g, 7], partner)]
        for k in range(7):
            a, b = chip_to(k)
            out.append(remote(mine, mine, ags.at[g, k], agr.at[g, k], dev(yh_=a, x_=b)))
        return out

    def gather_start(buf, g):
        for cp in gather_sends(buf, g):
            cp.start()

    def gather_finish(buf, g):
        forwards = []
        for k in range(7):
            slot = buf.at[chip_from(k), :, own_half]
            remote(slot, slot, ags.at[g, k], agr.at[g, k], partner).wait_recv()
            cp = remote(slot, slot, fws.at[g, k], fwr.at[g, k], partner)
            cp.start()
            forwards.append(cp)
        far = buf.at[chip, :, far_half]
        remote(far, far, ags.at[g, 7], agr.at[g, 7], partner).wait_recv()
        for k in range(7):
            far = buf.at[chip_from(k), :, far_half]
            remote(far, far, fws.at[g, k], fwr.at[g, k], partner).wait_recv()
        for cp in forwards + gather_sends(buf, g):
            cp.wait_send()

    agx[chip, :, own_half] = (gain_half * sc16[...]).astype(BF16)
    gather_start(agx, 0)
    agi[chip, :, own_half] = in16[...].astype(BF16)
    gather_start(agi, 1)

    row_tok = s * TOK + lax.broadcasted_iota(jnp.int32, (TOK, 1), 0)
    row_blk = row_tok // BLK
    blk_col = lax.broadcasted_iota(jnp.int32, (TOK, NBLK), 1)
    lay = jnp.where(lay_ref[...] > 0, 1.0, 0.0).astype(BF16)
    onehot = jnp.where(blk_col == row_blk, 1.0, 0.0).astype(BF16)
    chosen_q = jnp.where(blk_col < row_blk, dot(onehot, lay), 0.0).astype(BF16)
    chosen_k = jnp.where(blk_col > row_blk, dot(onehot, lay, NT), 0.0).astype(BF16)
    for part in range(2):
        plane = yl if part == 0 else 1 - yl
        col_blk = plane * (PLANE // BLK) + lax.broadcasted_iota(jnp.int32, (NBLK, PLANE), 1) // BLK
        spread = jnp.where(lax.broadcasted_iota(jnp.int32, (NBLK, PLANE), 0) == col_blk, 1.0, 0.0)
        spread = spread.astype(BF16)
        col_tok = plane * PLANE + lax.broadcasted_iota(jnp.int32, (1, PLANE), 1)
        same = row_blk == col_tok // BLK
        ok = (dot(chosen_q, spread) > 0.5) | (same & (col_tok <= row_tok))
        bq[part] = jnp.where(ok, 0.0, MASKED)
        ok = (dot(chosen_k, spread) > 0.5) | (same & (col_tok >= row_tok))
        bk[part] = jnp.where(ok, 0.0, MASKED)

    angle = row_tok.astype(F32) * freq_ref[...]
    lower = lax.broadcasted_iota(jnp.int32, (TOK, HEAD_DIM), 1) < HEAD_DIM // 2
    cosb[...] = jnp.cos(angle)
    sine = jnp.sin(angle)
    sinb[...] = jnp.where(lower, -sine, sine)

    def turn(v, back=False):
        turned = pltpu.roll(v, HEAD_DIM // 2, 1) * sinb[...]
        return v * cosb[...] - turned if back else v * cosb[...] + turned

    for cp in loads:
        cp.wait()

    @pl.loop(0, D // 512)
    def _(j):
        rows = pl.ds(pl.multiple_of(j * 512, 512), 512)
        wqkv_t[:, rows] = jnp.transpose(wqkv[rows, :])
        wo_t[rows, :] = jnp.transpose(wo[:, rows])

    gather_finish(agx, 0)

    def depth(sgn):
        return NZ // 2 - c if sgn > 0 else NZ // 2 - 1 + c

    def wanted(stream, sgn, d, at):
        full = depth(sgn)
        near = d <= full
        if stream == OA:
            return near
        if stream == OA2:
            return near & (yl == 0)
        origin = lax.rem(at - sgn * d + NZ, NZ)
        if (stream in (K, V)) == (sgn > 0):
            some = (at >= d) if sgn > 0 else (at + d <= NZ - 1)
        else:
            some = (origin + full >= NZ) if sgn > 0 else (origin < full)
        if stream == V:
            some = some | (yl == 0)
        if stream in (G, GB):
            some = some | (yl == 1)
        return near & some

    bufs = (kb, vb, qb, gb, oa, ga2, gb2, oa2)

    def hop(stream, sgn, d, at):
        block = bufs[stream].at[lax.rem(at - sgn * (d - 1) + NZ, NZ)]
        to = dev(z_=lax.rem(z + sgn + NZ, NZ))
        i = 0 if sgn > 0 else 1
        return remote(block, block, rgs.at[stream, i, d - 1], rgr.at[stream, i, d - 1], to)

    def send_hop(stream, sgn, d):
        @pl.when(wanted(stream, sgn, d, lax.rem(z + sgn + NZ, NZ)))
        def _():
            hop(stream, sgn, d, z).start()

    across = dev(yl_=1 - yl)

    def over(stream, origin):
        dst, n = (ob2, 1) if stream == GB else (ob, 0)
        return remote(
            bufs[stream].at[origin], dst.at[origin], yfs.at[n, origin], yfr.at[n, origin], across
        )

    def send_over(stream, origin):
        @pl.when(yl == (0 if stream == V else 1))
        def _():
            over(stream, origin).start()

    def take_hop(stream, sgn, d):
        @pl.when(wanted(stream, sgn, d, z))
        def _():
            hop(stream, sgn, d, lax.rem(z - sgn + NZ, NZ)).wait_recv()
            if stream in (V, G, GB):
                send_over(stream, lax.rem(z - sgn * d + NZ, NZ))

    def ring_start(stream):
        for sgn in (1, -1):
            send_hop(stream, sgn, 1)
        if stream in (V, G, GB):
            send_over(stream, z)

    def ring_step(d, *streams):
        for stream in streams:
            for sgn in (1, -1):
                take_hop(stream, sgn, d)
                if d < NZ // 2:
                    send_hop(stream, sgn, d + 1)

    def ring_sent(*streams):
        for stream in streams:
            for d in range(1, NZ // 2 + 1):
                for sgn in (1, -1):

                    @pl.when(wanted(stream, sgn, d, lax.rem(z + sgn + NZ, NZ)))
                    def _():
                        hop(stream, sgn, d, z).wait_send()

            if stream in (V, G, GB):

                @pl.when(yl == (0 if stream == V else 1))
                def _():
                    for i in range(NZ):
                        over(stream, i).wait_send()

    def over_wait(n):
        buf = ob2 if n else ob
        for i in range(NZ):
            remote(buf.at[i], buf.at[i], yfs.at[n, i], yfr.at[n, i], across).wait_recv()

    def cross(src, dst, i):
        return remote(src.at[z], dst.at[z], yxs.at[i], yxr.at[i], across)

    def project(i):
        return dot(agx[...].reshape(TOK, D), wqkv[:, i * WIDTH : (i + 1) * WIDTH])

    def turned_into(buf, v):
        for h in range(HEADS_DEV):
            buf[z, :, h * HEAD_DIM : (h + 1) * HEAD_DIM] = turn(
                v[:, h * HEAD_DIM : (h + 1) * HEAD_DIM]
            ).astype(BF16)

    turned_into(kb, project(1))

    @pl.when(yl == 0)
    def _():
        cross(kb, oa, 0).start()

    ring_start(K)
    vb[z] = project(2).astype(BF16)
    ring_start(V)
    turned_into(qb, project(0))

    @pl.when(yl == 1)
    def _():
        cross(qb, oa, 0).start()

    ring_start(Q)
    ring_step(1, K, V)
    cross(oa, oa, 0).wait_recv()
    ring_start(OA)
    gather_finish(agi, 1)
    gb[z] = dot(agi[...].reshape(TOK, D), wo_t[...]).astype(BF16)
    ring_start(G)
    ring_step(1, Q, OA)
    ring_step(2, K, V)
    ring_step(2, Q, OA)
    ring_step(1, G)
    ring_step(3, K, V)
    ring_step(3, Q, OA)
    ring_step(2, G)
    ring_step(4, K, V)
    ring_step(4, Q, OA)
    ring_step(3, G)
    @pl.when(yl == 1)
    def _():
        over_wait(0)

    def lanes(h):
        return pl.ds(h * HEAD_DIM, HEAD_DIM)

    def rows_of(buf, h):
        return buf[:, :, lanes(h)].reshape(PLANE, HEAD_DIM)

    def as_row(col):
        return jnp.transpose(jnp.broadcast_to(col, (TOK, TOK)))[0:1, :]

    def forward(parts):
        for h in range(HEADS_DEV):
            query = qb[z, :, lanes(h)]
            top = None
            for i, (buf, _) in enumerate(parts):
                sc = dot(query, rows_of(buf, h), NT) * scale + bq[i]
                pq[h, i] = sc
                m = jnp.max(sc, axis=1, keepdims=True)
                top = m if top is None else jnp.maximum(top, m)
            total = None
            for i in range(len(parts)):
                e = jnp.exp(pq[h, i] - top)
                pq[h, i] = e
                l = jnp.sum(e, axis=1, keepdims=True)
                total = l if total is None else total + l
            inv_total = 1.0 / total
            out = None
            for i, (_, buf) in enumerate(parts):
                p = pq[h, i] * inv_total
                pq[h, i] = p
                o = dot(p.astype(BF16), rows_of(buf, h))
                out = o if out is None else out + o
            out = out.astype(BF16)
            att[:, lanes(h)] = out
            grad = gb[z, :, lanes(h)]
            st[0, s, pl.ds(h, 1), :] = as_row(top + jnp.log(total))
            st[0, s, pl.ds(2 + h, 1), :] = as_row(
                jnp.sum(grad.astype(F32) * out.astype(F32), axis=1, keepdims=True)
            )

    @pl.when(yl == 0)
    def _():
        forward(((kb, vb),))

    @pl.when(yl == 1)
    def _():
        forward(((kb, vb), (oa, ob)))

    def stats_sends(it):
        out = []
        for k in range(len(SEQ_STEPS)):
            a, b = seq_to(k)
            mine = st.at[it, s]
            out.append(remote(mine, mine, sts.at[it, k], str_.at[it, k], dev(yl_=a, z_=b)))
        return out

    def stats_wait(it):
        for k in range(len(SEQ_STEPS)):
            slot = st.at[it, seq_from(k)]
            remote(slot, slot, sts.at[it, k], str_.at[it, k], partner).wait_recv()
        for cp in stats_sends(it):
            cp.wait_send()

    def own_grad(it, h):
        return gb[z, :, lanes(h)] if it == 0 else (ga2, gb2)[h][z]

    def query_side(it, parts):
        for h in range(HEADS_DEV):
            grad = own_grad(it, h)
            delta = jnp.sum(
                grad.astype(F32) * att[:, lanes(h)].astype(F32), axis=1, keepdims=True
            )
            out = None
            for i, (keys, values) in enumerate(parts):
                gp = dot(grad, rows_of(values, h), NT)
                gsc = (pq[h, i] * (gp - delta)).astype(BF16)
                o = dot(gsc, rows_of(keys, h))
                out = o if out is None else out + o
            dqkv[:, lanes(h)] = turn(out * scale, True).astype(BF16)

    def key_side(it, parts, planes):
        for h in range(HEADS_DEV):
            key = kb[z, :, lanes(h)]
            value = vb[z, :, lanes(h)]
            gk, gv = None, None
            for i, (queries, grads, late) in enumerate(parts):
                row = lambda n, r: jnp.concatenate(
                    [st[n, planes[i] * NZ + j, pl.ds(r, 1), :] for j in range(NZ)], axis=1
                )
                query = rows_of(queries, h)
                if it == 0:
                    p = jnp.exp(dot(key, query, NT) * scale + bk[i] - row(0, h))
                    pk[h, i] = p
                    grad = rows_of(grads, h)
                else:
                    p = pk[h, i]
                    grad = late[h][...].reshape(PLANE, HEAD_DIM)
                v = dot(p.astype(BF16), grad)
                gv = v if gv is None else gv + v
                gp = dot(value, grad, NT)
                gsc = (p * (gp - row(it, 2 + h))).astype(BF16)
                k = dot(gsc, query)
                gk = k if gk is None else gk + k
            dqkv[:, lanes(HEADS_DEV + h)] = turn(gk * scale, True).astype(BF16)
            dqkv[:, lanes(2 * HEADS_DEV + h)] = gv.astype(BF16)

    def backward(it):
        @pl.when(yl == 0)
        def _():
            query_side(it, ((kb, vb),))

        @pl.when(yl == 1)
        def _():
            query_side(it, ((kb, vb), (oa, ob)))

        stats_wait(it)

        @pl.when(yl == 0)
        def _():
            over_wait(it)

        @pl.when(yl == 0)
        def _():
            key_side(it, ((qb, gb, (ga2, gb2)), (oa, ob, (oa2, ob2))), (yl, 1 - yl))

        @pl.when(yl == 1)
        def _():
            key_side(it, ((qb, gb, (ga2, gb2)),), (yl,))

        wide = HALF // CHUNKS
        gives = []
        for j in range(CHUNKS):
            cols = pl.ds(pl.multiple_of((1 - c) * HALF + j * wide, wide), wide)
            tot[it, j] = dot(dqkv[...], wqkv_t[:, cols]).astype(BF16).reshape(CHIPS, CROWS, wide)
            cp = remote(tot.at[it, j], drv.at[it, j], gvs.at[it, j], gvr.at[it, j], partner)
            cp.start()
            gives.append(cp)
        sends = []
        for j in range(CHUNKS):
            cols = pl.ds(pl.multiple_of(c * HALF + j * wide, wide), wide)
            mine = dot(dqkv[...], wqkv_t[:, cols]).reshape(CHIPS, CROWS, wide)
            gives[j].wait_recv()
            pair[...] = mine + drv[it, j].astype(F32)
            for k in range(7):
                a, b = chip_to(k)
                rsrc[it, j, k] = pair[a * NX + b].astype(BF16)
                cp = remote(
                    rsrc.at[it, j, k], rrv.at[it, j, k], rss.at[it, j, k], rsr.at[it, j, k],
                    dev(yh_=a, x_=b),
                )
                cp.start()
                sends.append(cp)
            here = pl.ds(j * wide, wide)
            gn[:, here] = pair[chip]
            term = jnp.sum(
                (pair[...] * agx[:, :, cols].astype(F32)).reshape(TOK, wide), axis=0, keepdims=True
            )
            gacc[:, here] = term if it == 0 else gacc[:, here] + term
        if it == ITERS - 1:
            gt[chip] = gacc[...]
            sends.extend(gain_chip_sends())
            for cp in gain_chip_sends():
                cp.start()
            for k in range(7):
                slot = gt.at[chip_from(k)]
                remote(slot, slot, gts.at[k], gtr.at[k], partner).wait_recv()
            acc = gt[0]
            for i in range(1, CHIPS):
                acc = acc + gt[i]
            gs[s] = acc
            sends.extend(gain_seq_sends())
            for cp in gain_seq_sends():
                cp.start()
        for j in range(CHUNKS):
            here = pl.ds(j * wide, wide)
            for k in range(7):
                sends[7 * j + k].wait_recv()
                gn[:, here] += rrv[it, j, k].astype(F32)

        grad_normed = gn[...]
        scaled = sc16[...]
        weighted = gain_half * grad_normed
        inl[it] = jnp.broadcast_to(
            jnp.sum(weighted * scaled, axis=1, keepdims=True), (CROWS, 128)
        )
        share = remote(inl.at[it], inr.at[it], d2s.at[5 + it], d2r.at[5 + it], partner)
        share.start()
        share.wait_recv()
        inner = (inl[it] + inr[it])[:, 0:1]
        cot = ir16[:, 0:1] * (weighted - scaled * (inner / D))
        adj16[...] = (in16[...] if it == 0 else adj16[...]) + cot
        if it == 0:
            agc[chip, :, own_half] = cot.astype(BF16)
            gather_start(agc, 2)
        for cp in gives + [share] + sends:
            cp.wait_send()

    def gain_chip_sends():
        out = []
        for k in range(7):
            a, b = chip_to(k)
            out.append(
                remote(gt.at[chip], gt.at[chip], gts.at[k], gtr.at[k], dev(yh_=a, x_=b))
            )
        return out

    def gain_seq_sends():
        out = []
        for k in range(len(SEQ_STEPS)):
            a, b = seq_to(k)
            out.append(remote(gs.at[s], gs.at[s], gss.at[k], gsr.at[k], dev(yl_=a, z_=b)))
        return out

    for cp in stats_sends(0):
        cp.start()
    ring_step(4, G)
    backward(0)

    ring_sent(K, V, Q, G, OA)

    @pl.when(yl == 0)
    def _():
        cross(kb, oa, 0).wait_send()

    @pl.when(yl == 1)
    def _():
        cross(qb, oa, 0).wait_send()

    gather_finish(agc, 2)
    grad2 = dot(agc[...].reshape(TOK, D), wo_t[...]).astype(BF16)
    ga2[z] = grad2[:, :HEAD_DIM]
    gb2[z] = grad2[:, HEAD_DIM:]

    @pl.when(yl == 1)
    def _():
        cross(ga2, oa2, 1).start()

    ring_start(GB)
    ring_start(GA)
    for h in range(HEADS_DEV):
        st[1, s, pl.ds(2 + h, 1), :] = as_row(
            jnp.sum(
                own_grad(1, h).astype(F32) * att[:, lanes(h)].astype(F32), axis=1, keepdims=True
            )
        )
    for cp in stats_sends(1):
        cp.start()
    ring_step(1, GB)

    @pl.when(yl == 0)
    def _():
        cross(oa2, oa2, 1).wait_recv()

    ring_start(OA2)
    ring_step(1, GA)
    ring_step(2, GB)
    ring_step(1, OA2)
    ring_step(2, GA)
    ring_step(3, GB)
    ring_step(2, OA2)
    ring_step(3, GA)
    ring_step(4, GB)
    ring_step(3, OA2)
    ring_step(4, GA)
    ring_step(4, OA2)
    backward(1)

    back = remote(adj16.at[far_rows, :], adjr, d2s.at[7], d2r.at[7], partner)
    back.start()
    adj_ref[:, own_half] = adj16[own_rows, :]
    for k in range(len(SEQ_STEPS)):
        slot = gs.at[seq_from(k)]
        remote(slot, slot, gss.at[k], gsr.at[k], partner).wait_recv()
    acc = gs[0]
    for i in range(1, NY * NZ):
        acc = acc + gs[i]
    gh[0] = acc / gain_half * (NY * NZ * TOK) ** (-0.5)
    last = remote(gh.at[0], gh.at[1], d2s.at[8], d2r.at[8], partner)
    last.start()
    back.wait_recv()
    adj_ref[:, far_half] = adjr[...]
    gg_ref[:, own_half] = gh[0]
    last.wait_recv()
    gg_ref[:, far_half] = gh[1]
    ring_sent(GA, GB, OA2)

    @pl.when(yl == 1)
    def _():
        cross(ga2, oa2, 1).wait_send()

    for cp in [back, last]:
        cp.wait_send()


def scratch():
    v = pltpu.VMEM
    dma = pltpu.SemaphoreType.DMA
    wide = HALF // CHUNKS
    block = (NZ, TOK, WIDTH)
    half_block = (NZ, TOK, HEAD_DIM)
    return [
        v((D, 3 * WIDTH), BF16), v((WIDTH, D), BF16), v((3 * WIDTH, D), BF16), v((D, WIDTH), BF16),
        v((TOK, HEAD_DIM), F32), v((TOK, HEAD_DIM), F32),
        v((2, ROWS, D), F32), v((CROWS, HALF), F32), v((CROWS, HALF), F32), v((CROWS, 128), F32),
        v((ROWS, 128), F32),
        v((CHIPS, CROWS, D), BF16), v((CHIPS, CROWS, D), BF16), v((CHIPS, CROWS, D), BF16),
        v(block, BF16), v(block, BF16), v(block, BF16), v(block, BF16), v(block, BF16),
        v(block, BF16),
        v(half_block, BF16), v(half_block, BF16), v(half_block, BF16), v(half_block, BF16),
        v((ITERS, NY * NZ, 8, TOK), F32),
        v((2, TOK, PLANE), F32), v((2, TOK, PLANE), F32),
        v((HEADS_DEV, 2, TOK, PLANE), F32), v((HEADS_DEV, 2, TOK, PLANE), F32),
        v((TOK, WIDTH), BF16), v((TOK, 3 * WIDTH), BF16),
        v((ITERS, CHUNKS, CHIPS, CROWS, wide), BF16), v((ITERS, CHUNKS, CHIPS, CROWS, wide), BF16),
        v((ITERS, CHUNKS, 7, CROWS, wide), BF16), v((ITERS, CHUNKS, 7, CROWS, wide), BF16),
        v((CHIPS, CROWS, wide), F32), v((CROWS, HALF), F32),
        v((ITERS, CROWS, 128), F32), v((ITERS, CROWS, 128), F32),
        v((CROWS, HALF), F32), v((ROWS, HALF), F32), v((1, HALF), F32),
        v((CHIPS, 1, HALF), F32), v((NY * NZ, 1, HALF), F32), v((2, 1, HALF), F32),
        dma((4,)), dma((3, 8)), dma((3, 8)), dma((3, 7)), dma((3, 7)), dma((9,)), dma((9,)),
        dma((8, 2, 4)), dma((8, 2, 4)), dma((2,)), dma((2,)), dma((2, NZ)), dma((2, NZ)),
        dma((ITERS, 15)), dma((ITERS, 15)), dma((ITERS, CHUNKS)), dma((ITERS, CHUNKS)),
        dma((ITERS, CHUNKS, 7)), dma((ITERS, CHUNKS, 7)),
        dma((7,)), dma((7,)), dma((15,)), dma((15,)),
    ]


def body(
    fixed_point, incoming, norm_gain, query_weight, key_weight, value_weight, out_weight, layout
):
    pair = lax.rem(jnp.arange(HEAD_DIM, dtype=jnp.int32), HEAD_DIM // 2).astype(F32)
    freq = THETA ** (-2.0 * pair / HEAD_DIM)
    vmem = pl.BlockSpec(memory_space=pltpu.VMEM)
    hbm = pl.BlockSpec(memory_space=pl.ANY)
    adjoint, gain = pl.pallas_call(
        kernel,
        out_shape=(
            jax.ShapeDtypeStruct((ROWS, D), F32),
            jax.ShapeDtypeStruct((1, D), F32),
        ),
        in_specs=[vmem] * 5 + [hbm] * 4,
        out_specs=(vmem, vmem),
        scratch_shapes=scratch(),
        compiler_params=pltpu.CompilerParams(
            collective_id=0, has_side_effects=True, vmem_limit_bytes=62 * 1024 * 1024
        ),
        name="deq_backward",
    )(
        fixed_point, incoming, norm_gain[None, :], freq[None, :], layout,
        query_weight, key_weight, value_weight, out_weight,
    )
    return adjoint, gain[0]


def solution(mesh):
    split = Mesh(mesh.devices.reshape(NY, NZ, NH, NX, NC), AXES)
    in_specs = (
        P(SEQ_TENSOR, None),
        P(SEQ_TENSOR, None),
        P(),
        P(None, TENSOR),
        P(None, TENSOR),
        P(None, TENSOR),
        P(TENSOR, None),
        P(),
    )
    out_specs = (P(SEQ_TENSOR, None), P())
    return jax.shard_map(body, mesh=split, in_specs=in_specs, out_specs=out_specs, check_vma=False)
```

```python
import functools

import jax
import jax.numpy as jnp
import numpy as np
from jax import lax
from jax.experimental import pallas as pl
from jax.experimental.pallas import tpu as pltpu
from jax.sharding import Mesh
from jax.sharding import PartitionSpec as P

HEAD_DIM = 128
BLK = 64
ITERS = 2
EPS = 1e-05
THETA = 10000.0
MASKED = -1e30
AXES = ("seq_0", "seq_1", "tensor_0", "tensor_1", "tensor_2")
TENSOR = ("tensor_0", "tensor_1", "tensor_2")
SEQ = ("seq_0", "seq_1")
SEQ_TENSOR = AXES
MESH = pl.DeviceIdType.MESH
F32, BF16 = jnp.float32, jnp.bfloat16

NY, NZ, NH, NX, NC = 2, 8, 2, 4, 2
CHIPS = NH * NX
ROWS = 8
CROWS = NC * ROWS
TOK = CHIPS * CROWS
PLANE = NZ * TOK
D = 4096
HALF = D // 2
HEADS_DEV = 2
WIDTH = HEADS_DEV * HEAD_DIM
NBLK = 32

CHIP_STEPS = ((1, 2), (1, 1), (1, 3), (0, 2), (1, 0), (0, 1), (0, 3))
SEQ_STEPS = tuple(
    (a, b % NZ) for b in (4, 3, -3, 2, -2, 1, -1, 0) for a in (1, 0) if (a, b) != (0, 0)
)
K, V, Q, G, OA, GA, GB, OA2 = range(8)
CHUNKS = 2

NN = (((1,), (0,)), ((), ()))
NT = (((1,), (1,)), ((), ()))


def dot(a, b, dims=NN):
    return lax.dot_general(a, b, dims, preferred_element_type=F32)


def kernel(
    point_hbm, inc_hbm, gain_hbm, freq_hbm, lay_hbm, wq_hbm, wk_hbm, wv_hbm, wo_hbm,
    adj_ref, gg_ref,
    point_ref, inc_ref, gain_ref, freq_ref, lay_ref,
    wqkv, wo, wqkv_t, wo_t, cosb, sinb, loc, sc16, in16, ir16, irl, agx, agi, agc,
    kb, vb, qb, gb, oa, ob, ga2, gb2, oa2, ob2, st, bq, bk, pq, pk, att, dqkv,
    tot, drv, rsrc, rrv, pair, gn, inl, inr, adj16, adjr, gacc, gt, gs, gh,
    in_sem, w_sem, ags, agr, fws, fwr, d2s, d2r, rgs, rgr, yxs, yxr, yfs, yfr, sts, str_,
    gvs, gvr, rss, rsr, gts, gtr, gss, gsr,
):
    yl, z, yh, x, c = (lax.axis_index(a) for a in AXES)
    chip = yh * NX + x
    s = yl * NZ + z
    scale = HEAD_DIM ** (-0.5)

    def dev(yl_=None, z_=None, yh_=None, x_=None, c_=None):
        pick = lambda a, b: a if b is None else b
        return (pick(yl, yl_), pick(z, z_), pick(yh, yh_), pick(x, x_), pick(c, c_))

    partner = dev(c_=1 - c)
    sent = []
    own_half = pl.ds(pl.multiple_of(c * HALF, HALF), HALF)
    far_half = pl.ds(pl.multiple_of((1 - c) * HALF, HALF), HALF)
    own_rows = pl.ds(pl.multiple_of(c * ROWS, ROWS), ROWS)
    far_rows = pl.ds(pl.multiple_of((1 - c) * ROWS, ROWS), ROWS)

    def remote(src, dst, ssem, rsem, to):
        return pltpu.make_async_remote_copy(
            src_ref=src, dst_ref=dst, send_sem=ssem, recv_sem=rsem, device_id=to, device_id_type=MESH
        )

    def chip_to(k):
        a, b = CHIP_STEPS[k]
        return lax.rem(yh + a, NH), lax.rem(x + b, NX)

    def chip_from(k):
        a, b = CHIP_STEPS[k]
        return lax.rem(yh + NH - a, NH) * NX + lax.rem(x + NX - b, NX)

    def seq_to(k):
        a, b = SEQ_STEPS[k]
        return lax.rem(yl + a, NY), lax.rem(z + b, NZ)

    def seq_from(k):
        a, b = SEQ_STEPS[k]
        return lax.rem(yl + NY - a, NY) * NZ + lax.rem(z + NZ - b, NZ)

    small = [
        pltpu.make_async_copy(h, v, in_sem.at[i])
        for i, (h, v) in enumerate(
            ((point_hbm, point_ref), (inc_hbm, inc_ref), (gain_hbm, gain_ref),
             (freq_hbm, freq_ref), (lay_hbm, lay_ref))
        )
    ]
    for cp in small:
        cp.start()
    loads = [
        pltpu.make_async_copy(h, wqkv.at[:, pl.ds(i * WIDTH, WIDTH)], w_sem.at[i])
        for i, h in enumerate((wq_hbm, wk_hbm, wv_hbm))
    ]
    loads.append(pltpu.make_async_copy(wo_hbm, wo, w_sem.at[3]))
    for cp in loads:
        cp.start()

    @pl.loop(0, NZ)
    def _(i):
        for buf in (kb, vb, qb, gb):
            buf[i] = jnp.zeros((TOK, WIDTH), BF16)
        for buf in (ga2, gb2):
            buf[i] = jnp.zeros((TOK, HEAD_DIM), BF16)

    bar = pltpu.get_barrier_semaphore()
    greet = [partner]
    for k in range(len(CHIP_STEPS)):
        a, b = chip_to(k)
        greet.append(dev(yh_=a, x_=b))
    for k in range(len(SEQ_STEPS)):
        a, b = seq_to(k)
        greet.append(dev(yl_=a, z_=b))
    for g in greet:
        pl.semaphore_signal(bar, inc=1, device_id=g, device_id_type=MESH)

    for cp in small:
        cp.wait()
    pt = point_ref[...].astype(F32)
    inv = lax.rsqrt(jnp.mean(pt * pt, axis=1, keepdims=True) + EPS)
    loc[0] = pt * inv
    loc[1] = inc_ref[...].astype(F32)
    irl[...] = jnp.broadcast_to(inv, (ROWS, 128))
    pl.semaphore_wait(bar, len(greet))

    swaps = [
        remote(loc.at[0, :, far_half], sc16.at[own_rows, :], d2s.at[0], d2r.at[0], partner),
        remote(loc.at[1, :, far_half], in16.at[own_rows, :], d2s.at[1], d2r.at[1], partner),
        remote(irl, ir16.at[own_rows, :], d2s.at[2], d2r.at[2], partner),
    ]
    for cp in swaps:
        cp.start()
    sc16[own_rows, :] = loc[0, :, own_half]
    in16[own_rows, :] = loc[1, :, own_half]
    ir16[own_rows, :] = irl[...]
    gain_half = gain_ref[:, own_half]
    for cp, buf in zip(swaps, (sc16, in16, ir16)):
        cp.wait_send()
    remote(loc.at[0, :, far_half], sc16.at[far_rows, :], d2s.at[0], d2r.at[0], partner).wait_recv()
    remote(loc.at[1, :, far_half], in16.at[far_rows, :], d2s.at[1], d2r.at[1], partner).wait_recv()
    remote(irl, ir16.at[far_rows, :], d2s.at[2], d2r.at[2], partner).wait_recv()

    def gather_sends(buf, g):
        mine = buf.at[chip, :, own_half]
        out = [remote(mine, mine, ags.at[g, 7], agr.at[g, 7], partner)]
        for k in range(7):
            a, b = chip_to(k)
            out.append(remote(mine, mine, ags.at[g, k], agr.at[g, k], dev(yh_=a, x_=b)))
        return out

    def gather_start(buf, g):
        for cp in gather_sends(buf, g):
            cp.start()

    def gather_pass(buf, g):
        for k in range(7):
            slot = buf.at[chip_from(k), :, own_half]
            remote(slot, slot, ags.at[g, k], agr.at[g, k], partner).wait_recv()
            remote(slot, slot, fws.at[g, k], fwr.at[g, k], partner).start()

    def gather_finish(buf, g):
        far = buf.at[chip, :, far_half]
        remote(far, far, ags.at[g, 7], agr.at[g, 7], partner).wait_recv()
        for k in range(7):
            far = buf.at[chip_from(k), :, far_half]
            remote(far, far, fws.at[g, k], fwr.at[g, k], partner).wait_recv()

    def gather_sent(buf, g):
        for k in range(7):
            slot = buf.at[chip_from(k), :, own_half]
            remote(slot, slot, fws.at[g, k], fwr.at[g, k], partner).wait_send()
        for cp in gather_sends(buf, g):
            cp.wait_send()

    agx[chip, :, own_half] = (gain_half * sc16[...]).astype(BF16)
    gather_start(agx, 0)
    agi[chip, :, own_half] = in16[...].astype(BF16)
    gather_start(agi, 1)

    row_tok = s * TOK + lax.broadcasted_iota(jnp.int32, (TOK, 1), 0)
    row_blk = row_tok // BLK
    blk_col = lax.broadcasted_iota(jnp.int32, (TOK, NBLK), 1)
    lay = jnp.where(lay_ref[...] > 0, 1.0, 0.0).astype(BF16)
    onehot = jnp.where(blk_col == row_blk, 1.0, 0.0).astype(BF16)
    chosen_q = jnp.where(blk_col < row_blk, dot(onehot, lay), 0.0).astype(BF16)
    chosen_k = jnp.where(blk_col > row_blk, dot(onehot, lay, NT), 0.0).astype(BF16)
    for part in range(2):
        plane = yl if part == 0 else 1 - yl
        col_blk = plane * (PLANE // BLK) + lax.broadcasted_iota(jnp.int32, (NBLK, PLANE), 1) // BLK
        spread = jnp.where(lax.broadcasted_iota(jnp.int32, (NBLK, PLANE), 0) == col_blk, 1.0, 0.0)
        spread = spread.astype(BF16)
        col_tok = plane * PLANE + lax.broadcasted_iota(jnp.int32, (1, PLANE), 1)
        same = row_blk == col_tok // BLK
        ok = (dot(chosen_q, spread) > 0.5) | (same & (col_tok <= row_tok))
        bq[part] = jnp.where(ok, 0.0, MASKED)
        ok = (dot(chosen_k, spread) > 0.5) | (same & (col_tok >= row_tok))
        bk[part] = jnp.where(ok, 0.0, MASKED)

    angle = row_tok.astype(F32) * freq_ref[...]
    lower = lax.broadcasted_iota(jnp.int32, (TOK, HEAD_DIM), 1) < HEAD_DIM // 2
    cosb[...] = jnp.cos(angle)
    sine = jnp.sin(angle)
    sinb[...] = jnp.where(lower, -sine, sine)

    def turn(v, back=False):
        turned = pltpu.roll(v, HEAD_DIM // 2, 1) * sinb[...]
        return v * cosb[...] - turned if back else v * cosb[...] + turned

    for cp in loads:
        cp.wait()

    @pl.loop(0, D // 512)
    def _(j):
        rows = pl.ds(pl.multiple_of(j * 512, 512), 512)
        wqkv_t[:, rows] = jnp.transpose(wqkv[rows, :])
        wo_t[rows, :] = jnp.transpose(wo[:, rows])

    gather_pass(agx, 0)
    gather_finish(agx, 0)

    def depth(sgn):
        return NZ // 2 - c if sgn > 0 else NZ // 2 - 1 + c

    def wanted(stream, sgn, d, at):
        full = depth(sgn)
        near = d <= full
        if stream == OA:
            return near
        origin = lax.rem(at - sgn * d + NZ, NZ)
        if (stream in (K, V)) == (sgn > 0):
            some = (at >= d) if sgn > 0 else (at + d <= NZ - 1)
        else:
            some = (origin + full >= NZ) if sgn > 0 else (origin < full)
        if stream == V:
            some = some | (yl == 0)
        if stream == G:
            some = some | (yl == 1)
        return near & some

    bufs = (kb, vb, qb, gb, oa, ga2, gb2, oa2)

    def hop(stream, sgn, d, at):
        block = bufs[stream].at[lax.rem(at - sgn * (d - 1) + NZ, NZ)]
        to = dev(z_=lax.rem(z + sgn + NZ, NZ))
        i = 0 if sgn > 0 else 1
        return remote(block, block, rgs.at[stream, i, d - 1], rgr.at[stream, i, d - 1], to)

    def send_hop(stream, sgn, d):
        @pl.when(wanted(stream, sgn, d, lax.rem(z + sgn + NZ, NZ)))
        def _():
            hop(stream, sgn, d, z).start()

    across = dev(yl_=1 - yl)

    def over(stream, origin):
        dst, n = (ob2, 1) if stream == GB else (ob, 0)
        return remote(
            bufs[stream].at[origin], dst.at[origin], yfs.at[n, origin], yfr.at[n, origin], across
        )

    def send_over(stream, origin):
        @pl.when(yl == (0 if stream == V else 1))
        def _():
            over(stream, origin).start()

    def take_hop(stream, sgn, d):
        @pl.when(wanted(stream, sgn, d, z))
        def _():
            hop(stream, sgn, d, lax.rem(z - sgn + NZ, NZ)).wait_recv()
            if stream in (V, G, GB):
                send_over(stream, lax.rem(z - sgn * d + NZ, NZ))

    def ring_start(stream):
        for sgn in (1, -1):
            send_hop(stream, sgn, 1)
        if stream in (V, G, GB):
            send_over(stream, z)

    def ring_step(d, *streams):
        for stream in streams:
            for sgn in (1, -1):
                take_hop(stream, sgn, d)
                if d < NZ // 2:
                    send_hop(stream, sgn, d + 1)

    def ring_sent(*streams):
        for stream in streams:
            for d in range(1, NZ // 2 + 1):
                for sgn in (1, -1):

                    @pl.when(wanted(stream, sgn, d, lax.rem(z + sgn + NZ, NZ)))
                    def _():
                        hop(stream, sgn, d, z).wait_send()

            if stream in (V, G, GB):

                @pl.when(yl == (0 if stream == V else 1))
                def _():
                    for i in range(NZ):
                        over(stream, i).wait_send()

    def over_wait(n):
        buf = ob2 if n else ob
        for i in range(NZ):
            remote(buf.at[i], buf.at[i], yfs.at[n, i], yfr.at[n, i], across).wait_recv()

    def wanted2(stream, sgn, d, at):
        full = depth(sgn)
        near = d <= full
        if stream == OA2:
            return near & (yl == 0)
        origin = lax.rem(at - sgn * d + NZ, NZ)
        if sgn < 0:
            some = origin >= d
        else:
            some = origin + (full if d == 2 else d) >= NZ
        if stream == GB:
            some = some | (yl == 1)
        return near & some

    def far_hop(stream, sgn, d, at):
        base, step = ((0, 1), (0, 2), (2, 1), (2, 2))[d - 1]
        origin = lax.rem(at - sgn * base + NZ, NZ)
        block = bufs[stream].at[origin]
        z_to = lax.rem(z + sgn * step + NZ, NZ)
        i = 0 if sgn > 0 else 1
        sems = rgs.at[stream, i, d - 1], rgr.at[stream, i, d - 1]
        if stream == OA2 and d == 2:
            return remote(ga2.at[origin], block, *sems, dev(yl_=1 - yl, z_=z_to))
        return remote(block, block, *sems, dev(z_=z_to))

    def far_cond(stream, sgn, d):
        step = (1, 2, 1, 2)[d - 1]
        if stream == OA2 and d == 2:
            return yl == 1
        return wanted2(stream, sgn, d, lax.rem(z + sgn * step + NZ, NZ))

    def far_send(stream, *ds):
        for d in ds:
            for sgn in (1, -1):

                @pl.when(far_cond(stream, sgn, d))
                def _():
                    far_hop(stream, sgn, d, z).start()

    def far_take(stream, *ds):
        for d in ds:
            for sgn in (1, -1):

                @pl.when(wanted2(stream, sgn, d, z))
                def _():
                    step = (1, 2, 1, 2)[d - 1]
                    far_hop(stream, sgn, d, lax.rem(z - sgn * step + NZ, NZ)).wait_recv()
                    if stream == GB:
                        send_over(stream, lax.rem(z - sgn * d + NZ, NZ))

                if d == 2:
                    for e in (4, 3):

                        @pl.when(far_cond(stream, sgn, e))
                        def _():
                            far_hop(stream, sgn, e, z).start()

    def far_sent(*streams):
        for stream in streams:
            for d in range(1, NZ // 2 + 1):
                for sgn in (1, -1):

                    @pl.when(far_cond(stream, sgn, d))
                    def _():
                        far_hop(stream, sgn, d, z).wait_send()

            if stream == GB:

                @pl.when(yl == 1)
                def _():
                    for i in range(NZ):
                        over(stream, i).wait_send()

    def cross(src, dst, i):
        return remote(src.at[z], dst.at[z], yxs.at[i], yxr.at[i], across)

    def project(i):
        return dot(agx[...].reshape(TOK, D), wqkv[:, i * WIDTH : (i + 1) * WIDTH])

    def turned_into(buf, v):
        for h in range(HEADS_DEV):
            buf[z, :, h * HEAD_DIM : (h + 1) * HEAD_DIM] = turn(
                v[:, h * HEAD_DIM : (h + 1) * HEAD_DIM]
            ).astype(BF16)

    turned_into(kb, project(1))

    @pl.when(yl == 0)
    def _():
        cross(kb, oa, 0).start()

    ring_start(K)
    vb[z] = project(2).astype(BF16)
    ring_start(V)
    turned_into(qb, project(0))

    @pl.when(yl == 1)
    def _():
        cross(qb, oa, 0).start()

    ring_step(1, K)
    gather_pass(agi, 1)
    ring_step(1, V)
    cross(oa, oa, 0).wait_recv()
    ring_start(OA)
    ring_start(Q)
    gather_finish(agi, 1)
    gb[z] = dot(agi[...].reshape(TOK, D), wo_t[...]).astype(BF16)
    ring_start(G)
    ring_step(1, OA)
    ring_step(2, K, V)
    ring_step(2, OA)
    ring_step(1, Q, G)
    ring_step(3, K, V)
    ring_step(3, OA)
    ring_step(2, Q, G)
    ring_step(4, K, V)
    ring_step(4, OA)
    ring_step(3, Q, G)
    @pl.when(yl == 1)
    def _():
        over_wait(0)

    def lanes(h):
        return pl.ds(h * HEAD_DIM, HEAD_DIM)

    def rows_of(buf, h):
        return buf[:, :, lanes(h)].reshape(PLANE, HEAD_DIM)

    def as_row(col):
        return jnp.transpose(jnp.broadcast_to(col, (TOK, TOK)))[0:1, :]

    def forward(parts):
        for h in range(HEADS_DEV):
            query = qb[z, :, lanes(h)]
            top = None
            for i, (buf, _) in enumerate(parts):
                sc = dot(query, rows_of(buf, h), NT) * scale + bq[i]
                pq[h, i] = sc
                m = jnp.max(sc, axis=1, keepdims=True)
                top = m if top is None else jnp.maximum(top, m)
            total = None
            for i in range(len(parts)):
                e = jnp.exp(pq[h, i] - top)
                pq[h, i] = e
                l = jnp.sum(e, axis=1, keepdims=True)
                total = l if total is None else total + l
            inv_total = 1.0 / total
            out = None
            for i, (_, buf) in enumerate(parts):
                p = pq[h, i] * inv_total
                pq[h, i] = p
                o = dot(p.astype(BF16), rows_of(buf, h))
                out = o if out is None else out + o
            out = out.astype(BF16)
            att[:, lanes(h)] = out
            grad = gb[z, :, lanes(h)]
            st[0, s, pl.ds(h, 1), :] = as_row(top + jnp.log(total))
            st[0, s, pl.ds(2 + h, 1), :] = as_row(
                jnp.sum(grad.astype(F32) * out.astype(F32), axis=1, keepdims=True)
            )

    @pl.when(yl == 0)
    def _():
        forward(((kb, vb),))

    @pl.when(yl == 1)
    def _():
        forward(((kb, vb), (oa, ob)))

    def stats_sends(it):
        out = []
        for k in range(len(SEQ_STEPS)):
            a, b = seq_to(k)
            mine = st.at[it, s]
            out.append(remote(mine, mine, sts.at[it, k], str_.at[it, k], dev(yl_=a, z_=b)))
        return out

    def stats_wait(it):
        for k in range(len(SEQ_STEPS)):
            slot = st.at[it, seq_from(k)]
            remote(slot, slot, sts.at[it, k], str_.at[it, k], partner).wait_recv()

    def own_grad(it, h):
        return gb[z, :, lanes(h)] if it == 0 else (ga2, gb2)[h][z]

    def query_side(it, parts):
        for h in range(HEADS_DEV):
            grad = own_grad(it, h)
            delta = jnp.sum(
                grad.astype(F32) * att[:, lanes(h)].astype(F32), axis=1, keepdims=True
            )
            out = None
            for i, (keys, values) in enumerate(parts):
                gp = dot(grad, rows_of(values, h), NT)
                gsc = (pq[h, i] * (gp - delta)).astype(BF16)
                o = dot(gsc, rows_of(keys, h))
                out = o if out is None else out + o
            dqkv[:, lanes(h)] = turn(out * scale, True).astype(BF16)

    def key_side(it, parts, planes):
        for h in range(HEADS_DEV):
            key = kb[z, :, lanes(h)]
            value = vb[z, :, lanes(h)]
            gk, gv = None, None
            for i, (queries, grads, late) in enumerate(parts):
                row = lambda n, r: jnp.concatenate(
                    [st[n, planes[i] * NZ + j, pl.ds(r, 1), :] for j in range(NZ)], axis=1
                )
                query = rows_of(queries, h)
                if it == 0:
                    p = jnp.exp(dot(key, query, NT) * scale + bk[i] - row(0, h))
                    pk[h, i] = p
                    grad = rows_of(grads, h)
                else:
                    p = pk[h, i]
                    grad = late[h][...].reshape(PLANE, HEAD_DIM)
                v = dot(p.astype(BF16), grad)
                gv = v if gv is None else gv + v
                gp = dot(value, grad, NT)
                gsc = (p * (gp - row(it, 2 + h))).astype(BF16)
                k = dot(gsc, query)
                gk = k if gk is None else gk + k
            dqkv[:, lanes(HEADS_DEV + h)] = turn(gk * scale, True).astype(BF16)
            dqkv[:, lanes(2 * HEADS_DEV + h)] = gv.astype(BF16)

    def own_queries(it):
        @pl.when(yl == 0)
        def _():
            query_side(it, ((kb, vb),))

        @pl.when(yl == 1)
        def _():
            query_side(it, ((kb, vb), (oa, ob)))

    def backward(it):
        stats_wait(it)

        @pl.when(yl == 0)
        def _():
            over_wait(it)

        @pl.when(yl == 0)
        def _():
            key_side(it, ((qb, gb, (ga2, gb2)), (oa, ob, (oa2, ob2))), (yl, 1 - yl))

        @pl.when(yl == 1)
        def _():
            key_side(it, ((qb, gb, (ga2, gb2)),), (yl,))

        wide = HALF // CHUNKS
        gives = []
        for j in range(CHUNKS):
            cols = pl.ds(pl.multiple_of((1 - c) * HALF + j * wide, wide), wide)
            tot[it, j] = dot(dqkv[...], wqkv_t[:, cols]).astype(BF16).reshape(CHIPS, CROWS, wide)
            cp = remote(tot.at[it, j], drv.at[it, j], gvs.at[it, j], gvr.at[it, j], partner)
            cp.start()
            gives.append(cp)
        sends = []
        last_term = it == ITERS - 1
        for j in range(CHUNKS):
            cols = pl.ds(pl.multiple_of(c * HALF + j * wide, wide), wide)
            pair[j] = dot(dqkv[...], wqkv_t[:, cols]).reshape(CHIPS, CROWS, wide)

        def scatter(j):
            for k in range(7):
                a, b = chip_to(k)
                rsrc[it, j, k] = pair[j, a * NX + b].astype(BF16)
                cp = remote(
                    rsrc.at[it, j, k], rrv.at[it, j, k], rss.at[it, j, k], rsr.at[it, j, k],
                    dev(yh_=a, x_=b),
                )
                cp.start()
                sends.append(cp)

        for j in range(CHUNKS):
            gives[j].wait_recv()
            pair[j] += drv[it, j].astype(F32)
            if not last_term:
                scatter(j)
        for j in range(CHUNKS):
            cols = pl.ds(pl.multiple_of(c * HALF + j * wide, wide), wide)
            here = pl.ds(j * wide, wide)
            term = jnp.sum(
                (pair[j] * agx[:, :, cols].astype(F32)).reshape(TOK, wide), axis=0, keepdims=True
            )
            gacc[:, here] = term if it == 0 else gacc[:, here] + term
            gn[:, here] = pair[j, chip]
        if last_term:
            gs[s] = gacc[...]
            for cp in gain_seq_sends():
                cp.start()
            for j in range(CHUNKS):
                scatter(j)
            for k in range(len(SEQ_STEPS)):
                slot = gs.at[seq_from(k)]
                remote(slot, slot, gss.at[k], gsr.at[k], partner).wait_recv()
            acc = gs[0]
            for i in range(1, NY * NZ):
                acc = acc + gs[i]
            gt[chip] = acc
            for cp in gain_chip_sends():
                cp.start()
            sent.extend(gain_seq_sends() + gain_chip_sends())
        for j in range(CHUNKS):
            here = pl.ds(j * wide, wide)
            for k in range(7):
                sends[7 * j + k].wait_recv()
                gn[:, here] += rrv[it, j, k].astype(F32)

        grad_normed = gn[...]
        scaled = sc16[...]
        weighted = gain_half * grad_normed
        inl[it] = jnp.broadcast_to(
            jnp.sum(weighted * scaled, axis=1, keepdims=True), (CROWS, 128)
        )
        share = remote(inl.at[it], inr.at[it], d2s.at[5 + it], d2r.at[5 + it], partner)
        share.start()
        share.wait_recv()
        inner = (inl[it] + inr[it])[:, 0:1]
        cot = ir16[:, 0:1] * (weighted - scaled * (inner / D))
        adj16[...] = (in16[...] if it == 0 else adj16[...]) + cot
        if it == 0:
            agc[chip, :, own_half] = cot.astype(BF16)
            gather_start(agc, 2)
        sent.extend(gives + [share] + sends)

    def gain_chip_sends():
        out = []
        for k in range(7):
            a, b = chip_to(k)
            out.append(
                remote(gt.at[chip], gt.at[chip], gts.at[k], gtr.at[k], dev(yh_=a, x_=b))
            )
        return out

    def gain_seq_sends():
        out = []
        for k in range(len(SEQ_STEPS)):
            a, b = seq_to(k)
            out.append(remote(gs.at[s], gs.at[s], gss.at[k], gsr.at[k], dev(yl_=a, z_=b)))
        return out

    for cp in stats_sends(0):
        cp.start()
    ring_step(4, Q, G)
    own_queries(0)
    backward(0)

    gather_pass(agc, 2)
    gather_finish(agc, 2)
    grad2 = dot(agc[...].reshape(TOK, D), wo_t[...]).astype(BF16)
    ga2[z] = grad2[:, :HEAD_DIM]
    gb2[z] = grad2[:, HEAD_DIM:]

    far_send(OA2, 2)
    far_send(GB, 2)

    @pl.when(yl == 1)
    def _():
        cross(ga2, oa2, 1).start()

    far_send(GA, 2)
    far_send(GB, 1)
    send_over(GB, z)
    far_send(GA, 1)
    for h in range(HEADS_DEV):
        st[1, s, pl.ds(2 + h, 1), :] = as_row(
            jnp.sum(
                own_grad(1, h).astype(F32) * att[:, lanes(h)].astype(F32), axis=1, keepdims=True
            )
        )
    for cp in stats_sends(1):
        cp.start()
    own_queries(1)
    far_take(GB, 2)
    far_take(OA2, 2)
    far_take(GA, 2)

    @pl.when(yl == 0)
    def _():
        cross(oa2, oa2, 1).wait_recv()

    far_send(OA2, 1)
    far_take(GB, 1)
    far_take(GA, 1)
    far_take(GB, 3, 4)
    far_take(OA2, 1, 3, 4)
    far_take(GA, 3, 4)
    backward(1)

    back = remote(adj16.at[far_rows, :], adjr, d2s.at[7], d2r.at[7], partner)
    back.start()
    adj_ref[:, own_half] = adj16[own_rows, :]
    for k in range(7):
        slot = gt.at[chip_from(k)]
        remote(slot, slot, gts.at[k], gtr.at[k], partner).wait_recv()
    acc = gt[0]
    for i in range(1, CHIPS):
        acc = acc + gt[i]
    gh[0] = acc / gain_half * (NY * NZ * TOK) ** (-0.5)
    last = remote(gh.at[0], gh.at[1], d2s.at[8], d2r.at[8], partner)
    last.start()
    back.wait_recv()
    adj_ref[:, far_half] = adjr[...]
    gg_ref[:, own_half] = gh[0]
    last.wait_recv()
    gg_ref[:, far_half] = gh[1]
    ring_sent(K, V, Q, G, OA)
    far_sent(GA, GB, OA2)
    gather_sent(agx, 0)
    gather_sent(agi, 1)
    gather_sent(agc, 2)

    @pl.when(yl == 0)
    def _():
        cross(kb, oa, 0).wait_send()

    @pl.when(yl == 1)
    def _():
        cross(qb, oa, 0).wait_send()

    @pl.when(yl == 1)
    def _():
        cross(ga2, oa2, 1).wait_send()

    for cp in sent + stats_sends(0) + stats_sends(1) + [back, last]:
        cp.wait_send()


def scratch():
    v = pltpu.VMEM
    dma = pltpu.SemaphoreType.DMA
    wide = HALF // CHUNKS
    block = (NZ, TOK, WIDTH)
    half_block = (NZ, TOK, HEAD_DIM)
    return [
        v((ROWS, D), BF16), v((ROWS, D), BF16), v((1, D), F32), v((1, HEAD_DIM), F32),
        v((NBLK, NBLK), jnp.int32),
        v((D, 3 * WIDTH), BF16), v((WIDTH, D), BF16), v((3 * WIDTH, D), BF16), v((D, WIDTH), BF16),
        v((TOK, HEAD_DIM), F32), v((TOK, HEAD_DIM), F32),
        v((2, ROWS, D), F32), v((CROWS, HALF), F32), v((CROWS, HALF), F32), v((CROWS, 128), F32),
        v((ROWS, 128), F32),
        v((CHIPS, CROWS, D), BF16), v((CHIPS, CROWS, D), BF16), v((CHIPS, CROWS, D), BF16),
        v(block, BF16), v(block, BF16), v(block, BF16), v(block, BF16), v(block, BF16),
        v(block, BF16),
        v(half_block, BF16), v(half_block, BF16), v(half_block, BF16), v(half_block, BF16),
        v((ITERS, NY * NZ, 8, TOK), F32),
        v((2, TOK, PLANE), F32), v((2, TOK, PLANE), F32),
        v((HEADS_DEV, 2, TOK, PLANE), F32), v((HEADS_DEV, 2, TOK, PLANE), F32),
        v((TOK, WIDTH), BF16), v((TOK, 3 * WIDTH), BF16),
        v((ITERS, CHUNKS, CHIPS, CROWS, wide), BF16), v((ITERS, CHUNKS, CHIPS, CROWS, wide), BF16),
        v((ITERS, CHUNKS, 7, CROWS, wide), BF16), v((ITERS, CHUNKS, 7, CROWS, wide), BF16),
        v((CHUNKS, CHIPS, CROWS, wide), F32), v((CROWS, HALF), F32),
        v((ITERS, CROWS, 128), F32), v((ITERS, CROWS, 128), F32),
        v((CROWS, HALF), F32), v((ROWS, HALF), F32), v((1, HALF), F32),
        v((CHIPS, 1, HALF), F32), v((NY * NZ, 1, HALF), F32), v((2, 1, HALF), F32),
        dma((5,)), dma((4,)), dma((3, 8)), dma((3, 8)), dma((3, 7)), dma((3, 7)), dma((9,)), dma((9,)),
        dma((8, 2, 4)), dma((8, 2, 4)), dma((2,)), dma((2,)), dma((2, NZ)), dma((2, NZ)),
        dma((ITERS, 15)), dma((ITERS, 15)), dma((ITERS, CHUNKS)), dma((ITERS, CHUNKS)),
        dma((ITERS, CHUNKS, 7)), dma((ITERS, CHUNKS, 7)),
        dma((7,)), dma((7,)), dma((15,)), dma((15,)),
    ]


def body(
    fixed_point, incoming, norm_gain, query_weight, key_weight, value_weight, out_weight, layout
):
    pair = np.arange(HEAD_DIM) % (HEAD_DIM // 2)
    freq = jnp.asarray(THETA ** (-2.0 * pair / HEAD_DIM), F32)
    vmem = pl.BlockSpec(memory_space=pltpu.VMEM)
    hbm = pl.BlockSpec(memory_space=pl.ANY)
    adjoint, gain = pl.pallas_call(
        kernel,
        out_shape=(
            jax.ShapeDtypeStruct((ROWS, D), F32),
            jax.ShapeDtypeStruct((1, D), F32),
        ),
        in_specs=[hbm] * 9,
        out_specs=(vmem, vmem),
        scratch_shapes=scratch(),
        compiler_params=pltpu.CompilerParams(
            collective_id=0, has_side_effects=True, vmem_limit_bytes=62 * 1024 * 1024
        ),
        name="deq_backward",
    )(
        fixed_point, incoming, norm_gain[None, :], freq[None, :], layout,
        query_weight, key_weight, value_weight, out_weight,
    )
    return adjoint, gain[0]


def solution(mesh):
    split = Mesh(mesh.devices.reshape(NY, NZ, NH, NX, NC), AXES)
    in_specs = (
        P(SEQ_TENSOR, None),
        P(SEQ_TENSOR, None),
        P(),
        P(None, TENSOR),
        P(None, TENSOR),
        P(None, TENSOR),
        P(TENSOR, None),
        P(),
    )
    out_specs = (P(SEQ_TENSOR, None), P())
    return jax.shard_map(body, mesh=split, in_specs=in_specs, out_specs=out_specs, check_vma=False)
```

```python
import functools

import jax
import jax.numpy as jnp
import numpy as np
from jax import lax
from jax.experimental import pallas as pl
from jax.experimental.pallas import tpu as pltpu
from jax.sharding import Mesh
from jax.sharding import PartitionSpec as P

HEAD_DIM = 128
BLK = 64
ITERS = 2
EPS = 1e-05
THETA = 10000.0
MASKED = -1e30
AXES = ("seq_0", "seq_1", "tensor_0", "tensor_1", "tensor_2")
TENSOR = ("tensor_0", "tensor_1", "tensor_2")
SEQ = ("seq_0", "seq_1")
SEQ_TENSOR = AXES
MESH = pl.DeviceIdType.MESH
F32, BF16 = jnp.float32, jnp.bfloat16

NY, NZ, NH, NX, NC = 2, 8, 2, 4, 2
CHIPS = NH * NX
ROWS = 8
CROWS = NC * ROWS
TOK = CHIPS * CROWS
PLANE = NZ * TOK
D = 4096
HALF = D // 2
HEADS_DEV = 2
WIDTH = HEADS_DEV * HEAD_DIM
NBLK = 32

CHIP_STEPS = ((1, 2), (1, 1), (1, 3), (0, 2), (1, 0), (0, 1), (0, 3))
SEQ_STEPS = tuple(
    (a, b % NZ) for b in (4, 3, -3, 2, -2, 1, -1, 0) for a in (1, 0) if (a, b) != (0, 0)
)
K, V, Q, G, OA, GA, GB, OA2 = range(8)
CHUNKS = 2

NN = (((1,), (0,)), ((), ()))
NT = (((1,), (1,)), ((), ()))


def dot(a, b, dims=NN):
    return lax.dot_general(a, b, dims, preferred_element_type=F32)


def kernel(
    point_hbm, inc_hbm, gain_hbm, freq_hbm, lay_hbm, wq_hbm, wk_hbm, wv_hbm, wo_hbm,
    adj_ref, gg_ref,
    point_ref, inc_ref, gain_ref, freq_ref, lay_ref,
    wqkv, wo, wqkv_t, wo_t, cosb, sinb, loc, sc16, in16, ir16, irl, agx, agi, agc,
    gpk, kb, vb, qb, gb, oa, ob, ga2, gb2, oa2, ob2, st, bq, bk, pq, pk, att, dqkv,
    tot, drv, rsrc, rrv, pair, gn, inl, inr, adj16, adjr, gacc, gt, gs, gh,
    in_sem, w_sem, ags, agr, fws, fwr, d2s, d2r, rgs, rgr, yxs, yxr, yfs, yfr, sts, str_,
    gvs, gvr, rss, rsr, gts, gtr, gss, gsr,
):
    yl, z, yh, x, c = (lax.axis_index(a) for a in AXES)
    chip = yh * NX + x
    s = yl * NZ + z
    scale = HEAD_DIM ** (-0.5)

    def dev(yl_=None, z_=None, yh_=None, x_=None, c_=None):
        pick = lambda a, b: a if b is None else b
        return (pick(yl, yl_), pick(z, z_), pick(yh, yh_), pick(x, x_), pick(c, c_))

    partner = dev(c_=1 - c)
    sent = []
    own_half = pl.ds(pl.multiple_of(c * HALF, HALF), HALF)
    far_half = pl.ds(pl.multiple_of((1 - c) * HALF, HALF), HALF)
    own_rows = pl.ds(pl.multiple_of(c * ROWS, ROWS), ROWS)
    far_rows = pl.ds(pl.multiple_of((1 - c) * ROWS, ROWS), ROWS)

    def remote(src, dst, ssem, rsem, to):
        return pltpu.make_async_remote_copy(
            src_ref=src, dst_ref=dst, send_sem=ssem, recv_sem=rsem, device_id=to, device_id_type=MESH
        )

    def chip_to(k):
        a, b = CHIP_STEPS[k]
        return lax.rem(yh + a, NH), lax.rem(x + b, NX)

    def chip_from(k):
        a, b = CHIP_STEPS[k]
        return lax.rem(yh + NH - a, NH) * NX + lax.rem(x + NX - b, NX)

    def seq_to(k):
        a, b = SEQ_STEPS[k]
        return lax.rem(yl + a, NY), lax.rem(z + b, NZ)

    def seq_from(k):
        a, b = SEQ_STEPS[k]
        return lax.rem(yl + NY - a, NY) * NZ + lax.rem(z + NZ - b, NZ)

    small = [
        pltpu.make_async_copy(h, v, in_sem.at[i])
        for i, (h, v) in enumerate(
            ((point_hbm, point_ref), (inc_hbm, inc_ref), (gain_hbm, gain_ref),
             (freq_hbm, freq_ref), (lay_hbm, lay_ref))
        )
    ]
    for cp in small:
        cp.start()
    loads = [
        pltpu.make_async_copy(h, wqkv.at[:, pl.ds(i * WIDTH, WIDTH)], w_sem.at[i])
        for i, h in enumerate((wq_hbm, wk_hbm, wv_hbm))
    ]
    loads.append(pltpu.make_async_copy(wo_hbm, wo, w_sem.at[3]))

    @pl.loop(0, NZ)
    def _(i):
        for buf in (kb, vb, qb, gb):
            buf[i] = jnp.zeros((TOK, WIDTH), BF16)
        for buf in (ga2, gb2):
            buf[i] = jnp.zeros((TOK, HEAD_DIM), BF16)

    bar = pltpu.get_barrier_semaphore()
    greet = [partner]
    for k in range(len(CHIP_STEPS)):
        a, b = chip_to(k)
        greet.append(dev(yh_=a, x_=b))
    for k in range(len(SEQ_STEPS)):
        a, b = seq_to(k)
        greet.append(dev(yl_=a, z_=b))
    for g in greet:
        pl.semaphore_signal(bar, inc=1, device_id=g, device_id_type=MESH)

    for cp in small:
        cp.wait()
    for cp in loads:
        cp.start()
    pt = point_ref[...].astype(F32)
    inv = lax.rsqrt(jnp.mean(pt * pt, axis=1, keepdims=True) + EPS)
    loc[0] = pt * inv
    loc[1] = inc_ref[...].astype(F32)
    irl[...] = jnp.broadcast_to(inv, (ROWS, 128))
    pl.semaphore_wait(bar, len(greet))

    swaps = [
        remote(loc.at[0, :, far_half], sc16.at[own_rows, :], d2s.at[0], d2r.at[0], partner),
        remote(loc.at[1, :, far_half], in16.at[own_rows, :], d2s.at[1], d2r.at[1], partner),
        remote(irl, ir16.at[own_rows, :], d2s.at[2], d2r.at[2], partner),
    ]
    for cp in swaps:
        cp.start()
    sc16[own_rows, :] = loc[0, :, own_half]
    in16[own_rows, :] = loc[1, :, own_half]
    ir16[own_rows, :] = irl[...]
    gain_half = gain_ref[:, own_half]
    for cp, buf in zip(swaps, (sc16, in16, ir16)):
        cp.wait_send()
    remote(loc.at[0, :, far_half], sc16.at[far_rows, :], d2s.at[0], d2r.at[0], partner).wait_recv()
    remote(loc.at[1, :, far_half], in16.at[far_rows, :], d2s.at[1], d2r.at[1], partner).wait_recv()
    remote(irl, ir16.at[far_rows, :], d2s.at[2], d2r.at[2], partner).wait_recv()

    def gather_start(buf, g):
        mine = buf.at[chip, :, own_half]
        remote(mine, mine, fws.at[g], fwr.at[g], partner).start()
        for k in range(7):
            a, b = chip_to(k)
            remote(mine, mine, ags.at[g], agr.at[g, k], dev(yh_=a, x_=b)).start()

    def gather_pass(buf, g):
        for k in range(7):
            slot = buf.at[chip_from(k), :, own_half]
            remote(slot, slot, ags.at[g], agr.at[g, k], partner).wait_recv()
            remote(slot, slot, fws.at[g], fwr.at[g], partner).start()

    def gather_finish(buf, g):
        far = buf.at[:, :, far_half]
        remote(far, far, fws.at[g], fwr.at[g], partner).wait_recv()

    def gather_sent(buf, g):
        own = buf.at[:, :, own_half]
        remote(own, own, fws.at[g], fwr.at[g], partner).wait_send()
        seven = buf.at[pl.ds(0, 7), :, own_half]
        remote(seven, seven, ags.at[g], agr.at[g, 0], partner).wait_send()

    agx[chip, :, own_half] = (gain_half * sc16[...]).astype(BF16)
    gather_start(agx, 0)
    agi[chip, :, own_half] = in16[...].astype(BF16)

    row_tok = s * TOK + lax.broadcasted_iota(jnp.int32, (TOK, 1), 0)
    row_blk = row_tok // BLK
    blk_col = lax.broadcasted_iota(jnp.int32, (TOK, NBLK), 1)
    lay = jnp.where(lay_ref[...] > 0, 1.0, 0.0).astype(BF16)
    onehot = jnp.where(blk_col == row_blk, 1.0, 0.0).astype(BF16)
    chosen_q = jnp.where(blk_col < row_blk, dot(onehot, lay), 0.0).astype(BF16)
    chosen_k = jnp.where(blk_col > row_blk, dot(onehot, lay, NT), 0.0).astype(BF16)
    for part in range(2):
        plane = yl if part == 0 else 1 - yl
        col_blk = plane * (PLANE // BLK) + lax.broadcasted_iota(jnp.int32, (NBLK, PLANE), 1) // BLK
        spread = jnp.where(lax.broadcasted_iota(jnp.int32, (NBLK, PLANE), 0) == col_blk, 1.0, 0.0)
        spread = spread.astype(BF16)
        col_tok = plane * PLANE + lax.broadcasted_iota(jnp.int32, (1, PLANE), 1)
        same = row_blk == col_tok // BLK
        ok = (dot(chosen_q, spread) > 0.5) | (same & (col_tok <= row_tok))
        bq[part] = jnp.where(ok, 0.0, MASKED)
        ok = (dot(chosen_k, spread) > 0.5) | (same & (col_tok >= row_tok))
        bk[part] = jnp.where(ok, 0.0, MASKED)

    angle = row_tok.astype(F32) * freq_ref[...]
    lower = lax.broadcasted_iota(jnp.int32, (TOK, HEAD_DIM), 1) < HEAD_DIM // 2
    cosb[...] = jnp.cos(angle)
    sine = jnp.sin(angle)
    sinb[...] = jnp.where(lower, -sine, sine)

    def turn(v, back=False):
        turned = pltpu.roll(v, HEAD_DIM // 2, 1) * sinb[...]
        return v * cosb[...] - turned if back else v * cosb[...] + turned

    for cp in loads:
        cp.wait()

    @pl.loop(0, D // 512)
    def _(j):
        rows = pl.ds(pl.multiple_of(j * 512, 512), 512)
        wqkv_t[:, rows] = jnp.transpose(wqkv[rows, :])
        wo_t[rows, :] = jnp.transpose(wo[:, rows])

    gather_start(agi, 1)
    gather_pass(agx, 0)
    gather_finish(agx, 0)

    def depth(sgn):
        return NZ // 2 - c if sgn > 0 else NZ // 2 - 1 + c

    def wanted(stream, sgn, d, at):
        full = depth(sgn)
        near = d <= full
        if stream == OA:
            return near
        origin = lax.rem(at - sgn * d + NZ, NZ)
        if (stream in (K, V)) == (sgn > 0):
            some = (at >= d) if sgn > 0 else (at + d <= NZ - 1)
        else:
            some = (origin + full >= NZ) if sgn > 0 else (origin < full)
        if stream == V:
            some = some | (yl == 0)
        if stream == G:
            some = some | (yl == 1)
        return near & some

    bufs = (kb, vb, qb, gb, oa, ga2, gb2, oa2)
    slot_of = {GA: K, GB: V, OA2: OA}

    def hop(stream, sgn, d, at):
        block = bufs[stream].at[lax.rem(at - sgn * (d - 1) + NZ, NZ)]
        to = dev(z_=lax.rem(z + sgn + NZ, NZ))
        i = 0 if sgn > 0 else 1
        return remote(block, block, rgs.at[stream, i, d - 1], rgr.at[stream, i, d - 1], to)

    def send_hop(stream, sgn, d):
        @pl.when(wanted(stream, sgn, d, lax.rem(z + sgn + NZ, NZ)))
        def _():
            hop(stream, sgn, d, z).start()

    across = dev(yl_=1 - yl)

    def over(stream, origin):
        dst, n = (ob2, 1) if stream == GB else (ob, 0)
        return remote(
            bufs[stream].at[origin], dst.at[origin], yfs.at[n], yfr.at[n], across
        )

    def over_sent(stream):
        @pl.when(yl == (0 if stream == V else 1))
        def _():
            n = 1 if stream == GB else 0
            remote(bufs[stream], ob2 if n else ob, yfs.at[n], yfr.at[n], across).wait_send()

    def send_over(stream, origin):
        @pl.when(yl == (0 if stream == V else 1))
        def _():
            over(stream, origin).start()

    def take_hop(stream, sgn, d):
        @pl.when(wanted(stream, sgn, d, z))
        def _():
            hop(stream, sgn, d, lax.rem(z - sgn + NZ, NZ)).wait_recv()
            if stream in (V, G, GB):
                send_over(stream, lax.rem(z - sgn * d + NZ, NZ))

    def ring_start(stream):
        for sgn in (1, -1):
            send_hop(stream, sgn, 1)
        if stream in (V, G, GB):
            send_over(stream, z)

    def ring_step(d, *streams):
        for stream in streams:
            for sgn in (1, -1):
                take_hop(stream, sgn, d)
                if d < NZ // 2:
                    send_hop(stream, sgn, d + 1)

    def ring_sent(*streams):
        for stream in streams:
            for d in range(1, NZ // 2 + 1):
                for sgn in (1, -1):

                    @pl.when(wanted(stream, sgn, d, lax.rem(z + sgn + NZ, NZ)))
                    def _():
                        hop(stream, sgn, d, z).wait_send()

            if stream in (V, G):
                over_sent(stream)

    def over_wait(n):
        buf = ob2 if n else ob
        remote(buf, buf, yfs.at[n], yfr.at[n], across).wait_recv()

    def wanted2(stream, sgn, d, at):
        full = depth(sgn)
        near = d <= full
        if stream == OA2:
            return near & (yl == 0)
        origin = lax.rem(at - sgn * d + NZ, NZ)
        if sgn < 0:
            some = origin >= d
        else:
            some = origin + (full if d == 2 else d) >= NZ
        if stream == GB:
            some = some | (yl == 1)
        return near & some

    def far_hop(stream, sgn, d, at):
        base, step = ((0, 1), (0, 2), (2, 1), (2, 2))[d - 1]
        origin = lax.rem(at - sgn * base + NZ, NZ)
        block = bufs[stream].at[origin]
        z_to = lax.rem(z + sgn * step + NZ, NZ)
        i = 0 if sgn > 0 else 1
        n = slot_of[stream]
        sems = rgs.at[n, i, d - 1], rgr.at[n, i, d - 1]
        if stream == OA2 and d == 2:
            return remote(ga2.at[origin], block, *sems, dev(yl_=1 - yl, z_=z_to))
        return remote(block, block, *sems, dev(z_=z_to))

    def far_cond(stream, sgn, d):
        step = (1, 2, 1, 2)[d - 1]
        if stream == OA2 and d == 2:
            return yl == 1
        return wanted2(stream, sgn, d, lax.rem(z + sgn * step + NZ, NZ))

    def far_send(stream, *ds):
        for d in ds:
            for sgn in (1, -1):

                @pl.when(far_cond(stream, sgn, d))
                def _():
                    far_hop(stream, sgn, d, z).start()

    def far_take(stream, *ds):
        for d in ds:
            for sgn in (1, -1):

                @pl.when(wanted2(stream, sgn, d, z))
                def _():
                    step = (1, 2, 1, 2)[d - 1]
                    far_hop(stream, sgn, d, lax.rem(z - sgn * step + NZ, NZ)).wait_recv()
                    if stream == GB:
                        send_over(stream, lax.rem(z - sgn * d + NZ, NZ))

                if d == 2:
                    for e in (4, 3):

                        @pl.when(far_cond(stream, sgn, e))
                        def _():
                            far_hop(stream, sgn, e, z).start()

    def far_sent(*streams):
        for stream in streams:
            for d in range(1, NZ // 2 + 1):
                for sgn in (1, -1):

                    @pl.when(far_cond(stream, sgn, d))
                    def _():
                        far_hop(stream, sgn, d, z).wait_send()

            if stream == GB:
                over_sent(stream)

    def cross(src, dst, i):
        return remote(src.at[z], dst.at[z], yxs.at[i], yxr.at[i], across)

    def project(i):
        return dot(agx[...].reshape(TOK, D), wqkv[:, i * WIDTH : (i + 1) * WIDTH])

    def turned_into(buf, v):
        for h in range(HEADS_DEV):
            buf[z, :, h * HEAD_DIM : (h + 1) * HEAD_DIM] = turn(
                v[:, h * HEAD_DIM : (h + 1) * HEAD_DIM]
            ).astype(BF16)

    turned_into(kb, project(1))

    @pl.when(yl == 0)
    def _():
        cross(kb, oa, 0).start()

    ring_start(K)
    vb[z] = project(2).astype(BF16)
    ring_start(V)
    turned_into(qb, project(0))

    @pl.when(yl == 1)
    def _():
        cross(qb, oa, 0).start()

    ring_step(1, K)
    gather_pass(agi, 1)
    ring_step(1, V)
    cross(oa, oa, 0).wait_recv()
    ring_start(OA)
    ring_start(Q)
    gather_finish(agi, 1)
    gb[z] = dot(agi[...].reshape(TOK, D), wo_t[...]).astype(BF16)
    ring_start(G)
    ring_step(1, OA)
    ring_step(2, K, V)
    ring_step(2, OA)
    ring_step(1, Q, G)
    ring_step(3, K, V)
    ring_step(3, OA)
    ring_step(2, Q, G)
    ring_step(4, K, V)
    ring_step(4, OA)
    ring_step(3, Q, G)
    @pl.when(yl == 1)
    def _():
        over_wait(0)

    def lanes(h):
        return pl.ds(h * HEAD_DIM, HEAD_DIM)

    def rows_of(buf, h):
        return buf[:, :, lanes(h)].reshape(PLANE, HEAD_DIM)

    def as_row(col):
        return jnp.transpose(jnp.broadcast_to(col, (TOK, TOK)))[0:1, :]

    def forward(parts):
        for h in range(HEADS_DEV):
            query = qb[z, :, lanes(h)]
            top = None
            for i, (buf, _) in enumerate(parts):
                sc = dot(query, rows_of(buf, h), NT) * scale + bq[i]
                pq[h, i] = sc
                m = jnp.max(sc, axis=1, keepdims=True)
                top = m if top is None else jnp.maximum(top, m)
            total = None
            for i in range(len(parts)):
                e = jnp.exp(pq[h, i] - top)
                pq[h, i] = e
                l = jnp.sum(e, axis=1, keepdims=True)
                total = l if total is None else total + l
            inv_total = 1.0 / total
            out = None
            for i, (_, buf) in enumerate(parts):
                p = pq[h, i] * inv_total
                pq[h, i] = p
                o = dot(p.astype(BF16), rows_of(buf, h))
                out = o if out is None else out + o
            out = out.astype(BF16)
            att[:, lanes(h)] = out
            grad = gb[z, :, lanes(h)]
            st[0, s, pl.ds(h, 1), :] = as_row(top + jnp.log(total))
            st[0, s, pl.ds(2 + h, 1), :] = as_row(
                jnp.sum(grad.astype(F32) * out.astype(F32), axis=1, keepdims=True)
            )

    @pl.when(yl == 0)
    def _():
        forward(((kb, vb),))

    @pl.when(yl == 1)
    def _():
        forward(((kb, vb), (oa, ob)))

    def stats_start(it):
        mine = st.at[it, s]
        for k in range(len(SEQ_STEPS)):
            a, b = seq_to(k)
            remote(mine, mine, sts.at[it], str_.at[it], dev(yl_=a, z_=b)).start()

    def stats_all(it):
        most = st.at[it, pl.ds(0, len(SEQ_STEPS))]
        return remote(most, most, sts.at[it], str_.at[it], partner)

    def own_grad(it, h):
        return gb[z, :, lanes(h)] if it == 0 else (ga2, gb2)[h][z]

    def query_side(it, parts):
        for h in range(HEADS_DEV):
            grad = own_grad(it, h)
            delta = jnp.sum(
                grad.astype(F32) * att[:, lanes(h)].astype(F32), axis=1, keepdims=True
            )
            out = None
            for i, (keys, values) in enumerate(parts):
                gp = dot(grad, rows_of(values, h), NT)
                gsc = (pq[h, i] * (gp - delta)).astype(BF16)
                o = dot(gsc, rows_of(keys, h))
                out = o if out is None else out + o
            dqkv[:, lanes(h)] = turn(out * scale, True).astype(BF16)

    def key_scores(it, parts):
        for h in range(HEADS_DEV):
            for i, (queries, grads, late) in enumerate(parts):
                if it == 0:
                    query = rows_of(queries, h)
                    pk[h, i] = dot(kb[z, :, lanes(h)], query, NT) * scale + bk[i]
                    grad = rows_of(grads, h)
                else:
                    grad = late[h][...].reshape(PLANE, HEAD_DIM)
                gpk[h, i] = dot(vb[z, :, lanes(h)], grad, NT)

    def key_side(it, parts, planes):
        for h in range(HEADS_DEV):
            gk, gv = None, None
            for i, (queries, grads, late) in enumerate(parts):
                row = lambda n, r: jnp.concatenate(
                    [st[n, planes[i] * NZ + j, pl.ds(r, 1), :] for j in range(NZ)], axis=1
                )
                query = rows_of(queries, h)
                if it == 0:
                    p = jnp.exp(pk[h, i] - row(0, h))
                    pk[h, i] = p
                    grad = rows_of(grads, h)
                else:
                    p = pk[h, i]
                    grad = late[h][...].reshape(PLANE, HEAD_DIM)
                v = dot(p.astype(BF16), grad)
                gv = v if gv is None else gv + v
                gsc = (p * (gpk[h, i] - row(it, 2 + h))).astype(BF16)
                k = dot(gsc, query)
                gk = k if gk is None else gk + k
            dqkv[:, lanes(HEADS_DEV + h)] = turn(gk * scale, True).astype(BF16)
            dqkv[:, lanes(2 * HEADS_DEV + h)] = gv.astype(BF16)

    def own_queries(it):
        @pl.when(yl == 0)
        def _():
            query_side(it, ((kb, vb),))

        @pl.when(yl == 1)
        def _():
            query_side(it, ((kb, vb), (oa, ob)))

    most = gs.at[pl.ds(0, len(SEQ_STEPS))]
    gain_seq = remote(most, most, gss.at[0], gsr.at[0], partner)
    most = gt.at[pl.ds(0, 7)]
    gain_chip = remote(most, most, gts.at[0], gtr.at[0], partner)

    def backward(it):
        own = (qb, gb, (ga2, gb2))
        other = (oa, ob, (oa2, ob2))

        @pl.when(yl == 0)
        def _():
            over_wait(it)
            key_scores(it, (own, other))

        @pl.when(yl == 1)
        def _():
            key_scores(it, (own,))

        stats_all(it).wait_recv()

        @pl.when(yl == 0)
        def _():
            key_side(it, (own, other), (yl, 1 - yl))

        @pl.when(yl == 1)
        def _():
            key_side(it, (own,), (yl,))

        wide = HALF // CHUNKS
        gives = []
        for j in range(CHUNKS):
            cols = pl.ds(pl.multiple_of((1 - c) * HALF + j * wide, wide), wide)
            tot[it, j] = dot(dqkv[...], wqkv_t[:, cols]).astype(BF16).reshape(CHIPS, CROWS, wide)
            cp = remote(tot.at[it, j], drv.at[it, j], gvs.at[it, j], gvr.at[it, j], partner)
            cp.start()
            gives.append(cp)
        sends = []
        last_term = it == ITERS - 1
        for j in range(CHUNKS):
            cols = pl.ds(pl.multiple_of(c * HALF + j * wide, wide), wide)
            pair[j] = dot(dqkv[...], wqkv_t[:, cols]).reshape(CHIPS, CROWS, wide)

        def scatter(j):
            for k in range(7):
                a, b = chip_to(k)
                rsrc[it, j, k] = pair[j, a * NX + b].astype(BF16)
                remote(
                    rsrc.at[it, j, k], rrv.at[it, j, k], rss.at[it, j], rsr.at[it, j],
                    dev(yh_=a, x_=b),
                ).start()
            sends.append(
                remote(rsrc.at[it, j], rrv.at[it, j], rss.at[it, j], rsr.at[it, j], partner)
            )

        for j in range(CHUNKS):
            gives[j].wait_recv()
            pair[j] += drv[it, j].astype(F32)
            if not last_term:
                scatter(j)
        for j in range(CHUNKS):
            cols = pl.ds(pl.multiple_of(c * HALF + j * wide, wide), wide)
            here = pl.ds(j * wide, wide)
            term = jnp.sum(
                (pair[j] * agx[:, :, cols].astype(F32)).reshape(TOK, wide), axis=0, keepdims=True
            )
            gacc[:, here] = term if it == 0 else gacc[:, here] + term
            gn[:, here] = pair[j, chip]
        if last_term:
            gs[s] = gacc[...]
            for k in range(len(SEQ_STEPS)):
                a, b = seq_to(k)
                remote(gs.at[s], gs.at[s], gss.at[0], gsr.at[0], dev(yl_=a, z_=b)).start()
            for j in range(CHUNKS):
                scatter(j)
            gain_seq.wait_recv()
            acc = gs[0]
            for i in range(1, NY * NZ):
                acc = acc + gs[i]
            gt[chip] = acc
            for k in range(7):
                a, b = chip_to(k)
                remote(
                    gt.at[chip], gt.at[chip], gts.at[0], gtr.at[0], dev(yh_=a, x_=b)
                ).start()
            sent.extend([gain_seq, gain_chip])
        for j in range(CHUNKS):
            here = pl.ds(j * wide, wide)
            sends[j].wait_recv()
            total = gn[:, here]
            for k in range(7):
                total = total + rrv[it, j, k].astype(F32)
            gn[:, here] = total

        grad_normed = gn[...]
        scaled = sc16[...]
        weighted = gain_half * grad_normed
        inl[it] = jnp.broadcast_to(
            jnp.sum(weighted * scaled, axis=1, keepdims=True), (CROWS, 128)
        )
        share = remote(inl.at[it], inr.at[it], d2s.at[5 + it], d2r.at[5 + it], partner)
        share.start()
        share.wait_recv()
        inner = (inl[it] + inr[it])[:, 0:1]
        cot = ir16[:, 0:1] * (weighted - scaled * (inner / D))
        adj16[...] = (in16[...] if it == 0 else adj16[...]) + cot
        if it == 0:
            agc[chip, :, own_half] = cot.astype(BF16)
            gather_start(agc, 2)
        sent.extend(gives + [share] + sends)

    stats_start(0)
    ring_step(4, Q, G)
    own_queries(0)
    backward(0)

    ring_sent(K, V, Q, G, OA)
    gather_pass(agc, 2)
    gather_finish(agc, 2)
    grad2 = dot(agc[...].reshape(TOK, D), wo_t[...]).astype(BF16)
    ga2[z] = grad2[:, :HEAD_DIM]
    gb2[z] = grad2[:, HEAD_DIM:]

    far_send(OA2, 2)
    far_send(GB, 2)

    @pl.when(yl == 1)
    def _():
        cross(ga2, oa2, 1).start()

    far_send(GA, 2)
    far_send(GB, 1)
    send_over(GB, z)
    far_send(GA, 1)
    for h in range(HEADS_DEV):
        st[1, s, pl.ds(2 + h, 1), :] = as_row(
            jnp.sum(
                own_grad(1, h).astype(F32) * att[:, lanes(h)].astype(F32), axis=1, keepdims=True
            )
        )
    stats_start(1)
    own_queries(1)
    far_take(GB, 2)
    far_take(OA2, 2)
    far_take(GA, 2)

    @pl.when(yl == 0)
    def _():
        cross(oa2, oa2, 1).wait_recv()

    far_send(OA2, 1)
    far_take(GB, 1)
    far_take(GA, 1)
    far_take(GB, 3, 4)
    far_take(OA2, 1, 3, 4)
    far_take(GA, 3, 4)
    backward(1)

    back = remote(adj16.at[far_rows, :], adjr, d2s.at[7], d2r.at[7], partner)
    back.start()
    adj_ref[:, own_half] = adj16[own_rows, :]
    gain_chip.wait_recv()
    acc = gt[0]
    for i in range(1, CHIPS):
        acc = acc + gt[i]
    gh[0] = acc / gain_half * (NY * NZ * TOK) ** (-0.5)
    last = remote(gh.at[0], gh.at[1], d2s.at[8], d2r.at[8], partner)
    last.start()
    back.wait_recv()
    adj_ref[:, far_half] = adjr[...]
    gg_ref[:, own_half] = gh[0]
    last.wait_recv()
    gg_ref[:, far_half] = gh[1]
    far_sent(GA, GB, OA2)
    gather_sent(agx, 0)
    gather_sent(agi, 1)
    gather_sent(agc, 2)

    @pl.when(yl == 0)
    def _():
        cross(kb, oa, 0).wait_send()

    @pl.when(yl == 1)
    def _():
        cross(qb, oa, 0).wait_send()

    @pl.when(yl == 1)
    def _():
        cross(ga2, oa2, 1).wait_send()

    for cp in sent + [stats_all(0), stats_all(1), back, last]:
        cp.wait_send()


def scratch():
    v = pltpu.VMEM
    dma = pltpu.SemaphoreType.DMA
    wide = HALF // CHUNKS
    block = (NZ, TOK, WIDTH)
    half_block = (NZ, TOK, HEAD_DIM)
    return [
        v((ROWS, D), BF16), v((ROWS, D), BF16), v((1, D), F32), v((1, HEAD_DIM), F32),
        v((NBLK, NBLK), jnp.int32),
        v((D, 3 * WIDTH), BF16), v((WIDTH, D), BF16), v((3 * WIDTH, D), BF16), v((D, WIDTH), BF16),
        v((TOK, HEAD_DIM), F32), v((TOK, HEAD_DIM), F32),
        v((2, ROWS, D), F32), v((CROWS, HALF), F32), v((CROWS, HALF), F32), v((CROWS, 128), F32),
        v((ROWS, 128), F32),
        v((CHIPS, CROWS, D), BF16), v((CHIPS, CROWS, D), BF16), v((CHIPS, CROWS, D), BF16),
        v((HEADS_DEV, 2, TOK, PLANE), F32),
        v(block, BF16), v(block, BF16), v(block, BF16), v(block, BF16), v(block, BF16),
        v(block, BF16),
        v(half_block, BF16), v(half_block, BF16), v(half_block, BF16), v(half_block, BF16),
        v((ITERS, NY * NZ, 8, TOK), F32),
        v((2, TOK, PLANE), F32), v((2, TOK, PLANE), F32),
        v((HEADS_DEV, 2, TOK, PLANE), F32), v((HEADS_DEV, 2, TOK, PLANE), F32),
        v((TOK, WIDTH), BF16), v((TOK, 3 * WIDTH), BF16),
        v((ITERS, CHUNKS, CHIPS, CROWS, wide), BF16), v((ITERS, CHUNKS, CHIPS, CROWS, wide), BF16),
        v((ITERS, CHUNKS, 7, CROWS, wide), BF16), v((ITERS, CHUNKS, 7, CROWS, wide), BF16),
        v((CHUNKS, CHIPS, CROWS, wide), F32), v((CROWS, HALF), F32),
        v((ITERS, CROWS, 128), F32), v((ITERS, CROWS, 128), F32),
        v((CROWS, HALF), F32), v((ROWS, HALF), F32), v((1, HALF), F32),
        v((CHIPS, 1, HALF), F32), v((NY * NZ, 1, HALF), F32), v((2, 1, HALF), F32),
        dma((5,)), dma((4,)), dma((3,)), dma((3, 7)), dma((3,)), dma((3,)), dma((9,)), dma((9,)),
        dma((5, 2, 4)), dma((5, 2, 4)), dma((2,)), dma((2,)), dma((2,)), dma((2,)),
        dma((ITERS,)), dma((ITERS,)), dma((ITERS, CHUNKS)), dma((ITERS, CHUNKS)),
        dma((ITERS, CHUNKS)), dma((ITERS, CHUNKS)),
        dma((1,)), dma((1,)), dma((1,)), dma((1,)),
    ]


def body(
    fixed_point, incoming, norm_gain, query_weight, key_weight, value_weight, out_weight, layout
):
    pair = np.arange(HEAD_DIM) % (HEAD_DIM // 2)
    freq = jnp.asarray(THETA ** (-2.0 * pair / HEAD_DIM), F32)
    vmem = pl.BlockSpec(memory_space=pltpu.VMEM)
    hbm = pl.BlockSpec(memory_space=pl.ANY)
    adjoint, gain = pl.pallas_call(
        kernel,
        out_shape=(
            jax.ShapeDtypeStruct((ROWS, D), F32),
            jax.ShapeDtypeStruct((1, D), F32),
        ),
        in_specs=[hbm] * 9,
        out_specs=(vmem, vmem),
        scratch_shapes=scratch(),
        compiler_params=pltpu.CompilerParams(
            collective_id=0, has_side_effects=True, vmem_limit_bytes=62 * 1024 * 1024
        ),
        name="deq_backward",
    )(
        fixed_point, incoming, norm_gain[None, :], freq[None, :], layout,
        query_weight, key_weight, value_weight, out_weight,
    )
    return adjoint, gain[0]


def solution(mesh):
    split = Mesh(mesh.devices.reshape(NY, NZ, NH, NX, NC), AXES)
    in_specs = (
        P(SEQ_TENSOR, None),
        P(SEQ_TENSOR, None),
        P(),
        P(None, TENSOR),
        P(None, TENSOR),
        P(None, TENSOR),
        P(TENSOR, None),
        P(),
    )
    out_specs = (P(SEQ_TENSOR, None), P())
    return jax.shard_map(body, mesh=split, in_specs=in_specs, out_specs=out_specs, check_vma=False)
```

```python
import functools

import jax
import jax.numpy as jnp
import numpy as np
from jax import lax
from jax.experimental import pallas as pl
from jax.experimental.pallas import tpu as pltpu
from jax.sharding import Mesh
from jax.sharding import PartitionSpec as P

HEAD_DIM = 128
BLK = 64
ITERS = 2
EPS = 1e-05
THETA = 10000.0
MASKED = -1e30
AXES = ("seq_0", "seq_1", "tensor_0", "tensor_1", "tensor_2")
TENSOR = ("tensor_0", "tensor_1", "tensor_2")
SEQ = ("seq_0", "seq_1")
SEQ_TENSOR = AXES
MESH = pl.DeviceIdType.MESH
F32, BF16 = jnp.float32, jnp.bfloat16

NY, NZ, NH, NX, NC = 2, 8, 2, 4, 2
CHIPS = NH * NX
ROWS = 8
CROWS = NC * ROWS
TOK = CHIPS * CROWS
PLANE = NZ * TOK
D = 4096
HALF = D // 2
HEADS_DEV = 2
WIDTH = HEADS_DEV * HEAD_DIM
NBLK = 32

CHIP_STEPS = ((1, 2), (1, 1), (1, 3), (0, 2), (1, 0), (0, 1), (0, 3))
SEQ_STEPS = tuple(
    (a, b % NZ) for b in (4, 3, -3, 2, -2, 1, -1, 0) for a in (1, 0) if (a, b) != (0, 0)
)
K, V, Q, G, OA, GA, GB, OA2 = range(8)
CHUNKS = 2

NN = (((1,), (0,)), ((), ()))
NT = (((1,), (1,)), ((), ()))


def dot(a, b, dims=NN):
    return lax.dot_general(a, b, dims, preferred_element_type=F32)


def kernel(
    point_hbm, inc_hbm, gain_hbm, freq_hbm, lay_hbm, wq_hbm, wk_hbm, wv_hbm, wo_hbm,
    adj_ref, gg_ref,
    point_ref, inc_ref, gain_ref, freq_ref, lay_ref,
    wqkv, wo, wqkv_t, wo_t, cosb, sinb, loc, sc16, in16, ir16, irl, agx, agi, agc,
    gpk, kb, vb, qb, gb, oa, ob, ga2, gb2, oa2, ob2, st, bq, bk, pq, pk, att, dqkv,
    tot, drv, rsrc, rrv, pair, gn, inl, inr, adj16, adjr, gacc, gt, gs, gh,
    out_sem, in_sem, w_sem, ags, agr, fws, fwr, d2s, d2r, rgs, rgr, yxs, yxr, yfs, yfr, sts, str_,
    gvs, gvr, rss, rsr, gts, gtr, gss, gsr,
):
    yl, z, yh, x, c = (lax.axis_index(a) for a in AXES)
    chip = yh * NX + x
    s = yl * NZ + z
    scale = HEAD_DIM ** (-0.5)

    def dev(yl_=None, z_=None, yh_=None, x_=None, c_=None):
        pick = lambda a, b: a if b is None else b
        return (pick(yl, yl_), pick(z, z_), pick(yh, yh_), pick(x, x_), pick(c, c_))

    partner = dev(c_=1 - c)
    sent = []
    own_half = pl.ds(pl.multiple_of(c * HALF, HALF), HALF)
    far_half = pl.ds(pl.multiple_of((1 - c) * HALF, HALF), HALF)
    own_rows = pl.ds(pl.multiple_of(c * ROWS, ROWS), ROWS)
    far_rows = pl.ds(pl.multiple_of((1 - c) * ROWS, ROWS), ROWS)

    def remote(src, dst, ssem, rsem, to):
        return pltpu.make_async_remote_copy(
            src_ref=src, dst_ref=dst, send_sem=ssem, recv_sem=rsem, device_id=to, device_id_type=MESH
        )

    def chip_to(k):
        a, b = CHIP_STEPS[k]
        return lax.rem(yh + a, NH), lax.rem(x + b, NX)

    def chip_from(k):
        a, b = CHIP_STEPS[k]
        return lax.rem(yh + NH - a, NH) * NX + lax.rem(x + NX - b, NX)

    def seq_to(k):
        a, b = SEQ_STEPS[k]
        return lax.rem(yl + a, NY), lax.rem(z + b, NZ)

    def seq_from(k):
        a, b = SEQ_STEPS[k]
        return lax.rem(yl + NY - a, NY) * NZ + lax.rem(z + NZ - b, NZ)

    small = [
        pltpu.make_async_copy(h, v, in_sem.at[i])
        for i, (h, v) in enumerate(
            ((point_hbm, point_ref), (inc_hbm, inc_ref), (gain_hbm, gain_ref),
             (freq_hbm, freq_ref), (lay_hbm, lay_ref))
        )
    ]
    for cp in small:
        cp.start()
    loads = [
        pltpu.make_async_copy(h, wqkv.at[:, pl.ds(i * WIDTH, WIDTH)], w_sem.at[i])
        for i, h in enumerate((wq_hbm, wk_hbm, wv_hbm))
    ]
    loads.append(pltpu.make_async_copy(wo_hbm, wo, w_sem.at[3]))

    @pl.loop(0, NZ)
    def _(i):
        for buf in (kb, vb, qb, gb):
            buf[i] = jnp.zeros((TOK, WIDTH), BF16)
        for buf in (ga2, gb2):
            buf[i] = jnp.zeros((TOK, HEAD_DIM), BF16)

    bar = pltpu.get_barrier_semaphore()
    greet = [partner]
    for k in range(len(CHIP_STEPS)):
        a, b = chip_to(k)
        greet.append(dev(yh_=a, x_=b))
    for k in range(len(SEQ_STEPS)):
        a, b = seq_to(k)
        greet.append(dev(yl_=a, z_=b))
    for g in greet:
        pl.semaphore_signal(bar, inc=1, device_id=g, device_id_type=MESH)

    for cp in small:
        cp.wait()
    for cp in loads:
        cp.start()
    pt = point_ref[...].astype(F32)
    inv = lax.rsqrt(jnp.mean(pt * pt, axis=1, keepdims=True) + EPS)
    loc[0] = pt * inv
    loc[1] = inc_ref[...].astype(F32)
    irl[...] = jnp.broadcast_to(inv, (ROWS, 128))
    pl.semaphore_wait(bar, len(greet))

    swaps = [
        remote(loc.at[0, :, far_half], sc16.at[own_rows, :], d2s.at[0], d2r.at[0], partner),
        remote(loc.at[1, :, far_half], in16.at[own_rows, :], d2s.at[1], d2r.at[1], partner),
        remote(irl, ir16.at[own_rows, :], d2s.at[2], d2r.at[2], partner),
    ]
    for cp in swaps:
        cp.start()
    sc16[own_rows, :] = loc[0, :, own_half]
    in16[own_rows, :] = loc[1, :, own_half]
    ir16[own_rows, :] = irl[...]
    gain_half = gain_ref[:, own_half]
    for cp, buf in zip(swaps, (sc16, in16, ir16)):
        cp.wait_send()
    remote(loc.at[0, :, far_half], sc16.at[far_rows, :], d2s.at[0], d2r.at[0], partner).wait_recv()
    remote(loc.at[1, :, far_half], in16.at[far_rows, :], d2s.at[1], d2r.at[1], partner).wait_recv()
    remote(irl, ir16.at[far_rows, :], d2s.at[2], d2r.at[2], partner).wait_recv()

    def gather_start(buf, g):
        mine = buf.at[chip, :, own_half]
        remote(mine, mine, fws.at[g], fwr.at[g], partner).start()
        for k in range(7):
            a, b = chip_to(k)
            remote(mine, mine, ags.at[g], agr.at[g, k], dev(yh_=a, x_=b)).start()

    def gather_pass(buf, g):
        for k in range(7):
            slot = buf.at[chip_from(k), :, own_half]
            remote(slot, slot, ags.at[g], agr.at[g, k], partner).wait_recv()
            remote(slot, slot, fws.at[g], fwr.at[g], partner).start()

    def gather_finish(buf, g):
        far = buf.at[:, :, far_half]
        remote(far, far, fws.at[g], fwr.at[g], partner).wait_recv()

    def gather_sent(buf, g):
        own = buf.at[:, :, own_half]
        remote(own, own, fws.at[g], fwr.at[g], partner).wait_send()
        seven = buf.at[pl.ds(0, 7), :, own_half]
        remote(seven, seven, ags.at[g], agr.at[g, 0], partner).wait_send()

    agx[chip, :, own_half] = (gain_half * sc16[...]).astype(BF16)
    gather_start(agx, 0)
    agi[chip, :, own_half] = in16[...].astype(BF16)

    row_tok = s * TOK + lax.broadcasted_iota(jnp.int32, (TOK, 1), 0)
    row_blk = row_tok // BLK
    blk_col = lax.broadcasted_iota(jnp.int32, (TOK, NBLK), 1)
    lay = jnp.where(lay_ref[...] > 0, 1.0, 0.0).astype(BF16)
    onehot = jnp.where(blk_col == row_blk, 1.0, 0.0).astype(BF16)
    chosen_q = jnp.where(blk_col < row_blk, dot(onehot, lay), 0.0).astype(BF16)
    chosen_k = jnp.where(blk_col > row_blk, dot(onehot, lay, NT), 0.0).astype(BF16)
    for part in range(2):
        plane = yl if part == 0 else 1 - yl
        col_blk = plane * (PLANE // BLK) + lax.broadcasted_iota(jnp.int32, (NBLK, PLANE), 1) // BLK
        spread = jnp.where(lax.broadcasted_iota(jnp.int32, (NBLK, PLANE), 0) == col_blk, 1.0, 0.0)
        spread = spread.astype(BF16)
        col_tok = plane * PLANE + lax.broadcasted_iota(jnp.int32, (1, PLANE), 1)
        same = row_blk == col_tok // BLK
        ok = (dot(chosen_q, spread) > 0.5) | (same & (col_tok <= row_tok))
        bq[part] = jnp.where(ok, 0.0, MASKED)
        ok = (dot(chosen_k, spread) > 0.5) | (same & (col_tok >= row_tok))
        bk[part] = jnp.where(ok, 0.0, MASKED)

    angle = row_tok.astype(F32) * freq_ref[...]
    lower = lax.broadcasted_iota(jnp.int32, (TOK, HEAD_DIM), 1) < HEAD_DIM // 2
    cosb[...] = jnp.cos(angle)
    sine = jnp.sin(angle)
    sinb[...] = jnp.where(lower, -sine, sine)

    def turn(v, back=False):
        turned = pltpu.roll(v, HEAD_DIM // 2, 1) * sinb[...]
        return v * cosb[...] - turned if back else v * cosb[...] + turned

    for cp in loads:
        cp.wait()

    @pl.loop(0, D // 512)
    def _(j):
        rows = pl.ds(pl.multiple_of(j * 512, 512), 512)
        wqkv_t[:, rows] = jnp.transpose(wqkv[rows, :])
        wo_t[rows, :] = jnp.transpose(wo[:, rows])

    gather_start(agi, 1)
    gather_pass(agx, 0)
    gather_finish(agx, 0)

    def depth(sgn):
        return NZ // 2 - c if sgn > 0 else NZ // 2 - 1 + c

    def wanted(stream, sgn, d, at):
        full = depth(sgn)
        near = d <= full
        if stream == OA:
            return near
        origin = lax.rem(at - sgn * d + NZ, NZ)
        if (stream in (K, V)) == (sgn > 0):
            some = (at >= d) if sgn > 0 else (at + d <= NZ - 1)
        else:
            some = (origin + full >= NZ) if sgn > 0 else (origin < full)
        if stream == V:
            some = some | (yl == 0)
        if stream == G:
            some = some | (yl == 1)
        return near & some

    bufs = (kb, vb, qb, gb, oa, ga2, gb2, oa2)
    slot_of = {GA: K, GB: V, OA2: OA}

    def hop(stream, sgn, d, at):
        block = bufs[stream].at[lax.rem(at - sgn * (d - 1) + NZ, NZ)]
        to = dev(z_=lax.rem(z + sgn + NZ, NZ))
        i = 0 if sgn > 0 else 1
        return remote(block, block, rgs.at[stream, i, d - 1], rgr.at[stream, i, d - 1], to)

    def send_hop(stream, sgn, d):
        @pl.when(wanted(stream, sgn, d, lax.rem(z + sgn + NZ, NZ)))
        def _():
            hop(stream, sgn, d, z).start()

    across = dev(yl_=1 - yl)

    def over(stream, origin):
        dst, n = (ob2, 1) if stream == GB else (ob, 0)
        return remote(
            bufs[stream].at[origin], dst.at[origin], yfs.at[n], yfr.at[n], across
        )

    def over_sent(stream):
        @pl.when(yl == (0 if stream == V else 1))
        def _():
            n = 1 if stream == GB else 0
            remote(bufs[stream], ob2 if n else ob, yfs.at[n], yfr.at[n], across).wait_send()

    def send_over(stream, origin):
        @pl.when(yl == (0 if stream == V else 1))
        def _():
            over(stream, origin).start()

    def take_hop(stream, sgn, d):
        @pl.when(wanted(stream, sgn, d, z))
        def _():
            hop(stream, sgn, d, lax.rem(z - sgn + NZ, NZ)).wait_recv()
            if stream in (V, G, GB):
                send_over(stream, lax.rem(z - sgn * d + NZ, NZ))

    def ring_start(stream):
        for sgn in (1, -1):
            send_hop(stream, sgn, 1)
        if stream in (V, G, GB):
            send_over(stream, z)

    def ring_step(d, *streams):
        for stream in streams:
            for sgn in (1, -1):
                take_hop(stream, sgn, d)
                if d < NZ // 2:
                    send_hop(stream, sgn, d + 1)

    def ring_sent(*streams):
        for stream in streams:
            for d in range(1, NZ // 2 + 1):
                for sgn in (1, -1):

                    @pl.when(wanted(stream, sgn, d, lax.rem(z + sgn + NZ, NZ)))
                    def _():
                        hop(stream, sgn, d, z).wait_send()

            if stream in (V, G):
                over_sent(stream)

    def over_wait(n):
        buf = ob2 if n else ob
        remote(buf, buf, yfs.at[n], yfr.at[n], across).wait_recv()

    def wanted2(stream, sgn, d, at):
        full = depth(sgn)
        near = d <= full
        if stream == OA2:
            return near & (yl == 0)
        origin = lax.rem(at - sgn * d + NZ, NZ)
        if sgn < 0:
            some = origin >= d
        else:
            some = origin + (full if d == 2 else d) >= NZ
        if stream == GB:
            some = some | (yl == 1)
        return near & some

    def far_hop(stream, sgn, d, at):
        base, step = ((0, 1), (0, 2), (2, 1), (2, 2))[d - 1]
        origin = lax.rem(at - sgn * base + NZ, NZ)
        block = bufs[stream].at[origin]
        z_to = lax.rem(z + sgn * step + NZ, NZ)
        i = 0 if sgn > 0 else 1
        n = slot_of[stream]
        sems = rgs.at[n, i, d - 1], rgr.at[n, i, d - 1]
        if stream == OA2 and d == 2:
            return remote(ga2.at[origin], block, *sems, dev(yl_=1 - yl, z_=z_to))
        return remote(block, block, *sems, dev(z_=z_to))

    def far_cond(stream, sgn, d):
        step = (1, 2, 1, 2)[d - 1]
        if stream == OA2 and d == 2:
            return yl == 1
        return wanted2(stream, sgn, d, lax.rem(z + sgn * step + NZ, NZ))

    def far_send(stream, *ds):
        for d in ds:
            for sgn in (1, -1):

                @pl.when(far_cond(stream, sgn, d))
                def _():
                    far_hop(stream, sgn, d, z).start()

    def far_take(stream, *ds):
        for d in ds:
            for sgn in (1, -1):

                @pl.when(wanted2(stream, sgn, d, z))
                def _():
                    step = (1, 2, 1, 2)[d - 1]
                    far_hop(stream, sgn, d, lax.rem(z - sgn * step + NZ, NZ)).wait_recv()
                    if stream == GB:
                        send_over(stream, lax.rem(z - sgn * d + NZ, NZ))

                if d == 2:
                    for e in (4, 3):

                        @pl.when(far_cond(stream, sgn, e))
                        def _():
                            far_hop(stream, sgn, e, z).start()

    def far_sent(*streams):
        for stream in streams:
            for d in range(1, NZ // 2 + 1):
                for sgn in (1, -1):

                    @pl.when(far_cond(stream, sgn, d))
                    def _():
                        far_hop(stream, sgn, d, z).wait_send()

            if stream == GB:
                over_sent(stream)

    def cross(src, dst, i):
        return remote(src.at[z], dst.at[z], yxs.at[i], yxr.at[i], across)

    def project(i):
        return dot(agx[...].reshape(TOK, D), wqkv[:, i * WIDTH : (i + 1) * WIDTH])

    def turned_into(buf, v):
        for h in range(HEADS_DEV):
            buf[z, :, h * HEAD_DIM : (h + 1) * HEAD_DIM] = turn(
                v[:, h * HEAD_DIM : (h + 1) * HEAD_DIM]
            ).astype(BF16)

    turned_into(kb, project(1))

    @pl.when(yl == 0)
    def _():
        cross(kb, oa, 0).start()

    ring_start(K)
    vb[z] = project(2).astype(BF16)
    ring_start(V)
    turned_into(qb, project(0))

    @pl.when(yl == 1)
    def _():
        cross(qb, oa, 0).start()

    ring_step(1, K)
    gather_pass(agi, 1)
    ring_step(1, V)
    cross(oa, oa, 0).wait_recv()
    ring_start(OA)
    ring_start(Q)
    gather_finish(agi, 1)
    gb[z] = dot(agi[...].reshape(TOK, D), wo_t[...]).astype(BF16)
    ring_start(G)
    ring_step(1, OA)
    ring_step(2, K)
    ring_step(2, V)
    ring_step(1, G)
    ring_step(1, Q)
    ring_step(2, OA)
    ring_step(3, K)
    ring_step(3, V)
    ring_step(2, G)
    ring_step(2, Q)
    ring_step(3, OA)
    ring_step(4, K)
    ring_step(4, V)
    ring_step(3, G)
    ring_step(3, Q)
    ring_step(4, OA)
    @pl.when(yl == 1)
    def _():
        over_wait(0)

    def lanes(h):
        return pl.ds(h * HEAD_DIM, HEAD_DIM)

    def rows_of(buf, h):
        return buf[:, :, lanes(h)].reshape(PLANE, HEAD_DIM)

    def as_row(col):
        return jnp.transpose(jnp.broadcast_to(col, (TOK, TOK)))[0:1, :]

    def forward(parts):
        for h in range(HEADS_DEV):
            query = qb[z, :, lanes(h)]
            top = None
            for i, (buf, _) in enumerate(parts):
                sc = dot(query, rows_of(buf, h), NT) * scale + bq[i]
                pq[h, i] = sc
                m = jnp.max(sc, axis=1, keepdims=True)
                top = m if top is None else jnp.maximum(top, m)
            total = None
            for i in range(len(parts)):
                e = jnp.exp(pq[h, i] - top)
                pq[h, i] = e
                l = jnp.sum(e, axis=1, keepdims=True)
                total = l if total is None else total + l
            inv_total = 1.0 / total
            out = None
            for i, (_, buf) in enumerate(parts):
                p = pq[h, i] * inv_total
                pq[h, i] = p
                o = dot(p.astype(BF16), rows_of(buf, h))
                out = o if out is None else out + o
            out = out.astype(BF16)
            att[:, lanes(h)] = out
            grad = gb[z, :, lanes(h)]
            st[0, s, pl.ds(h, 1), :] = as_row(top + jnp.log(total))
            st[0, s, pl.ds(2 + h, 1), :] = as_row(
                jnp.sum(grad.astype(F32) * out.astype(F32), axis=1, keepdims=True)
            )

    @pl.when(yl == 0)
    def _():
        forward(((kb, vb),))

    @pl.when(yl == 1)
    def _():
        forward(((kb, vb), (oa, ob)))

    def stats_start(it):
        mine = st.at[it, s]
        for k in range(len(SEQ_STEPS)):
            a, b = seq_to(k)
            remote(mine, mine, sts.at[it], str_.at[it], dev(yl_=a, z_=b)).start()

    def stats_all(it):
        most = st.at[it, pl.ds(0, len(SEQ_STEPS))]
        return remote(most, most, sts.at[it], str_.at[it], partner)

    def own_grad(it, h):
        return gb[z, :, lanes(h)] if it == 0 else (ga2, gb2)[h][z]

    def query_side(it, parts):
        for h in range(HEADS_DEV):
            grad = own_grad(it, h)
            delta = jnp.sum(
                grad.astype(F32) * att[:, lanes(h)].astype(F32), axis=1, keepdims=True
            )
            out = None
            for i, (keys, values) in enumerate(parts):
                gp = dot(grad, rows_of(values, h), NT)
                gsc = (pq[h, i] * (gp - delta)).astype(BF16)
                o = dot(gsc, rows_of(keys, h))
                out = o if out is None else out + o
            dqkv[:, lanes(h)] = turn(out * scale, True).astype(BF16)

    def key_scores(it, parts):
        for h in range(HEADS_DEV):
            for i, (queries, grads, late) in enumerate(parts):
                if it == 0:
                    query = rows_of(queries, h)
                    pk[h, i] = dot(kb[z, :, lanes(h)], query, NT) * scale + bk[i]
                    grad = rows_of(grads, h)
                else:
                    grad = late[h][...].reshape(PLANE, HEAD_DIM)
                gpk[h, i] = dot(vb[z, :, lanes(h)], grad, NT)

    def key_side(it, parts, planes):
        for h in range(HEADS_DEV):
            gk, gv = None, None
            for i, (queries, grads, late) in enumerate(parts):
                row = lambda n, r: jnp.concatenate(
                    [st[n, planes[i] * NZ + j, pl.ds(r, 1), :] for j in range(NZ)], axis=1
                )
                query = rows_of(queries, h)
                if it == 0:
                    p = jnp.exp(pk[h, i] - row(0, h))
                    pk[h, i] = p
                    grad = rows_of(grads, h)
                else:
                    p = pk[h, i]
                    grad = late[h][...].reshape(PLANE, HEAD_DIM)
                v = dot(p.astype(BF16), grad)
                gv = v if gv is None else gv + v
                gsc = (p * (gpk[h, i] - row(it, 2 + h))).astype(BF16)
                k = dot(gsc, query)
                gk = k if gk is None else gk + k
            dqkv[:, lanes(HEADS_DEV + h)] = turn(gk * scale, True).astype(BF16)
            dqkv[:, lanes(2 * HEADS_DEV + h)] = gv.astype(BF16)

    def own_queries(it):
        @pl.when(yl == 0)
        def _():
            query_side(it, ((kb, vb),))

        @pl.when(yl == 1)
        def _():
            query_side(it, ((kb, vb), (oa, ob)))

    most = gs.at[pl.ds(0, len(SEQ_STEPS))]
    gain_seq = remote(most, most, gss.at[0], gsr.at[0], partner)
    most = gt.at[pl.ds(0, 7)]
    gain_chip = remote(most, most, gts.at[0], gtr.at[0], partner)

    def backward(it):
        own = (qb, gb, (ga2, gb2))
        other = (oa, ob, (oa2, ob2))

        @pl.when(yl == 0)
        def _():
            over_wait(it)
            key_scores(it, (own, other))

        @pl.when(yl == 1)
        def _():
            key_scores(it, (own,))

        stats_all(it).wait_recv()

        @pl.when(yl == 0)
        def _():
            key_side(it, (own, other), (yl, 1 - yl))

        @pl.when(yl == 1)
        def _():
            key_side(it, (own,), (yl,))

        wide = HALF // CHUNKS
        gives = []
        for j in range(CHUNKS):
            cols = pl.ds(pl.multiple_of((1 - c) * HALF + j * wide, wide), wide)
            tot[it, j] = dot(dqkv[...], wqkv_t[:, cols]).astype(BF16).reshape(CHIPS, CROWS, wide)
            cp = remote(tot.at[it, j], drv.at[it, j], gvs.at[it, j], gvr.at[it, j], partner)
            cp.start()
            gives.append(cp)
        sends = []
        last_term = it == ITERS - 1
        for j in range(CHUNKS):
            cols = pl.ds(pl.multiple_of(c * HALF + j * wide, wide), wide)
            pair[j] = dot(dqkv[...], wqkv_t[:, cols]).reshape(CHIPS, CROWS, wide)

        def scatter(j):
            for k in range(7):
                a, b = chip_to(k)
                rsrc[it, j, k] = pair[j, a * NX + b].astype(BF16)
                remote(
                    rsrc.at[it, j, k], rrv.at[it, j, k], rss.at[it, j], rsr.at[it, j],
                    dev(yh_=a, x_=b),
                ).start()
            sends.append(
                remote(rsrc.at[it, j], rrv.at[it, j], rss.at[it, j], rsr.at[it, j], partner)
            )

        for j in range(CHUNKS):
            gives[j].wait_recv()
            pair[j] += drv[it, j].astype(F32)
            if not last_term:
                scatter(j)
        for j in range(CHUNKS):
            cols = pl.ds(pl.multiple_of(c * HALF + j * wide, wide), wide)
            here = pl.ds(j * wide, wide)
            term = jnp.sum(
                (pair[j] * agx[:, :, cols].astype(F32)).reshape(TOK, wide), axis=0, keepdims=True
            )
            gacc[:, here] = term if it == 0 else gacc[:, here] + term
            gn[:, here] = pair[j, chip]
        if last_term:
            gs[s] = gacc[...]
            for k in range(len(SEQ_STEPS)):
                a, b = seq_to(k)
                remote(gs.at[s], gs.at[s], gss.at[0], gsr.at[0], dev(yl_=a, z_=b)).start()
            for j in range(CHUNKS):
                scatter(j)
            gain_seq.wait_recv()
            acc = gs[0]
            for i in range(1, NY * NZ):
                acc = acc + gs[i]
            gt[chip] = acc
            for k in range(7):
                a, b = chip_to(k)
                remote(
                    gt.at[chip], gt.at[chip], gts.at[0], gtr.at[0], dev(yh_=a, x_=b)
                ).start()
            sent.extend([gain_seq, gain_chip])
        for j in range(CHUNKS):
            here = pl.ds(j * wide, wide)
            sends[j].wait_recv()
            total = gn[:, here]
            for k in range(7):
                total = total + rrv[it, j, k].astype(F32)
            gn[:, here] = total

        grad_normed = gn[...]
        scaled = sc16[...]
        weighted = gain_half * grad_normed
        inl[it] = jnp.broadcast_to(
            jnp.sum(weighted * scaled, axis=1, keepdims=True), (CROWS, 128)
        )
        share = remote(inl.at[it], inr.at[it], d2s.at[5 + it], d2r.at[5 + it], partner)
        share.start()
        share.wait_recv()
        inner = (inl[it] + inr[it])[:, 0:1]
        cot = ir16[:, 0:1] * (weighted - scaled * (inner / D))
        adj16[...] = (in16[...] if it == 0 else adj16[...]) + cot
        if it == 0:
            agc[chip, :, own_half] = cot.astype(BF16)
            gather_start(agc, 2)
        sent.extend(gives + [share] + sends)

    stats_start(0)
    ring_step(4, Q, G)
    own_queries(0)
    backward(0)

    ring_sent(K, V, Q, G, OA)
    gather_pass(agc, 2)
    gather_finish(agc, 2)
    grad2 = dot(agc[...].reshape(TOK, D), wo_t[...]).astype(BF16)
    ga2[z] = grad2[:, :HEAD_DIM]
    gb2[z] = grad2[:, HEAD_DIM:]

    far_send(OA2, 2)
    far_send(GB, 2)

    @pl.when(yl == 1)
    def _():
        cross(ga2, oa2, 1).start()

    far_send(GA, 2)
    far_send(GB, 1)
    send_over(GB, z)
    far_send(GA, 1)
    for h in range(HEADS_DEV):
        st[1, s, pl.ds(2 + h, 1), :] = as_row(
            jnp.sum(
                own_grad(1, h).astype(F32) * att[:, lanes(h)].astype(F32), axis=1, keepdims=True
            )
        )
    stats_start(1)
    own_queries(1)
    far_take(GB, 2)
    far_take(OA2, 2)
    far_take(GA, 2)

    @pl.when(yl == 0)
    def _():
        cross(oa2, oa2, 1).wait_recv()

    far_send(OA2, 1)
    far_take(GB, 1)
    far_take(GA, 1)
    far_take(GB, 3, 4)
    far_take(OA2, 1, 3, 4)
    far_take(GA, 3, 4)
    backward(1)

    back = remote(adj16.at[far_rows, :], adjr, d2s.at[7], d2r.at[7], partner)
    back.start()
    outs = [pltpu.make_async_copy(adj16.at[own_rows, :], adj_ref.at[:, own_half], out_sem.at[0])]
    outs[0].start()
    gain_chip.wait_recv()
    acc = gt[0]
    for i in range(1, CHIPS):
        acc = acc + gt[i]
    gh[0] = acc / gain_half * (NY * NZ * TOK) ** (-0.5)
    last = remote(gh.at[0], gh.at[1], d2s.at[8], d2r.at[8], partner)
    last.start()
    back.wait_recv()
    outs.append(pltpu.make_async_copy(adjr, adj_ref.at[:, far_half], out_sem.at[1]))
    outs[1].start()
    outs.append(pltpu.make_async_copy(gh.at[0], gg_ref.at[:, own_half], out_sem.at[2]))
    outs[2].start()
    last.wait_recv()
    outs.append(pltpu.make_async_copy(gh.at[1], gg_ref.at[:, far_half], out_sem.at[3]))
    outs[3].start()
    far_sent(GA, GB, OA2)
    gather_sent(agx, 0)
    gather_sent(agi, 1)
    gather_sent(agc, 2)

    @pl.when(yl == 0)
    def _():
        cross(kb, oa, 0).wait_send()

    @pl.when(yl == 1)
    def _():
        cross(qb, oa, 0).wait_send()

    @pl.when(yl == 1)
    def _():
        cross(ga2, oa2, 1).wait_send()

    for cp in sent + [stats_all(0), stats_all(1), back, last]:
        cp.wait_send()
    for cp in outs:
        cp.wait()


def scratch():
    v = pltpu.VMEM
    dma = pltpu.SemaphoreType.DMA
    wide = HALF // CHUNKS
    block = (NZ, TOK, WIDTH)
    half_block = (NZ, TOK, HEAD_DIM)
    return [
        v((ROWS, D), BF16), v((ROWS, D), BF16), v((1, D), F32), v((1, HEAD_DIM), F32),
        v((NBLK, NBLK), jnp.int32),
        v((D, 3 * WIDTH), BF16), v((WIDTH, D), BF16), v((3 * WIDTH, D), BF16), v((D, WIDTH), BF16),
        v((TOK, HEAD_DIM), F32), v((TOK, HEAD_DIM), F32),
        v((2, ROWS, D), F32), v((CROWS, HALF), F32), v((CROWS, HALF), F32), v((CROWS, 128), F32),
        v((ROWS, 128), F32),
        v((CHIPS, CROWS, D), BF16), v((CHIPS, CROWS, D), BF16), v((CHIPS, CROWS, D), BF16),
        v((HEADS_DEV, 2, TOK, PLANE), F32),
        v(block, BF16), v(block, BF16), v(block, BF16), v(block, BF16), v(block, BF16),
        v(block, BF16),
        v(half_block, BF16), v(half_block, BF16), v(half_block, BF16), v(half_block, BF16),
        v((ITERS, NY * NZ, 8, TOK), F32),
        v((2, TOK, PLANE), F32), v((2, TOK, PLANE), F32),
        v((HEADS_DEV, 2, TOK, PLANE), F32), v((HEADS_DEV, 2, TOK, PLANE), F32),
        v((TOK, WIDTH), BF16), v((TOK, 3 * WIDTH), BF16),
        v((ITERS, CHUNKS, CHIPS, CROWS, wide), BF16), v((ITERS, CHUNKS, CHIPS, CROWS, wide), BF16),
        v((ITERS, CHUNKS, 7, CROWS, wide), BF16), v((ITERS, CHUNKS, 7, CROWS, wide), BF16),
        v((CHUNKS, CHIPS, CROWS, wide), F32), v((CROWS, HALF), F32),
        v((ITERS, CROWS, 128), F32), v((ITERS, CROWS, 128), F32),
        v((CROWS, HALF), F32), v((ROWS, HALF), F32), v((1, HALF), F32),
        v((CHIPS, 1, HALF), F32), v((NY * NZ, 1, HALF), F32), v((2, 1, HALF), F32),
        dma((4,)), dma((5,)), dma((4,)), dma((3,)), dma((3, 7)), dma((3,)), dma((3,)), dma((9,)), dma((9,)),
        dma((5, 2, 4)), dma((5, 2, 4)), dma((2,)), dma((2,)), dma((2,)), dma((2,)),
        dma((ITERS,)), dma((ITERS,)), dma((ITERS, CHUNKS)), dma((ITERS, CHUNKS)),
        dma((ITERS, CHUNKS)), dma((ITERS, CHUNKS)),
        dma((1,)), dma((1,)), dma((1,)), dma((1,)),
    ]


def hand_over(a_ref, g_ref, a_out, g_out):
    a_out[...] = a_ref[...]
    g_out[...] = g_ref[...]


def body(
    fixed_point, incoming, norm_gain, query_weight, key_weight, value_weight, out_weight, layout
):
    pair = np.arange(HEAD_DIM) % (HEAD_DIM // 2)
    freq = jnp.asarray(THETA ** (-2.0 * pair / HEAD_DIM), F32)
    vmem = pl.BlockSpec(memory_space=pltpu.VMEM)
    hbm = pl.BlockSpec(memory_space=pl.ANY)
    adjoint, gain = pl.pallas_call(
        kernel,
        out_shape=(
            jax.ShapeDtypeStruct((ROWS, D), F32),
            jax.ShapeDtypeStruct((1, D), F32),
        ),
        in_specs=[hbm] * 9,
        out_specs=(hbm, hbm),
        scratch_shapes=scratch(),
        compiler_params=pltpu.CompilerParams(
            collective_id=0, has_side_effects=True, vmem_limit_bytes=62 * 1024 * 1024
        ),
        name="deq_backward",
    )(
        fixed_point, incoming, norm_gain[None, :], freq[None, :], layout,
        query_weight, key_weight, value_weight, out_weight,
    )
    adjoint, gain = pl.pallas_call(
        hand_over,
        out_shape=(
            jax.ShapeDtypeStruct((ROWS, D), F32),
            jax.ShapeDtypeStruct((1, D), F32),
        ),
        in_specs=[vmem] * 2,
        out_specs=(vmem, vmem),
        name="hand_over",
    )(adjoint, gain)
    return adjoint, gain[0]


def solution(mesh):
    split = Mesh(mesh.devices.reshape(NY, NZ, NH, NX, NC), AXES)
    in_specs = (
        P(SEQ_TENSOR, None),
        P(SEQ_TENSOR, None),
        P(),
        P(None, TENSOR),
        P(None, TENSOR),
        P(None, TENSOR),
        P(TENSOR, None),
        P(),
    )
    out_specs = (P(SEQ_TENSOR, None), P())
    return jax.shard_map(body, mesh=split, in_specs=in_specs, out_specs=out_specs, check_vma=False)
```

```python
import functools

import jax
import jax.numpy as jnp
import numpy as np
from jax import lax
from jax.experimental import pallas as pl
from jax.experimental.pallas import tpu as pltpu
from jax.sharding import Mesh
from jax.sharding import PartitionSpec as P

HEAD_DIM = 128
BLK = 64
ITERS = 2
EPS = 1e-05
THETA = 10000.0
MASKED = -1e30
AXES = ("seq_0", "seq_1", "tensor_0", "tensor_1", "tensor_2")
TENSOR = ("tensor_0", "tensor_1", "tensor_2")
SEQ = ("seq_0", "seq_1")
SEQ_TENSOR = AXES
MESH = pl.DeviceIdType.MESH
F32, BF16 = jnp.float32, jnp.bfloat16

NY, NZ, NH, NX, NC = 2, 8, 2, 4, 2
CHIPS = NH * NX
ROWS = 8
CROWS = NC * ROWS
TOK = CHIPS * CROWS
PLANE = NZ * TOK
D = 4096
HALF = D // 2
HEADS_DEV = 2
WIDTH = HEADS_DEV * HEAD_DIM
NBLK = 32

CHIP_STEPS = ((1, 2), (1, 1), (1, 3), (0, 2), (1, 0), (0, 1), (0, 3))
SEQ_STEPS = tuple(
    (a, b % NZ) for b in (4, 3, -3, 2, -2, 1, -1, 0) for a in (1, 0) if (a, b) != (0, 0)
)
K, V, Q, G, OA, GA, GB, OA2 = range(8)
CHUNKS = 2

NN = (((1,), (0,)), ((), ()))
NT = (((1,), (1,)), ((), ()))


def dot(a, b, dims=NN):
    return lax.dot_general(a, b, dims, preferred_element_type=F32)


def kernel(
    point_hbm, inc_hbm, gain_hbm, freq_hbm, lay_hbm, wq_hbm, wk_hbm, wv_hbm, wo_hbm,
    adj_ref, gg_ref,
    point_ref, inc_ref, gain_ref, freq_ref, lay_ref,
    wqkv, wo, wqkv_t, wo_t, cosb, sinb, loc, sc16, in16, ir16, irl, agx, agi, agc,
    gpk, kb, vb, qb, gb, oa, ob, ga2, gb2, oa2, ob2, st, bq, bk, pq, pk, att, dqkv,
    tot, drv, rsrc, rrv, pair, gn, inl, inr, adj16, adjr, gacc, gt, gs, gh,
    out_sem, in_sem, w_sem, ags, agr, fws, fwr, d2s, d2r, rgs, rgr, yxs, yxr, yfs, yfr, sts, str_,
    gvs, gvr, rss, rsr, gts, gtr, gss, gsr,
):
    yl, z, yh, x, c = (lax.axis_index(a) for a in AXES)
    chip = yh * NX + x
    s = yl * NZ + z
    scale = HEAD_DIM ** (-0.5)

    def dev(yl_=None, z_=None, yh_=None, x_=None, c_=None):
        pick = lambda a, b: a if b is None else b
        return (pick(yl, yl_), pick(z, z_), pick(yh, yh_), pick(x, x_), pick(c, c_))

    partner = dev(c_=1 - c)
    sent = []
    own_half = pl.ds(pl.multiple_of(c * HALF, HALF), HALF)
    far_half = pl.ds(pl.multiple_of((1 - c) * HALF, HALF), HALF)
    own_rows = pl.ds(pl.multiple_of(c * ROWS, ROWS), ROWS)
    far_rows = pl.ds(pl.multiple_of((1 - c) * ROWS, ROWS), ROWS)

    def remote(src, dst, ssem, rsem, to):
        return pltpu.make_async_remote_copy(
            src_ref=src, dst_ref=dst, send_sem=ssem, recv_sem=rsem, device_id=to, device_id_type=MESH
        )

    def chip_to(k):
        a, b = CHIP_STEPS[k]
        return lax.rem(yh + a, NH), lax.rem(x + b, NX)

    def chip_from(k):
        a, b = CHIP_STEPS[k]
        return lax.rem(yh + NH - a, NH) * NX + lax.rem(x + NX - b, NX)

    def seq_to(k):
        a, b = SEQ_STEPS[k]
        return lax.rem(yl + a, NY), lax.rem(z + b, NZ)

    def seq_from(k):
        a, b = SEQ_STEPS[k]
        return lax.rem(yl + NY - a, NY) * NZ + lax.rem(z + NZ - b, NZ)

    small = [
        pltpu.make_async_copy(h, v, in_sem.at[i])
        for i, (h, v) in enumerate(
            ((point_hbm, point_ref), (inc_hbm, inc_ref), (gain_hbm, gain_ref),
             (freq_hbm, freq_ref), (lay_hbm, lay_ref))
        )
    ]
    for cp in small:
        cp.start()
    loads = [
        pltpu.make_async_copy(h, wqkv.at[:, pl.ds(i * WIDTH, WIDTH)], w_sem.at[i])
        for i, h in enumerate((wq_hbm, wk_hbm, wv_hbm))
    ]
    loads.append(pltpu.make_async_copy(wo_hbm, wo, w_sem.at[3]))

    @pl.loop(0, NZ)
    def _(i):
        for buf in (kb, vb, qb, gb):
            buf[i] = jnp.zeros((TOK, WIDTH), BF16)
        for buf in (ga2, gb2):
            buf[i] = jnp.zeros((TOK, HEAD_DIM), BF16)

    bar = pltpu.get_barrier_semaphore()
    greet = [partner]
    for k in range(len(CHIP_STEPS)):
        a, b = chip_to(k)
        greet.append(dev(yh_=a, x_=b))
    for k in range(len(SEQ_STEPS)):
        a, b = seq_to(k)
        greet.append(dev(yl_=a, z_=b))
    for g in greet:
        pl.semaphore_signal(bar, inc=1, device_id=g, device_id_type=MESH)

    for cp in small:
        cp.wait()
    for cp in loads:
        cp.start()
    pt = point_ref[...].astype(F32)
    inv = lax.rsqrt(jnp.mean(pt * pt, axis=1, keepdims=True) + EPS)
    loc[0] = pt * inv
    loc[1] = inc_ref[...].astype(F32)
    irl[...] = jnp.broadcast_to(inv, (ROWS, 128))
    pl.semaphore_wait(bar, len(greet))

    swaps = [
        remote(loc.at[0, :, far_half], sc16.at[own_rows, :], d2s.at[0], d2r.at[0], partner),
        remote(loc.at[1, :, far_half], in16.at[own_rows, :], d2s.at[1], d2r.at[1], partner),
        remote(irl, ir16.at[own_rows, :], d2s.at[2], d2r.at[2], partner),
    ]
    for cp in swaps:
        cp.start()
    sc16[own_rows, :] = loc[0, :, own_half]
    in16[own_rows, :] = loc[1, :, own_half]
    ir16[own_rows, :] = irl[...]
    gain_half = gain_ref[:, own_half]
    for cp, buf in zip(swaps, (sc16, in16, ir16)):
        cp.wait_send()
    remote(loc.at[0, :, far_half], sc16.at[far_rows, :], d2s.at[0], d2r.at[0], partner).wait_recv()
    remote(loc.at[1, :, far_half], in16.at[far_rows, :], d2s.at[1], d2r.at[1], partner).wait_recv()
    remote(irl, ir16.at[far_rows, :], d2s.at[2], d2r.at[2], partner).wait_recv()

    def gather_start(buf, g):
        mine = buf.at[chip, :, own_half]
        remote(mine, mine, fws.at[g], fwr.at[g], partner).start()
        for k in range(7):
            a, b = chip_to(k)
            remote(mine, mine, ags.at[g], agr.at[g, k], dev(yh_=a, x_=b)).start()

    def gather_pass(buf, g):
        for k in range(7):
            slot = buf.at[chip_from(k), :, own_half]
            remote(slot, slot, ags.at[g], agr.at[g, k], partner).wait_recv()
            remote(slot, slot, fws.at[g], fwr.at[g], partner).start()

    def gather_finish(buf, g):
        far = buf.at[:, :, far_half]
        remote(far, far, fws.at[g], fwr.at[g], partner).wait_recv()

    def gather_sent(buf, g):
        own = buf.at[:, :, own_half]
        remote(own, own, fws.at[g], fwr.at[g], partner).wait_send()
        seven = buf.at[pl.ds(0, 7), :, own_half]
        remote(seven, seven, ags.at[g], agr.at[g, 0], partner).wait_send()

    agx[chip, :, own_half] = (gain_half * sc16[...]).astype(BF16)
    gather_start(agx, 0)
    agi[chip, :, own_half] = in16[...].astype(BF16)

    row_tok = s * TOK + lax.broadcasted_iota(jnp.int32, (TOK, 1), 0)
    row_blk = row_tok // BLK
    blk_col = lax.broadcasted_iota(jnp.int32, (TOK, NBLK), 1)
    lay = jnp.where(lay_ref[...] > 0, 1.0, 0.0).astype(BF16)
    onehot = jnp.where(blk_col == row_blk, 1.0, 0.0).astype(BF16)
    chosen_q = jnp.where(blk_col < row_blk, dot(onehot, lay), 0.0).astype(BF16)
    chosen_k = jnp.where(blk_col > row_blk, dot(onehot, lay, NT), 0.0).astype(BF16)
    for part in range(2):
        plane = yl if part == 0 else 1 - yl
        col_blk = plane * (PLANE // BLK) + lax.broadcasted_iota(jnp.int32, (NBLK, PLANE), 1) // BLK
        spread = jnp.where(lax.broadcasted_iota(jnp.int32, (NBLK, PLANE), 0) == col_blk, 1.0, 0.0)
        spread = spread.astype(BF16)
        col_tok = plane * PLANE + lax.broadcasted_iota(jnp.int32, (1, PLANE), 1)
        same = row_blk == col_tok // BLK
        ok = (dot(chosen_q, spread) > 0.5) | (same & (col_tok <= row_tok))
        bq[part] = jnp.where(ok, 0.0, MASKED)
        ok = (dot(chosen_k, spread) > 0.5) | (same & (col_tok >= row_tok))
        bk[part] = jnp.where(ok, 0.0, MASKED)

    angle = row_tok.astype(F32) * freq_ref[...]
    lower = lax.broadcasted_iota(jnp.int32, (TOK, HEAD_DIM), 1) < HEAD_DIM // 2
    cosb[...] = jnp.cos(angle)
    sine = jnp.sin(angle)
    sinb[...] = jnp.where(lower, -sine, sine)

    def turn(v, back=False):
        turned = pltpu.roll(v, HEAD_DIM // 2, 1) * sinb[...]
        return v * cosb[...] - turned if back else v * cosb[...] + turned

    for cp in loads:
        cp.wait()

    @pl.loop(0, D // 512)
    def _(j):
        rows = pl.ds(pl.multiple_of(j * 512, 512), 512)
        wqkv_t[:, rows] = jnp.transpose(wqkv[rows, :])
        wo_t[rows, :] = jnp.transpose(wo[:, rows])

    gather_start(agi, 1)
    gather_pass(agx, 0)
    gather_finish(agx, 0)

    def depth(sgn):
        return NZ // 2 - c if sgn > 0 else NZ // 2 - 1 + c

    def wanted(stream, sgn, d, at):
        full = depth(sgn)
        near = d <= full
        if stream == OA:
            return near
        origin = lax.rem(at - sgn * d + NZ, NZ)
        if (stream in (K, V)) == (sgn > 0):
            some = (at >= d) if sgn > 0 else (at + d <= NZ - 1)
        else:
            some = (origin + full >= NZ) if sgn > 0 else (origin < full)
        if stream == V:
            some = some | (yl == 0)
        if stream == G:
            some = some | (yl == 1)
        return near & some

    bufs = (kb, vb, qb, gb, oa, ga2, gb2, oa2)
    slot_of = {GA: K, GB: V, OA2: OA}

    def hop(stream, sgn, d, at):
        block = bufs[stream].at[lax.rem(at - sgn * (d - 1) + NZ, NZ)]
        to = dev(z_=lax.rem(z + sgn + NZ, NZ))
        i = 0 if sgn > 0 else 1
        return remote(block, block, rgs.at[stream, i, d - 1], rgr.at[stream, i, d - 1], to)

    def send_hop(stream, sgn, d):
        @pl.when(wanted(stream, sgn, d, lax.rem(z + sgn + NZ, NZ)))
        def _():
            hop(stream, sgn, d, z).start()

    across = dev(yl_=1 - yl)

    def over(stream, origin):
        dst, n = (ob2, 1) if stream == GB else (ob, 0)
        return remote(
            bufs[stream].at[origin], dst.at[origin], yfs.at[n], yfr.at[n], across
        )

    def over_sent(stream):
        @pl.when(yl == (0 if stream == V else 1))
        def _():
            n = 1 if stream == GB else 0
            remote(bufs[stream], ob2 if n else ob, yfs.at[n], yfr.at[n], across).wait_send()

    def send_over(stream, origin):
        @pl.when(yl == (0 if stream == V else 1))
        def _():
            over(stream, origin).start()

    def take_hop(stream, sgn, d):
        @pl.when(wanted(stream, sgn, d, z))
        def _():
            hop(stream, sgn, d, lax.rem(z - sgn + NZ, NZ)).wait_recv()
            if stream in (V, G, GB):
                send_over(stream, lax.rem(z - sgn * d + NZ, NZ))

    def ring_start(stream):
        for sgn in (1, -1):
            send_hop(stream, sgn, 1)
        if stream in (V, G, GB):
            send_over(stream, z)

    def ring_step(d, *streams):
        for stream in streams:
            for sgn in (1, -1):
                take_hop(stream, sgn, d)
                if d < NZ // 2:
                    send_hop(stream, sgn, d + 1)

    def ring_sent(*streams):
        for stream in streams:
            for d in range(1, NZ // 2 + 1):
                for sgn in (1, -1):

                    @pl.when(wanted(stream, sgn, d, lax.rem(z + sgn + NZ, NZ)))
                    def _():
                        hop(stream, sgn, d, z).wait_send()

            if stream in (V, G):
                over_sent(stream)

    def over_wait(n):
        buf = ob2 if n else ob
        remote(buf, buf, yfs.at[n], yfr.at[n], across).wait_recv()

    def wanted2(stream, sgn, d, at):
        full = depth(sgn)
        near = d <= full
        if stream == OA2:
            return near & (yl == 0)
        origin = lax.rem(at - sgn * d + NZ, NZ)
        if sgn < 0:
            some = origin >= d
        else:
            some = origin + (full if d == 2 else d) >= NZ
        if stream == GB:
            some = some | (yl == 1)
        return near & some

    def far_hop(stream, sgn, d, at):
        base, step = ((0, 1), (0, 2), (2, 1), (2, 2))[d - 1]
        origin = lax.rem(at - sgn * base + NZ, NZ)
        block = bufs[stream].at[origin]
        z_to = lax.rem(z + sgn * step + NZ, NZ)
        i = 0 if sgn > 0 else 1
        n = slot_of[stream]
        sems = rgs.at[n, i, d - 1], rgr.at[n, i, d - 1]
        if stream == OA2 and d == 2:
            return remote(ga2.at[origin], block, *sems, dev(yl_=1 - yl, z_=z_to))
        return remote(block, block, *sems, dev(z_=z_to))

    def far_cond(stream, sgn, d):
        step = (1, 2, 1, 2)[d - 1]
        if stream == OA2 and d == 2:
            return yl == 1
        return wanted2(stream, sgn, d, lax.rem(z + sgn * step + NZ, NZ))

    def far_send(stream, *ds):
        for d in ds:
            for sgn in (1, -1):

                @pl.when(far_cond(stream, sgn, d))
                def _():
                    far_hop(stream, sgn, d, z).start()

    def far_take(stream, *ds):
        for d in ds:
            for sgn in (1, -1):

                @pl.when(wanted2(stream, sgn, d, z))
                def _():
                    step = (1, 2, 1, 2)[d - 1]
                    far_hop(stream, sgn, d, lax.rem(z - sgn * step + NZ, NZ)).wait_recv()
                    if stream == GB:
                        send_over(stream, lax.rem(z - sgn * d + NZ, NZ))

                if d == 2:
                    for e in (4, 3):

                        @pl.when(far_cond(stream, sgn, e))
                        def _():
                            far_hop(stream, sgn, e, z).start()

    def far_sent(*streams):
        for stream in streams:
            for d in range(1, NZ // 2 + 1):
                for sgn in (1, -1):

                    @pl.when(far_cond(stream, sgn, d))
                    def _():
                        far_hop(stream, sgn, d, z).wait_send()

            if stream == GB:
                over_sent(stream)

    def cross(src, dst, i):
        return remote(src.at[z], dst.at[z], yxs.at[i], yxr.at[i], across)

    def project(i):
        return dot(agx[...].reshape(TOK, D), wqkv[:, i * WIDTH : (i + 1) * WIDTH])

    def turned_into(buf, v):
        for h in range(HEADS_DEV):
            buf[z, :, h * HEAD_DIM : (h + 1) * HEAD_DIM] = turn(
                v[:, h * HEAD_DIM : (h + 1) * HEAD_DIM]
            ).astype(BF16)

    turned_into(kb, project(1))

    @pl.when(yl == 0)
    def _():
        cross(kb, oa, 0).start()

    ring_start(K)
    vb[z] = project(2).astype(BF16)
    ring_start(V)
    turned_into(qb, project(0))

    @pl.when(yl == 1)
    def _():
        cross(qb, oa, 0).start()

    ring_step(1, K)
    gather_pass(agi, 1)
    ring_step(1, V)
    cross(oa, oa, 0).wait_recv()
    ring_start(OA)
    ring_start(Q)
    gather_finish(agi, 1)
    gb[z] = dot(agi[...].reshape(TOK, D), wo_t[...]).astype(BF16)
    ring_start(G)
    ring_step(1, OA)
    ring_step(2, K)
    ring_step(2, V)
    ring_step(1, G)
    ring_step(1, Q)
    ring_step(2, OA)
    ring_step(3, K)
    ring_step(3, V)
    ring_step(2, G)
    ring_step(2, Q)
    ring_step(3, OA)
    ring_step(4, K)
    ring_step(4, V)
    ring_step(3, G)
    ring_step(3, Q)
    ring_step(4, OA)
    @pl.when(yl == 1)
    def _():
        over_wait(0)

    def lanes(h):
        return pl.ds(h * HEAD_DIM, HEAD_DIM)

    def rows_of(buf, h):
        return buf[:, :, lanes(h)].reshape(PLANE, HEAD_DIM)

    def as_row(col):
        return jnp.transpose(jnp.broadcast_to(col, (TOK, TOK)))[0:1, :]

    def forward(parts):
        for h in range(HEADS_DEV):
            query = qb[z, :, lanes(h)]
            top = None
            for i, (buf, _) in enumerate(parts):
                sc = dot(query, rows_of(buf, h), NT) * scale + bq[i]
                pq[h, i] = sc
                m = jnp.max(sc, axis=1, keepdims=True)
                top = m if top is None else jnp.maximum(top, m)
            total = None
            for i in range(len(parts)):
                e = jnp.exp(pq[h, i] - top)
                pq[h, i] = e
                l = jnp.sum(e, axis=1, keepdims=True)
                total = l if total is None else total + l
            inv_total = 1.0 / total
            out = None
            for i, (_, buf) in enumerate(parts):
                p = pq[h, i] * inv_total
                pq[h, i] = p
                o = dot(p.astype(BF16), rows_of(buf, h))
                out = o if out is None else out + o
            out = out.astype(BF16)
            att[:, lanes(h)] = out
            grad = gb[z, :, lanes(h)]
            st[0, s, pl.ds(h, 1), :] = as_row(top + jnp.log(total))
            st[0, s, pl.ds(2 + h, 1), :] = as_row(
                jnp.sum(grad.astype(F32) * out.astype(F32), axis=1, keepdims=True)
            )

    @pl.when(yl == 0)
    def _():
        forward(((kb, vb),))

    @pl.when(yl == 1)
    def _():
        forward(((kb, vb), (oa, ob)))

    def stats_start(it):
        mine = st.at[it, s]
        for k in range(len(SEQ_STEPS)):
            a, b = seq_to(k)
            remote(mine, mine, sts.at[it], str_.at[it], dev(yl_=a, z_=b)).start()

    def stats_all(it):
        most = st.at[it, pl.ds(0, len(SEQ_STEPS))]
        return remote(most, most, sts.at[it], str_.at[it], partner)

    def own_grad(it, h):
        return gb[z, :, lanes(h)] if it == 0 else (ga2, gb2)[h][z]

    def query_side(it, parts):
        for h in range(HEADS_DEV):
            grad = own_grad(it, h)
            delta = jnp.sum(
                grad.astype(F32) * att[:, lanes(h)].astype(F32), axis=1, keepdims=True
            )
            out = None
            for i, (keys, values) in enumerate(parts):
                gp = dot(grad, rows_of(values, h), NT)
                gsc = (pq[h, i] * (gp - delta)).astype(BF16)
                o = dot(gsc, rows_of(keys, h))
                out = o if out is None else out + o
            dqkv[:, lanes(h)] = turn(out * scale, True).astype(BF16)

    def key_scores(it, parts):
        for h in range(HEADS_DEV):
            for i, (queries, grads, late) in enumerate(parts):
                if it == 0:
                    query = rows_of(queries, h)
                    pk[h, i] = dot(kb[z, :, lanes(h)], query, NT) * scale + bk[i]
                    grad = rows_of(grads, h)
                else:
                    grad = late[h][...].reshape(PLANE, HEAD_DIM)
                gpk[h, i] = dot(vb[z, :, lanes(h)], grad, NT)

    def key_side(it, parts, planes):
        for h in range(HEADS_DEV):
            gk, gv = None, None
            for i, (queries, grads, late) in enumerate(parts):
                row = lambda n, r: jnp.concatenate(
                    [st[n, planes[i] * NZ + j, pl.ds(r, 1), :] for j in range(NZ)], axis=1
                )
                query = rows_of(queries, h)
                if it == 0:
                    p = jnp.exp(pk[h, i] - row(0, h))
                    pk[h, i] = p
                    grad = rows_of(grads, h)
                else:
                    p = pk[h, i]
                    grad = late[h][...].reshape(PLANE, HEAD_DIM)
                v = dot(p.astype(BF16), grad)
                gv = v if gv is None else gv + v
                gsc = (p * (gpk[h, i] - row(it, 2 + h))).astype(BF16)
                k = dot(gsc, query)
                gk = k if gk is None else gk + k
            dqkv[:, lanes(HEADS_DEV + h)] = turn(gk * scale, True).astype(BF16)
            dqkv[:, lanes(2 * HEADS_DEV + h)] = gv.astype(BF16)

    def own_queries(it):
        @pl.when(yl == 0)
        def _():
            query_side(it, ((kb, vb),))

        @pl.when(yl == 1)
        def _():
            query_side(it, ((kb, vb), (oa, ob)))

    most = gs.at[pl.ds(0, len(SEQ_STEPS))]
    gain_seq = remote(most, most, gss.at[0], gsr.at[0], partner)
    most = gt.at[pl.ds(0, 7)]
    gain_chip = remote(most, most, gts.at[0], gtr.at[0], partner)

    def backward(it):
        own = (qb, gb, (ga2, gb2))
        other = (oa, ob, (oa2, ob2))

        @pl.when(yl == 0)
        def _():
            over_wait(it)
            key_scores(it, (own, other))

        @pl.when(yl == 1)
        def _():
            key_scores(it, (own,))

        stats_all(it).wait_recv()

        @pl.when(yl == 0)
        def _():
            key_side(it, (own, other), (yl, 1 - yl))

        @pl.when(yl == 1)
        def _():
            key_side(it, (own,), (yl,))

        wide = HALF // CHUNKS
        gives = []
        for j in range(CHUNKS):
            cols = pl.ds(pl.multiple_of((1 - c) * HALF + j * wide, wide), wide)
            tot[it, j] = dot(dqkv[...], wqkv_t[:, cols]).astype(BF16).reshape(CHIPS, CROWS, wide)
            cp = remote(tot.at[it, j], drv.at[it, j], gvs.at[it, j], gvr.at[it, j], partner)
            cp.start()
            gives.append(cp)
        sends = []
        last_term = it == ITERS - 1
        for j in range(CHUNKS):
            cols = pl.ds(pl.multiple_of(c * HALF + j * wide, wide), wide)
            pair[j] = dot(dqkv[...], wqkv_t[:, cols]).reshape(CHIPS, CROWS, wide)

        def scatter(j):
            for k in range(7):
                a, b = chip_to(k)
                rsrc[it, j, k] = pair[j, a * NX + b].astype(BF16)
                remote(
                    rsrc.at[it, j, k], rrv.at[it, j, k], rss.at[it, j], rsr.at[it, j],
                    dev(yh_=a, x_=b),
                ).start()
            sends.append(
                remote(rsrc.at[it, j], rrv.at[it, j], rss.at[it, j], rsr.at[it, j], partner)
            )

        for j in range(CHUNKS):
            gives[j].wait_recv()
            pair[j] += drv[it, j].astype(F32)
            if not last_term:
                scatter(j)
        for j in range(CHUNKS):
            cols = pl.ds(pl.multiple_of(c * HALF + j * wide, wide), wide)
            here = pl.ds(j * wide, wide)
            term = jnp.sum(
                (pair[j] * agx[:, :, cols].astype(F32)).reshape(TOK, wide), axis=0, keepdims=True
            )
            gacc[:, here] = term if it == 0 else gacc[:, here] + term
            gn[:, here] = pair[j, chip]
        if last_term:
            gs[s] = gacc[...]
            for k in range(len(SEQ_STEPS)):
                a, b = seq_to(k)
                remote(gs.at[s], gs.at[s], gss.at[0], gsr.at[0], dev(yl_=a, z_=b)).start()
            for j in range(CHUNKS):
                scatter(j)
            gain_seq.wait_recv()
            acc = gs[0]
            for i in range(1, NY * NZ):
                acc = acc + gs[i]
            gt[chip] = acc
            for k in range(7):
                a, b = chip_to(k)
                remote(
                    gt.at[chip], gt.at[chip], gts.at[0], gtr.at[0], dev(yh_=a, x_=b)
                ).start()
            sent.extend([gain_seq, gain_chip])
        for j in range(CHUNKS):
            here = pl.ds(j * wide, wide)
            sends[j].wait_recv()
            total = gn[:, here]
            for k in range(7):
                total = total + rrv[it, j, k].astype(F32)
            gn[:, here] = total

        grad_normed = gn[...]
        scaled = sc16[...]
        weighted = gain_half * grad_normed
        inl[it] = jnp.broadcast_to(
            jnp.sum(weighted * scaled, axis=1, keepdims=True), (CROWS, 128)
        )
        share = remote(inl.at[it], inr.at[it], d2s.at[5 + it], d2r.at[5 + it], partner)
        share.start()
        share.wait_recv()
        inner = (inl[it] + inr[it])[:, 0:1]
        cot = ir16[:, 0:1] * (weighted - scaled * (inner / D))
        adj16[...] = (in16[...] if it == 0 else adj16[...]) + cot
        if it == 0:
            agc[chip, :, own_half] = cot.astype(BF16)
            gather_start(agc, 2)
        sent.extend(gives + [share] + sends)

    stats_start(0)
    ring_step(4, Q, G)
    own_queries(0)
    backward(0)

    ring_sent(K, V, Q, G, OA)
    gather_pass(agc, 2)
    gather_finish(agc, 2)
    grad2 = dot(agc[...].reshape(TOK, D), wo_t[...]).astype(BF16)
    ga2[z] = grad2[:, :HEAD_DIM]
    gb2[z] = grad2[:, HEAD_DIM:]

    far_send(GB, 2)
    far_send(GB, 1)
    send_over(GB, z)
    far_send(OA2, 2)

    @pl.when(yl == 1)
    def _():
        cross(ga2, oa2, 1).start()

    far_send(GA, 2)
    far_send(GA, 1)
    for h in range(HEADS_DEV):
        st[1, s, pl.ds(2 + h, 1), :] = as_row(
            jnp.sum(
                own_grad(1, h).astype(F32) * att[:, lanes(h)].astype(F32), axis=1, keepdims=True
            )
        )
    stats_start(1)
    own_queries(1)
    far_take(GB, 2)
    far_take(OA2, 2)
    far_take(GA, 2)

    @pl.when(yl == 0)
    def _():
        cross(oa2, oa2, 1).wait_recv()

    far_send(OA2, 1)
    far_take(GB, 1)
    far_take(GA, 1)
    far_take(GB, 3, 4)
    far_take(OA2, 1, 3, 4)
    far_take(GA, 3, 4)
    backward(1)

    back = remote(adj16.at[far_rows, :], adjr, d2s.at[7], d2r.at[7], partner)
    back.start()
    outs = [pltpu.make_async_copy(adj16.at[own_rows, :], adj_ref.at[:, own_half], out_sem.at[0])]
    outs[0].start()
    gain_chip.wait_recv()
    acc = gt[0]
    for i in range(1, CHIPS):
        acc = acc + gt[i]
    gh[0] = acc / gain_half * (NY * NZ * TOK) ** (-0.5)
    last = remote(gh.at[0], gh.at[1], d2s.at[8], d2r.at[8], partner)
    last.start()
    back.wait_recv()
    outs.append(pltpu.make_async_copy(adjr, adj_ref.at[:, far_half], out_sem.at[1]))
    outs[1].start()
    outs.append(pltpu.make_async_copy(gh.at[0], gg_ref.at[:, own_half], out_sem.at[2]))
    outs[2].start()
    last.wait_recv()
    outs.append(pltpu.make_async_copy(gh.at[1], gg_ref.at[:, far_half], out_sem.at[3]))
    outs[3].start()
    far_sent(GA, GB, OA2)
    gather_sent(agx, 0)
    gather_sent(agi, 1)
    gather_sent(agc, 2)

    @pl.when(yl == 0)
    def _():
        cross(kb, oa, 0).wait_send()

    @pl.when(yl == 1)
    def _():
        cross(qb, oa, 0).wait_send()

    @pl.when(yl == 1)
    def _():
        cross(ga2, oa2, 1).wait_send()

    for cp in sent + [stats_all(0), stats_all(1), back, last]:
        cp.wait_send()
    for cp in outs:
        cp.wait()


def scratch():
    v = pltpu.VMEM
    dma = pltpu.SemaphoreType.DMA
    wide = HALF // CHUNKS
    block = (NZ, TOK, WIDTH)
    half_block = (NZ, TOK, HEAD_DIM)
    return [
        v((ROWS, D), BF16), v((ROWS, D), BF16), v((1, D), F32), v((1, HEAD_DIM), F32),
        v((NBLK, NBLK), jnp.int32),
        v((D, 3 * WIDTH), BF16), v((WIDTH, D), BF16), v((3 * WIDTH, D), BF16), v((D, WIDTH), BF16),
        v((TOK, HEAD_DIM), F32), v((TOK, HEAD_DIM), F32),
        v((2, ROWS, D), F32), v((CROWS, HALF), F32), v((CROWS, HALF), F32), v((CROWS, 128), F32),
        v((ROWS, 128), F32),
        v((CHIPS, CROWS, D), BF16), v((CHIPS, CROWS, D), BF16), v((CHIPS, CROWS, D), BF16),
        v((HEADS_DEV, 2, TOK, PLANE), F32),
        v(block, BF16), v(block, BF16), v(block, BF16), v(block, BF16), v(block, BF16),
        v(block, BF16),
        v(half_block, BF16), v(half_block, BF16), v(half_block, BF16), v(half_block, BF16),
        v((ITERS, NY * NZ, 8, TOK), F32),
        v((2, TOK, PLANE), F32), v((2, TOK, PLANE), F32),
        v((HEADS_DEV, 2, TOK, PLANE), F32), v((HEADS_DEV, 2, TOK, PLANE), F32),
        v((TOK, WIDTH), BF16), v((TOK, 3 * WIDTH), BF16),
        v((ITERS, CHUNKS, CHIPS, CROWS, wide), BF16), v((ITERS, CHUNKS, CHIPS, CROWS, wide), BF16),
        v((ITERS, CHUNKS, 7, CROWS, wide), BF16), v((ITERS, CHUNKS, 7, CROWS, wide), BF16),
        v((CHUNKS, CHIPS, CROWS, wide), F32), v((CROWS, HALF), F32),
        v((ITERS, CROWS, 128), F32), v((ITERS, CROWS, 128), F32),
        v((CROWS, HALF), F32), v((ROWS, HALF), F32), v((1, HALF), F32),
        v((CHIPS, 1, HALF), F32), v((NY * NZ, 1, HALF), F32), v((2, 1, HALF), F32),
        dma((4,)), dma((5,)), dma((4,)), dma((3,)), dma((3, 7)), dma((3,)), dma((3,)), dma((9,)), dma((9,)),
        dma((5, 2, 4)), dma((5, 2, 4)), dma((2,)), dma((2,)), dma((2,)), dma((2,)),
        dma((ITERS,)), dma((ITERS,)), dma((ITERS, CHUNKS)), dma((ITERS, CHUNKS)),
        dma((ITERS, CHUNKS)), dma((ITERS, CHUNKS)),
        dma((1,)), dma((1,)), dma((1,)), dma((1,)),
    ]


def hand_over(a_ref, g_ref, a_out, g_out):
    a_out[...] = a_ref[...]
    g_out[...] = g_ref[...]


def body(
    fixed_point, incoming, norm_gain, query_weight, key_weight, value_weight, out_weight, layout
):
    pair = np.arange(HEAD_DIM) % (HEAD_DIM // 2)
    freq = jnp.asarray(THETA ** (-2.0 * pair / HEAD_DIM), F32)
    vmem = pl.BlockSpec(memory_space=pltpu.VMEM)
    hbm = pl.BlockSpec(memory_space=pl.ANY)
    adjoint, gain = pl.pallas_call(
        kernel,
        out_shape=(
            jax.ShapeDtypeStruct((ROWS, D), F32),
            jax.ShapeDtypeStruct((1, D), F32),
        ),
        in_specs=[hbm] * 9,
        out_specs=(hbm, hbm),
        scratch_shapes=scratch(),
        compiler_params=pltpu.CompilerParams(
            collective_id=0, has_side_effects=True, vmem_limit_bytes=62 * 1024 * 1024
        ),
        name="deq_backward",
    )(
        fixed_point, incoming, norm_gain[None, :], freq[None, :], layout,
        query_weight, key_weight, value_weight, out_weight,
    )
    adjoint, gain = pl.pallas_call(
        hand_over,
        out_shape=(
            jax.ShapeDtypeStruct((ROWS, D), F32),
            jax.ShapeDtypeStruct((1, D), F32),
        ),
        in_specs=[vmem] * 2,
        out_specs=(vmem, vmem),
        name="hand_over",
    )(adjoint, gain)
    return adjoint, gain[0]


def solution(mesh):
    split = Mesh(mesh.devices.reshape(NY, NZ, NH, NX, NC), AXES)
    in_specs = (
        P(SEQ_TENSOR, None),
        P(SEQ_TENSOR, None),
        P(),
        P(None, TENSOR),
        P(None, TENSOR),
        P(None, TENSOR),
        P(TENSOR, None),
        P(),
    )
    out_specs = (P(SEQ_TENSOR, None), P())
    return jax.shard_map(body, mesh=split, in_specs=in_specs, out_specs=out_specs, check_vma=False)
```
